32 devices in a mesh: group: 4 (over z), member: 8 (over y, x, core).
Axes of the slice: x: 2, y: 2, z: 4, core: 2. Of those that a mesh axis runs over, the one named last changes fastest.
Arguments:
- patterns: float32 [32, 2, 256, 512], P('group', None, 'member'), may hold values from -6 to 6
- operators: float32 [100, 2, 256, 512], P(None, None, 'member'), may hold values from -1 to 1
- partners: int32 [32, 8], P('group'), may hold values from 0 to 31, as said below
- operator_index: int32 [32, 8], P('group'), may hold values from 0 to 99
- child_parent: int32 [64], P('group'), may hold values from 0 to 31, as said below
- child_octant: int32 [64], P('group'), may hold values from 0 to 7, as said below
Outputs:
- child_patterns: float32 [64, 2, 128, 256], P('group', None, 'member')
The draws below stay inside these ranges and needn't reach their ends.
Inputs may be any that keep to these rules, and one draw needn't show every extreme that they name: `partners`: an entry of cluster c's list lies in c's own group block (clusters g * 8 to (g + 1) * 8 - 1); only the first 2 clusters of a block may also name any of the last 2 clusters of the previous block, and only the last 2 clusters any of the first 2 clusters of the next block. `child_parent`: the parent of a child in child block g (children g * 16 to (g + 1) * 16 - 1) lies in cluster block g; every cluster has at least one child; every cluster has 1 to 3 children, and in every block some cluster has exactly 3. `child_octant`: children of one parent have different octants.
All inputs are finite; a program needn't handle non-finite values.
Results may differ from the reference program's by a relative error of at most 0.0003.
Values sent between devices are 32-bit elements; how exact they have to be, the bound alone decides.
No kernel may reach another device: no remote copies, remote signals or barrier semaphores. Data moves between devices by JAX's collectives and lax.ppermute only.
A program may use at most 64 MiB of HBM per device.

```python
import math
import jax
import jax.numpy as jnp
from jax import lax

NT = 256
NP = 512
NTC = 128
NPC = 256
NOPS = 100
NPART = 8
PAR_DEV = 1
CL_GRP = 8
CLUSTERS = 32
BAND = 2
CH_GRP = 16
CHILDREN = 64


def children_helper(key):
    groups = CLUSTERS // CL_GRP
    members = CL_GRP // PAR_DEV
    key_a, key_b, key_c = jax.random.split(jax.random.fold_in(key, 71), 3)
    swing = jax.random.randint(key_a, (groups, members // 2), -PAR_DEV, PAR_DEV + 1)
    forced = jax.random.randint(key_b, (groups, 1), 0, members // 2)
    swing = jnp.where(jnp.arange(members // 2)[None, :] == forced, PAR_DEV, swing)
    counts = jnp.stack([2 * PAR_DEV + swing, 2 * PAR_DEV - swing], axis=2).reshape(groups, members)
    run_ends = jnp.cumsum(counts, axis=1)
    starts = run_ends - counts
    slot_ids = jnp.arange(CH_GRP)
    holder = jnp.sum((slot_ids[None, :, None] >= run_ends[:, None, :]).astype(jnp.int32), axis=2)
    offset = slot_ids[None, :] - jnp.take_along_axis(starts, holder, axis=1)
    perm_keys = jax.random.split(key_c, groups * members)

    def one_perm(single_key):
        return jax.random.permutation(single_key, 8)
    octant_perms = jax.vmap(one_perm)(perm_keys).reshape(groups, members * 8)
    octant_ids = jnp.take_along_axis(octant_perms, holder * 8 + offset // PAR_DEV, axis=1)
    parent_ids = jnp.arange(groups)[:, None] * CL_GRP + holder * PAR_DEV + offset % PAR_DEV
    return (parent_ids.reshape(-1).astype(jnp.int32), octant_ids.reshape(-1).astype(jnp.int32))


def draw_child_parent(key, part):
    return children_helper(key)[0]


def draw_child_octant(key, part):
    return children_helper(key)[1]


def draw_partners(key, part):
    groups = CLUSTERS // CL_GRP
    key_a, key_b, key_c = jax.random.split(jax.random.fold_in(key, 13), 3)
    cluster_ids = jnp.arange(CLUSTERS)[:, None]
    group_ids = cluster_ids // CL_GRP
    local_ids = cluster_ids % CL_GRP
    same_block = group_ids * CL_GRP + jax.random.randint(key_a, (CLUSTERS, NPART), 0, CL_GRP)
    cross_pick = jax.random.randint(key_b, (CLUSTERS, NPART), 0, 3)
    edge_ids = jax.random.randint(key_c, (CLUSTERS, NPART), 0, BAND)
    from_below = group_ids * CL_GRP - BAND + edge_ids
    from_above = (group_ids + 1) * CL_GRP + edge_ids
    use_below = (local_ids < BAND) & (group_ids > 0) & (cross_pick == 0)
    use_above = (local_ids >= CL_GRP - BAND) & (group_ids < groups - 1) & (cross_pick == 1)
    return jnp.where(use_below, from_below, jnp.where(use_above, from_above, same_block)).astype(jnp.int32)


def plant(values, rng, least, largest):
    place = [jax.random.randint(jax.random.fold_in(rng, axis), (), 0, length) for axis, length in enumerate(values.shape)]
    longest = values.shape.index(max(values.shape))
    neighbour = place[:longest] + [(place[longest] + 1) % values.shape[longest]] + place[longest + 1:]
    return values.at[tuple(place)].set(least).at[tuple(neighbour)].set(largest)


def block_levels(own_key, shape, pieces, smallest, high):
    loudness, own = 1.0, jax.random.fold_in(own_key, 6)
    for position, shards_of in pieces:
        heights = jnp.exp(jax.random.uniform(jax.random.fold_in(own, position), (shards_of,), jnp.float32, smallest / len(pieces), high / len(pieces)))
        loudness = loudness * jnp.repeat(heights, shape[position] // shards_of).reshape([-1 if axis == position else 1 for axis in range(len(shape))])
    return loudness


def bell_draw(key, extent, width, reach, shards=(), kind=jnp.bfloat16):
    values = jax.random.normal(key, extent, jnp.float32) * width
    if len(shards) > 0:
        values = block_levels(key, extent, shards, -0.22, 0.18) * values
    return jnp.clip(values, min=-reach, max=reach).astype(kind)


def setup_inputs(seed: int = 0) -> dict:
    splits = jax.random.split(jax.random.key(seed), 7)
    return {
        "patterns": bell_draw(splits[0], (CLUSTERS, 2, NT, NP), 1.0, 6.0, ((0, 4), (2, 8)), jnp.float32),
        "operators": bell_draw(splits[1], (NOPS, 2, NT, NP), 0.16, 1.0, ((2, 8),), jnp.float32),
        "partners": draw_partners(jax.random.fold_in(splits[6], 71), 0),
        "operator_index": plant(jax.random.randint(splits[3], (CLUSTERS, NPART), 0, NOPS), jax.random.fold_in(splits[3], 1), 0, NOPS - 1).astype(jnp.int32),
        "child_parent": draw_child_parent(jax.random.fold_in(splits[6], 71), 0),
        "child_octant": draw_child_octant(jax.random.fold_in(splits[6], 71), 0),
    }


shift_reach = 6.0


def anterp_tables(theta_count, phi_count, theta_child, phi_child):
    theta_fine = math.pi * (jnp.arange(theta_count, dtype=jnp.float32) + 0.5) / theta_count
    theta_coarse = math.pi * (jnp.arange(theta_child, dtype=jnp.float32) + 0.5) / theta_child
    orders = jnp.arange(theta_child, dtype=jnp.float32)
    weights = jnp.where(orders > 0, 2.0, 1.0).astype(jnp.float32)
    theta_matrix = jnp.dot(jnp.cos(jnp.outer(theta_coarse, orders)) * weights, jnp.cos(jnp.outer(theta_fine, orders)).T, precision=lax.Precision.HIGHEST) / theta_count
    phi_fine = 2.0 * math.pi * jnp.arange(phi_count, dtype=jnp.float32) / phi_count
    phi_coarse = 2.0 * math.pi * jnp.arange(phi_child, dtype=jnp.float32) / phi_child
    phi_modes = jnp.arange(phi_child // 2 + 1, dtype=jnp.float32)
    mode_weights = jnp.where((phi_modes > 0) & (phi_modes < phi_child // 2), 2.0, 1.0).astype(jnp.float32)
    cos_part = jnp.dot(jnp.cos(jnp.outer(phi_coarse, phi_modes)) * mode_weights, jnp.cos(jnp.outer(phi_fine, phi_modes)).T, precision=lax.Precision.HIGHEST)
    sin_part = jnp.dot(jnp.sin(jnp.outer(phi_coarse, phi_modes)) * mode_weights, jnp.sin(jnp.outer(phi_fine, phi_modes)).T, precision=lax.Precision.HIGHEST)
    phi_matrix = (cos_part + sin_part) / phi_count
    sin_theta = jnp.sin(theta_fine)[:, None]
    dir_x = sin_theta * jnp.cos(phi_fine)[None, :]
    dir_y = sin_theta * jnp.sin(phi_fine)[None, :]
    dir_z = jnp.cos(theta_fine)[:, None] * jnp.ones((1, phi_count), jnp.float32)
    return theta_matrix, phi_matrix, dir_x, dir_y, dir_z


def anterpolate(parents, octants, tables):
    theta_matrix, phi_matrix, dir_x, dir_y, dir_z = tables
    sign_x = (1 - 2 * (octants % 2)).astype(jnp.float32)[:, None, None]
    sign_y = (1 - 2 * ((octants // 2) % 2)).astype(jnp.float32)[:, None, None]
    sign_z = (1 - 2 * (octants // 4)).astype(jnp.float32)[:, None, None]
    phase_arg = shift_reach * (sign_x * dir_x + sign_y * dir_y + sign_z * dir_z)
    cosine = jnp.cos(phase_arg)
    sine_part = jnp.sin(phase_arg)
    real_part = parents[:, 0] * cosine - parents[:, 1] * sine_part
    imag_part = parents[:, 0] * sine_part + parents[:, 1] * cosine
    shifted = jnp.stack([real_part, imag_part], axis=1)
    coarse = jnp.einsum("jt,sktf->skjf", theta_matrix, shifted, precision=lax.Precision.HIGHEST)
    return jnp.einsum("skjf,gf->skjg", coarse, phi_matrix, precision=lax.Precision.HIGHEST)


def reference(patterns, operators, partners, operator_index, child_parent, child_octant):
    def add_partner(column, running):
        partner_rows = jnp.take(patterns, partners[:, column], axis=0)
        factors = jnp.take(operators, operator_index[:, column], axis=0)
        real_part = factors[:, 0] * partner_rows[:, 0] - factors[:, 1] * partner_rows[:, 1]
        imag_part = factors[:, 0] * partner_rows[:, 1] + factors[:, 1] * partner_rows[:, 0]
        return running + jnp.stack([real_part, imag_part], axis=1)

    translated = lax.fori_loop(0, NPART, add_partner, jnp.zeros(patterns.shape, jnp.float32))
    tables = anterp_tables(NT, NP, NTC, NPC)

    def child_block(block_in):
        parent_ids, octants = block_in
        return anterpolate(jnp.take(translated, parent_ids, axis=0), octants, tables)

    blocks = lax.map(child_block, (child_parent.reshape(-1, 16), child_octant.reshape(-1, 16)))
    return blocks.reshape(CHILDREN, 2, NTC, NPC)
```

```python
import functools
import math

import jax
import jax.numpy as jnp
import numpy as np
from jax import lax
from jax.experimental import pallas as pl
from jax.experimental.pallas import tpu as pltpu
from jax.sharding import PartitionSpec as P

NTC = 128
NPC = 256
CORES = 2
REACH = 6.0
F32 = jnp.float32
BF16 = jnp.bfloat16
MIB = 1 << 20


VMEM = pl.BlockSpec(memory_space=pltpu.VMEM)
SMEM = pl.BlockSpec(memory_space=pltpu.SMEM)
ANY = pl.BlockSpec(memory_space=pl.ANY)


def theta_table(fine, coarse):
    t = math.pi * (np.arange(fine) + 0.5) / fine
    j = math.pi * (np.arange(coarse) + 0.5) / coarse
    m = np.arange(coarse)
    w = np.where(m > 0, 2.0, 1.0)
    return (np.cos(np.outer(j, m)) * w) @ np.cos(np.outer(t, m)).T / fine


def phi_table(fine, coarse):
    f = 2.0 * math.pi * np.arange(fine) / fine
    g = 2.0 * math.pi * np.arange(coarse) / coarse
    m = np.arange(coarse // 2 + 1)
    v = np.where((m > 0) & (m < coarse // 2), 2.0, 1.0)
    cos_part = (np.cos(np.outer(g, m)) * v) @ np.cos(np.outer(f, m)).T
    sin_part = (np.sin(np.outer(g, m)) * v) @ np.sin(np.outer(f, m)).T
    return (cos_part + sin_part) / fine


def split_const(a):
    hi = np.asarray(a, np.float32).astype(BF16)
    lo = (np.asarray(a) - hi.astype(np.float64)).astype(np.float32).astype(BF16)
    return jnp.asarray(hi), jnp.asarray(lo)


def split(x):
    hi = x.astype(BF16)
    return hi, (x - hi.astype(F32)).astype(BF16)


def dot(a, b):
    return jnp.dot(a, b, preferred_element_type=F32)


def dot3(a, b):
    return dot(a[0], b[0]) + (dot(a[0], b[1]) + dot(a[1], b[0]))


def phase_tables(member, theta_count, phase_ref):
    rows, lons = phase_ref.shape[2], phase_ref.shape[3]
    quarter = lons // 4
    row = lax.broadcasted_iota(jnp.int32, (rows, 2 * quarter), 0)
    lon = lax.broadcasted_iota(jnp.int32, (rows, 2 * quarter), 1)
    theta = math.pi * ((row + member * rows).astype(F32) + 0.5) / theta_count
    phi = 2.0 * math.pi * lon.astype(F32) / lons
    x_arg = REACH * (jnp.sin(theta) * jnp.cos(phi))
    cos_x, sin_x = jnp.cos(x_arg), jnp.sin(x_arg)
    z_arg = REACH * jnp.cos(theta[:, :quarter])
    cz, sz = jnp.cos(z_arg), jnp.sin(z_arg)
    c0, c1 = cos_x[:, :quarter], cos_x[:, quarter:]
    s0, s1 = sin_x[:, :quarter], sin_x[:, quarter:]
    x_parts = ((c0, s0), (c1, s1), (c0, -s0), (c1, -s1))
    for q in range(4):
        ca, sa = x_parts[q]
        cb, sb = x_parts[(q + 3) % 4]
        cc, ss, sc, cs = ca * cb, sa * sb, sa * cb, ca * sb
        lanes = pl.ds(q * quarter, quarter)
        for octant in range(8):
            sgx = 1 - 2 * (octant % 2)
            sgy = 1 - 2 * (octant // 2 % 2)
            sgz = 1 - 2 * (octant // 4)
            re = cc - ss if sgx * sgy > 0 else cc + ss
            im = (sc if sgx > 0 else -sc) + (cs if sgy > 0 else -cs)
            szz = sz if sgz > 0 else -sz
            phase_ref[octant, 0, :, lanes] = re * cz - im * szz
            phase_ref[octant, 1, :, lanes] = re * szz + im * cz


def own_kernel(
    theta_count, place, partners, op_index, patterns, operators, out, phase, held, sems
):
    clusters, terms = partners.shape
    rows = out.shape[2]

    def fetch(e):
        c, p = e // terms, e % terms
        return pltpu.make_async_copy(operators.at[op_index[c, p]], held.at[e], sems.at[e])

    @pl.loop(0, clusters * terms)
    def _(e):
        fetch(e).start()

    phase_tables(place[0], theta_count, phase)
    base = place[1] * clusters

    @pl.loop(0, clusters)
    def _(c):
        for p in range(terms):
            fetch(c * terms + p).wait()
        for r in range(rows // 8):
            band = pl.ds(r * 8, 8)
            re, im = 0.0, 0.0
            for p in range(terms):
                e = c * terms + p
                q = partners[c, p] - base
                mine = jnp.where((q >= 0) & (q < clusters), 1.0, 0.0).astype(F32)
                q = jnp.clip(q, 0, clusters - 1)
                ore, oim = held[e, 0, band, :], held[e, 1, band, :]
                pre, pim = patterns[q, 0, band, :] * mine, patterns[q, 1, band, :] * mine
                re = re + (ore * pre - oim * pim)
                im = im + (ore * pim + oim * pre)
            out[c, 0, band, :] = re
            out[c, 1, band, :] = im


def child_kernel(
    place, partners, op_index, child_parent, child_octant, own, below, above, phase,
    phi_hi, phi_lo, operators, *rest
):
    clusters, terms = partners.shape
    chips = len(rest) - 4
    outs, (total, held, shifted, sems) = rest[:chips], rest[chips:]
    width = below.shape[0]
    rows = own.shape[2]
    base = place[1] * clusters
    chip = place[2]
    edges = list(range(width)) + list(range(clusters - width, clusters))

    def edge_terms(body):
        for n, c in enumerate(edges):
            for p in range(terms):
                q = partners[c, p] - base

                @pl.when((q < 0) | (q >= clusters))
                def _(n=n, c=c, p=p, q=q):
                    e = n * terms + p
                    copy = pltpu.make_async_copy(
                        operators.at[op_index[c, p]], held.at[e], sems.at[e]
                    )
                    body(copy, e, c, q)

    edge_terms(lambda copy, e, c, q: copy.start())
    total[...] = own[...]

    def add(copy, e, c, q):
        copy.wait()

        def accumulate(halo, h):
            @pl.loop(0, rows // 8)
            def _(r):
                band = pl.ds(pl.multiple_of(r * 8, 8), 8)
                ore, oim = held[e, 0, band, :], held[e, 1, band, :]
                pre, pim = halo[h, 0, band, :], halo[h, 1, band, :]
                total[c, 0, band, :] += ore * pre - oim * pim
                total[c, 1, band, :] += ore * pim + oim * pre

        @pl.when(q < 0)
        def _():
            accumulate(below, jnp.clip(q + width, 0, width - 1))

        @pl.when(q >= clusters)
        def _():
            accumulate(above, jnp.clip(q - clusters, 0, width - 1))

    edge_terms(add)

    per_chip = outs[0].shape[0]
    for s in range(chips):
        first = (chip ^ s) * per_chip
        for i in range(per_chip):
            q = child_parent[first + i] - base
            o = child_octant[first + i]
            for r in range(rows // 8):
                band = pl.ds(r * 8, 8)
                pre, pim = total[q, 0, band, :], total[q, 1, band, :]
                ere, eim = phase[o, 0, band, :], phase[o, 1, band, :]
                at = i * 2 * rows + r * 8
                shifted[pl.ds(at, 8), :] = pre * ere - pim * eim
                shifted[pl.ds(at + rows, 8), :] = pre * eim + pim * ere
        y = dot3(split(shifted[...]), (phi_hi[...], phi_lo[...]))
        outs[s][...] = y.reshape(outs[s].shape)


def theta_kernel(place, t_hi, t_lo, *rest):
    chips = len(rest) - 3
    blocks, (away, keep, lats) = rest[:chips], rest[chips:]
    chip, core = place[2], place[3]
    rows = blocks[0].shape[2]
    per_chip = blocks[0].shape[0]
    for i in range(per_chip):
        for part in range(2):
            for s in range(chips):
                at = pl.multiple_of((chip ^ s) * rows, rows)
                lats[pl.ds(at, rows), :] = blocks[s][i, part]
            x = split(lats[...])
            for out, which in ((away, 1 - core), (keep, core)):
                t = core * CORES + which
                out[i, part] = dot3((t_hi[t], t_lo[t]), x)


def sum_kernel(place, keep, arrived, *outs):
    chip = place[2]
    rows = outs[0].shape[2]
    for s, out in enumerate(outs):
        at = pl.multiple_of((chip ^ s) * rows, rows)
        for i in range(out.shape[0]):
            for part in range(2):
                band = pl.ds(at, rows)
                out[i, part] = keep[i, part, band, :] + arrived[i, part, band, :]


def place_kernel(place, *rest):
    chips = (len(rest) - 2)
    blocks, (out, sems) = rest[:chips], rest[chips:]
    per_chip = blocks[0].shape[0]
    copies = []
    for s in range(chips):
        first = (place[2] ^ s) * per_chip
        copy = pltpu.make_async_copy(
            blocks[s], out.at[pl.ds(first, per_chip)], sems.at[s]
        )
        copy.start()
        copies.append(copy)
    for copy in copies:
        copy.wait()


def shape(*dims):
    return jax.ShapeDtypeStruct(dims, F32)


def params(limit):
    return pltpu.CompilerParams(vmem_limit_bytes=limit * MIB)


def on_device(patterns, operators, partners, operator_index, child_parent, child_octant):
    clusters, _, rows, lons = patterns.shape
    terms = partners.shape[1]
    members = lax.axis_size("member")
    groups = lax.axis_size("group")
    theta_count = rows * members
    chips = members // CORES
    children = child_parent.shape[0]
    per_chip = children // chips
    out_rows = NTC // members
    width = clusters // 4
    member = lax.axis_index("member")
    group = lax.axis_index("group")
    chip, core = member // CORES, member % CORES
    place = jnp.stack([member, group, chip, core]).astype(jnp.int32)

    up = [(i, i + 1) for i in range(groups - 1)]
    down = [(i + 1, i) for i in range(groups - 1)]
    below = lax.ppermute(patterns[clusters - width:], "group", up)
    above = lax.ppermute(patterns[:width], "group", down)

    own, phase = pl.pallas_call(
        functools.partial(own_kernel, theta_count),
        out_shape=(shape(clusters, 2, rows, lons), shape(8, 2, rows, lons)),
        in_specs=[SMEM, SMEM, SMEM, VMEM, ANY],
        out_specs=(VMEM, VMEM),
        scratch_shapes=[
            pltpu.VMEM((clusters * terms, 2, rows, lons), F32),
            pltpu.SemaphoreType.DMA((clusters * terms,)),
        ],
        compiler_params=params(20),
        cost_estimate=pl.CostEstimate(
            flops=20_000_000, bytes_accessed=10_000_000, transcendentals=0
        ),
    )(place, partners, operator_index, patterns, operators)

    phi_hi, phi_lo = split_const(phi_table(lons, NPC).T)
    block = shape(per_chip, 2, rows, NPC)
    edge = 2 * width * terms
    sent = pl.pallas_call(
        child_kernel,
        out_shape=(block,) * chips,
        in_specs=[SMEM] * 5 + [VMEM] * 6 + [ANY],
        out_specs=(VMEM,) * chips,
        scratch_shapes=[
            pltpu.VMEM((clusters, 2, rows, lons), F32),
            pltpu.VMEM((edge, 2, rows, lons), F32),
            pltpu.VMEM((per_chip * 2 * rows, lons), F32),
            pltpu.SemaphoreType.DMA((edge,)),
        ],
        compiler_params=params(24),
        cost_estimate=pl.CostEstimate(
            flops=20_000_000, bytes_accessed=10_000_000, transcendentals=0
        ),
    )(
        place, partners, operator_index, child_parent, child_octant, own, below, above,
        phase, phi_hi, phi_lo, operators,
    )

    def between_chips(blocks):
        return [blocks[0]] + [
            lax.ppermute(
                blocks[s], "member", [(i, i ^ (CORES * s)) for i in range(members)]
            )
            for s in range(1, chips)
        ]

    blocks = between_chips(sent)

    table = theta_table(theta_count, NTC).reshape(chips, CORES, out_rows, chips, CORES, rows)
    table = table.transpose(4, 1, 0, 2, 3, 5).reshape(
        CORES * CORES, chips * out_rows, chips * rows
    )
    half = shape(per_chip, 2, chips * out_rows, NPC)
    piece = shape(per_chip, 2, out_rows, NPC)
    swap = [(i, i ^ 1) for i in range(members)]
    if out_rows % 8 == 0:
        t_hi, t_lo = split_const(table)
        away, keep = pl.pallas_call(
            theta_kernel,
            out_shape=(half, half),
            in_specs=[SMEM] + [VMEM] * (2 + chips),
            out_specs=(VMEM, VMEM),
            scratch_shapes=[pltpu.VMEM((chips * rows, NPC), F32)],
            compiler_params=params(12),
        )(place, t_hi, t_lo, *blocks)
        arrived = lax.ppermute(away, "member", swap)
        pieces = pl.pallas_call(
            sum_kernel,
            out_shape=(piece,) * chips,
            in_specs=[SMEM, VMEM, VMEM],
            out_specs=(VMEM,) * chips,
            compiler_params=params(12),
        )(place, keep, arrived)
    else:
        order = chip ^ jnp.arange(chips)
        lats = jnp.take(jnp.stack(blocks), order, axis=0)
        lats = lats.transpose(1, 2, 0, 3, 4).reshape(per_chip, 2, chips * rows, NPC)
        both = jnp.take(
            jnp.asarray(table, F32).reshape(CORES, CORES, chips * out_rows, chips * rows),
            core, axis=0,
        )
        sums = jnp.einsum(
            "wjt,kptg->wkpjg", both, lats, precision=lax.Precision.HIGHEST
        )
        arrived = lax.ppermute(jnp.take(sums, 1 - core, axis=0), "member", swap)
        total = jnp.take(sums, core, axis=0) + arrived
        total = total.reshape(per_chip, 2, chips, out_rows, NPC)
        pieces = [jnp.take(total, order[s], axis=2) for s in range(chips)]

    final = between_chips(list(pieces))
    return pl.pallas_call(
        place_kernel,
        out_shape=shape(children, 2, out_rows, NPC),
        in_specs=[SMEM] + [VMEM] * chips,
        out_specs=ANY,
        scratch_shapes=[pltpu.SemaphoreType.DMA((chips,))],
        compiler_params=params(12),
    )(place, *final)


def solution(mesh):
    return jax.shard_map(
        on_device,
        mesh=mesh,
        in_specs=(
            P("group", None, "member", None),
            P(None, None, "member", None),
            P("group", None),
            P("group", None),
            P("group"),
            P("group"),
        ),
        out_specs=P("group", None, "member", None),
        check_vma=False,
    )
```

```python
import functools
import math

import jax
import jax.numpy as jnp
import numpy as np
from jax import lax
from jax.experimental import pallas as pl
from jax.experimental.pallas import tpu as pltpu
from jax.sharding import PartitionSpec as P


NTC = 128
NPC = 256
CORES = 2
REACH = 6.0
F32 = jnp.float32
BF16 = jnp.bfloat16
MIB = 1 << 20


VMEM = pl.BlockSpec(memory_space=pltpu.VMEM)
SMEM = pl.BlockSpec(memory_space=pltpu.SMEM)
HBM = pl.BlockSpec(memory_space=pltpu.HBM)


def theta_table(fine, coarse):
    t = math.pi * (np.arange(fine) + 0.5) / fine
    j = math.pi * (np.arange(coarse) + 0.5) / coarse
    m = np.arange(coarse)
    w = np.where(m > 0, 2.0, 1.0)
    return (np.cos(np.outer(j, m)) * w) @ np.cos(np.outer(t, m)).T / fine


def phi_table(fine, coarse):
    f = 2.0 * math.pi * np.arange(fine) / fine
    g = 2.0 * math.pi * np.arange(coarse) / coarse
    m = np.arange(coarse // 2 + 1)
    v = np.where((m > 0) & (m < coarse // 2), 2.0, 1.0)
    cos_part = (np.cos(np.outer(g, m)) * v) @ np.cos(np.outer(f, m)).T
    sin_part = (np.sin(np.outer(g, m)) * v) @ np.sin(np.outer(f, m)).T
    return (cos_part + sin_part) / fine


def split_const(a):
    hi = np.asarray(a, np.float32).astype(BF16)
    lo = (np.asarray(a) - hi.astype(np.float64)).astype(np.float32).astype(BF16)
    return jnp.asarray(hi), jnp.asarray(lo)


def split(x):
    hi = x.astype(BF16)
    return hi, (x - hi.astype(F32)).astype(BF16)


def dot(a, b):
    return jnp.dot(a, b, preferred_element_type=F32)


def dot3(a, b):
    return dot(a[0], b[0]) + (dot(a[0], b[1]) + dot(a[1], b[0]))


def phase_tables(member, theta_count, phase_ref):
    rows, lons = phase_ref.shape[2], phase_ref.shape[3]
    quarter = lons // 4
    row = lax.broadcasted_iota(jnp.int32, (rows, 2 * quarter), 0)
    lon = lax.broadcasted_iota(jnp.int32, (rows, 2 * quarter), 1)
    theta = math.pi * ((row + member * rows).astype(F32) + 0.5) / theta_count
    phi = 2.0 * math.pi * lon.astype(F32) / lons
    x_arg = REACH * (jnp.sin(theta) * jnp.cos(phi))
    cos_x, sin_x = jnp.cos(x_arg), jnp.sin(x_arg)
    z_arg = REACH * jnp.cos(theta[:, :quarter])
    cz, sz = jnp.cos(z_arg), jnp.sin(z_arg)
    c0, c1 = cos_x[:, :quarter], cos_x[:, quarter:]
    s0, s1 = sin_x[:, :quarter], sin_x[:, quarter:]
    x_parts = ((c0, s0), (c1, s1), (c0, -s0), (c1, -s1))
    for q in range(4):
        ca, sa = x_parts[q]
        cb, sb = x_parts[(q + 3) % 4]
        cc, ss, sc, cs = ca * cb, sa * sb, sa * cb, ca * sb
        lanes = pl.ds(q * quarter, quarter)
        for octant in range(8):
            sgx = 1 - 2 * (octant % 2)
            sgy = 1 - 2 * (octant // 2 % 2)
            sgz = 1 - 2 * (octant // 4)
            re = cc - ss if sgx * sgy > 0 else cc + ss
            im = (sc if sgx > 0 else -sc) + (cs if sgy > 0 else -cs)
            szz = sz if sgz > 0 else -sz
            phase_ref[octant, 0, :, lanes] = re * cz - im * szz
            phase_ref[octant, 1, :, lanes] = re * szz + im * cz


def own_kernel(
    theta_count, width, table, patterns, operators, out, edge_ops, phase,
    mine, held, sems, mine_sem,
):
    clusters, _, rows, _ = out.shape
    terms = table.shape[1]
    inner = clusters - 2 * width

    def slot(c):
        return jnp.where(c < width, c, c - inner) * terms

    def fetch_edge(c, p):
        e = slot(c) + p
        return pltpu.make_async_copy(
            operators.at[table[clusters + c, p]], edge_ops.at[e], sems.at[c * terms + p]
        )

    def fetch_inner(c, p):
        return pltpu.make_async_copy(
            operators.at[table[clusters + c, p]], held.at[(c - width) * terms + p],
            sems.at[c * terms + p],
        )

    def edge_cluster(n):
        return jnp.where(n < width, n, n + inner)

    @pl.loop(0, inner * terms)
    def _(e):
        fetch_inner(width + e // terms, e % terms).start()

    @pl.loop(0, 2 * width * terms)
    def _(e):
        fetch_edge(edge_cluster(e // terms), e % terms).start()

    whole = pltpu.make_async_copy(patterns, mine, mine_sem)
    whole.start()
    phase_tables(table[2 * clusters, 0], theta_count, phase)
    base = table[2 * clusters, 1] * clusters
    whole.wait()

    def translate(c, ops, first):
        for r in range(rows // 8):
            band = pl.ds(r * 8, 8)
            re, im = 0.0, 0.0
            for p in range(terms):
                q = table[c, p] - base
                keep = jnp.where((q >= 0) & (q < clusters), 1.0, 0.0).astype(F32)
                q = jnp.clip(q, 0, clusters - 1)
                ore, oim = ops[first + p, 0, band, :], ops[first + p, 1, band, :]
                pre, pim = mine[q, 0, band, :] * keep, mine[q, 1, band, :] * keep
                re = re + (ore * pre - oim * pim)
                im = im + (ore * pim + oim * pre)
            out[c, 0, band, :] = re
            out[c, 1, band, :] = im

    @pl.loop(width, clusters - width)
    def _(c):
        for p in range(terms):
            fetch_inner(c, p).wait()
        translate(c, held, (c - width) * terms)

    @pl.loop(0, 2 * width)
    def _(n):
        c = edge_cluster(n)
        for p in range(terms):
            fetch_edge(c, p).wait()
        translate(c, edge_ops, n * terms)


def halo_terms(table, own, edge_ops, below, above, total):
    clusters, _, rows, _ = own.shape
    terms = table.shape[1]
    width = below.shape[0]
    base = table[2 * clusters, 1] * clusters
    total[...] = own[...]

    @pl.loop(0, 2 * width * terms)
    def _(e):
        n = e // terms
        c = jnp.where(n < width, n, n + clusters - 2 * width)
        q = table[c, e % terms] - base

        def accumulate(halo, h):
            for r in range(rows // 8):
                band = pl.ds(r * 8, 8)
                ore, oim = edge_ops[e, 0, band, :], edge_ops[e, 1, band, :]
                pre, pim = halo[h, 0, band, :], halo[h, 1, band, :]
                total[c, 0, band, :] += ore * pre - oim * pim
                total[c, 1, band, :] += ore * pim + oim * pre

        @pl.when(q < 0)
        def _():
            accumulate(below, jnp.clip(q + width, 0, width - 1))

        @pl.when(q >= clusters)
        def _():
            accumulate(above, jnp.clip(q - clusters, 0, width - 1))


def shift_and_phi(
    start, per_chip, others, table, child_parent, child_octant, total, phase, phi_hi, phi_lo,
    outs, shifted,
):
    clusters, _, rows, _ = total.shape
    base, chip = table[2 * clusters, 1] * clusters, table[2 * clusters, 2]
    for s, out in zip(others, outs):
        first = (chip ^ s) * per_chip + start
        size = out.shape[0] * 2 * rows
        for i in range(out.shape[0]):
            q = child_parent[first + i] - base
            o = child_octant[first + i]
            for r in range(rows // 8):
                band = pl.ds(r * 8, 8)
                pre, pim = total[q, 0, band, :], total[q, 1, band, :]
                ere, eim = phase[o, 0, band, :], phase[o, 1, band, :]
                at = i * 2 * rows + r * 8
                shifted[pl.ds(at, 8), :] = pre * ere - pim * eim
                shifted[pl.ds(at + rows, 8), :] = pre * eim + pim * ere
        y = dot3(split(shifted[pl.ds(0, size), :]), (phi_hi[...], phi_lo[...]))
        out[...] = y.reshape(out.shape)


def first_kernel(
    per_chip, table, child_parent, child_octant, own, edge_ops, below, above, phase,
    phi_hi, phi_lo, *rest
):
    outs, (total, shifted) = rest[:-2], rest[-2:]
    halo_terms(table, own, edge_ops, below, above, total)
    shift_and_phi(
        0, per_chip, range(1, len(outs) + 1), table, child_parent, child_octant, total, phase,
        phi_hi, phi_lo, outs, shifted,
    )


def later_kernel(
    start, per_chip, table, child_parent, child_octant, total, phase, phi_hi, phi_lo, *rest
):
    (mine, *outs), shifted = rest[:-1], rest[-1]
    args = (table, child_parent, child_octant, total, phase, phi_hi, phi_lo)
    shift_and_phi(start, per_chip, range(1, len(outs) + 1), *args, outs, shifted)
    shift_and_phi(0, per_chip, [0], *args, [mine], shifted)


def theta_kernel(start, table, t_hi, t_lo, mine, *rest):
    others, (away, keep, lats) = rest[:-3], rest[-3:]
    last = table.shape[0] - 1
    chip, core = table[last, 2], table[last, 3]
    rows = mine.shape[2]
    for i in range(away.shape[0]):
        for part in range(2):
            at = pl.multiple_of(chip * rows, rows)
            lats[pl.ds(at, rows), :] = mine[start + i, part]
            for s, block in enumerate(others, 1):
                at = pl.multiple_of((chip ^ s) * rows, rows)
                lats[pl.ds(at, rows), :] = block[i, part]
            x = split(lats[...])
            for out, which in ((away, 1 - core), (keep, core)):
                t = core * CORES + which
                out[i, part] = dot3((t_hi[t], t_lo[t]), x)


def sum_kernel(*refs):
    *halves, out = refs
    parts = len(halves) // 2
    chips, _, _, rows, _ = out.shape
    first = 0
    for keep, arrived in zip(halves[:parts], halves[parts:]):
        per = keep.shape[0]
        for chip in range(chips):
            band = pl.ds(chip * rows, rows)
            out[chip, pl.ds(first, per)] = keep[:, :, band, :] + arrived[:, :, band, :]
        first += per


def in_hbm(x):
    return pltpu.with_memory_space_constraint(x, pltpu.HBM)


def shape(*dims):
    return jax.ShapeDtypeStruct(dims, F32)


def params(limit):
    return pltpu.CompilerParams(vmem_limit_bytes=limit * MIB)


def call(*args, **kwargs):
    return pl.pallas_call(*args, **kwargs)


def cost(us):
    return pl.CostEstimate(flops=us * 2_000_000, bytes_accessed=0, transcendentals=0)


def on_device(patterns, operators, partners, operator_index, child_parent, child_octant):
    clusters, _, rows, lons = patterns.shape
    members = lax.axis_size("member")
    groups = lax.axis_size("group")
    theta_count = rows * members
    chips = members // CORES
    children = child_parent.shape[0]
    per_chip = children // chips
    out_rows = NTC // members
    width = clusters // 4
    member = lax.axis_index("member")
    group = lax.axis_index("group")
    chip, core = member // CORES, member % CORES
    terms = partners.shape[1]
    here = jnp.stack([member, group, chip, core]).astype(jnp.int32)
    table = jnp.concatenate(
        [partners, operator_index, jnp.pad(here, (0, terms - 4))[None, :]]
    )

    up = [(i, i + 1) for i in range(groups - 1)]
    down = [(i + 1, i) for i in range(groups - 1)]
    below = lax.ppermute(patterns[clusters - width:], "group", up)
    above = lax.ppermute(patterns[:width], "group", down)

    edge = 2 * width * terms
    total_shape = shape(clusters, 2, rows, lons)
    own, edge_ops, phase = pl.pallas_call(
        functools.partial(own_kernel, theta_count, width),
        out_shape=(
            total_shape, shape(edge, 2, rows, lons), shape(8, 2, rows, lons),
        ),
        in_specs=[SMEM, HBM, HBM],
        out_specs=(VMEM, VMEM, VMEM),
        scratch_shapes=[
            pltpu.VMEM((clusters, 2, rows, lons), F32),
            pltpu.VMEM((clusters * terms - edge, 2, rows, lons), F32),
            pltpu.SemaphoreType.DMA((clusters * terms,)),
            pltpu.SemaphoreType.DMA,
        ],
        compiler_params=params(20),
        cost_estimate=cost(8),
    )(table, in_hbm(patterns), in_hbm(operators))

    phi = split_const(phi_table(lons, NPC).T)
    lead = max(per_chip // 2, 1)
    sizes = [lead, per_chip - lead]

    def blocks_of(count):
        return (shape(count, 2, rows, NPC),) * (chips - 1)

    shifted = pltpu.VMEM((per_chip * 2 * rows, lons), F32)
    *blocks0, total = call(
        functools.partial(first_kernel, per_chip),
        out_shape=blocks_of(sizes[0]) + (total_shape,),
        in_specs=[SMEM] * 3 + [VMEM] * 7,
        out_specs=(VMEM,) * chips,
        scratch_shapes=[shifted],
        compiler_params=params(20),
        cost_estimate=cost(2),
    )(table, child_parent, child_octant, own, edge_ops, below, above, phase, *phi)
    mine, *blocks1 = call(
        functools.partial(later_kernel, sizes[0], per_chip),
        out_shape=(shape(per_chip, 2, rows, NPC),) + blocks_of(sizes[1]),
        in_specs=[SMEM] * 3 + [VMEM] * 4,
        out_specs=(VMEM,) * chips,
        scratch_shapes=[shifted],
        compiler_params=params(20),
        cost_estimate=cost(1),
    )(table, child_parent, child_octant, total, phase, *phi)

    def between_chips(blocks):
        moved = []
        for s, block in enumerate(blocks, 1):
            pairs = [(i, i ^ (CORES * s)) for i in range(members)]
            moved.append(lax.ppermute(block, "member", pairs))
        return moved

    arrived = [between_chips(blocks0), between_chips(blocks1)]

    theta = theta_table(theta_count, NTC).reshape(chips, CORES, out_rows, chips, CORES, rows)
    theta = theta.transpose(4, 1, 0, 2, 3, 5).reshape(
        CORES * CORES, chips * out_rows, chips * rows
    )
    swap = [(i, i ^ 1) for i in range(members)]
    if out_rows % 8 == 0:
        t_hi, t_lo = split_const(theta)
        keeps, swapped = [], []
        for h, first in enumerate((0, sizes[0])):
            half = shape(sizes[h], 2, chips * out_rows, NPC)
            away, keep = call(
                functools.partial(theta_kernel, first),
                out_shape=(half, half),
                in_specs=[SMEM] + [VMEM] * (2 + chips),
                out_specs=(VMEM, VMEM),
                scratch_shapes=[pltpu.VMEM((chips * rows, NPC), F32)],
                compiler_params=params(12),
                cost_estimate=cost(1),
            )(table, t_hi, t_lo, mine, *arrived[h])
            keeps.append(keep)
            swapped.append(lax.ppermute(away, "member", swap))
        pieces = call(
            sum_kernel,
            out_shape=shape(chips, per_chip, 2, out_rows, NPC),
            in_specs=[VMEM] * 4,
            out_specs=VMEM,
            compiler_params=params(12),
            cost_estimate=cost(1),
        )(*keeps, *swapped)
    else:
        lats = jnp.stack([jnp.concatenate(pair) for pair in zip(*arrived)])
        lats = jnp.concatenate([mine[None], lats])
        lats = jnp.take(lats, chip ^ jnp.arange(chips), axis=0)
        lats = lats.transpose(1, 2, 0, 3, 4).reshape(per_chip, 2, chips * rows, NPC)
        both = jnp.take(
            jnp.asarray(theta, F32).reshape(CORES, CORES, chips * out_rows, chips * rows),
            core, axis=0,
        )
        sums = jnp.einsum(
            "wjt,kptg->wkpjg", both, lats, precision=lax.Precision.HIGHEST
        )
        moved = lax.ppermute(jnp.take(sums, 1 - core, axis=0), "member", swap)
        pieces = jnp.take(sums, core, axis=0) + moved
        pieces = pieces.reshape(per_chip, 2, chips, out_rows, NPC).transpose(2, 0, 1, 3, 4)

    same_core = [list(range(c, members, CORES)) for c in range(CORES)]
    out = lax.all_to_all(
        pieces, "member", 0, 0, tiled=True, axis_index_groups=same_core
    )
    return out.reshape(children, 2, out_rows, NPC)


def solution(mesh):
    return jax.shard_map(
        on_device,
        mesh=mesh,
        in_specs=(
            P("group", None, "member", None),
            P(None, None, "member", None),
            P("group", None),
            P("group", None),
            P("group"),
            P("group"),
        ),
        out_specs=P("group", None, "member", None),
        check_vma=False,
    )
```

```python
import functools
import math

import jax
import jax.numpy as jnp
import numpy as np
from jax import lax
from jax.experimental import pallas as pl
from jax.experimental.pallas import tpu as pltpu
from jax.sharding import PartitionSpec as P


NTC = 128
NPC = 256
CORES = 2
REACH = 6.0
F32 = jnp.float32
BF16 = jnp.bfloat16
MIB = 1 << 20


VMEM = pl.BlockSpec(memory_space=pltpu.VMEM)
SMEM = pl.BlockSpec(memory_space=pltpu.SMEM)
HBM = pl.BlockSpec(memory_space=pltpu.HBM)


def theta_table(fine, coarse):
    t = math.pi * (np.arange(fine) + 0.5) / fine
    j = math.pi * (np.arange(coarse) + 0.5) / coarse
    m = np.arange(coarse)
    w = np.where(m > 0, 2.0, 1.0)
    return (np.cos(np.outer(j, m)) * w) @ np.cos(np.outer(t, m)).T / fine


def phi_table(fine, coarse):
    f = 2.0 * math.pi * np.arange(fine) / fine
    g = 2.0 * math.pi * np.arange(coarse) / coarse
    m = np.arange(coarse // 2 + 1)
    v = np.where((m > 0) & (m < coarse // 2), 2.0, 1.0)
    cos_part = (np.cos(np.outer(g, m)) * v) @ np.cos(np.outer(f, m)).T
    sin_part = (np.sin(np.outer(g, m)) * v) @ np.sin(np.outer(f, m)).T
    return (cos_part + sin_part) / fine


def split_const(a):
    hi = np.asarray(a, np.float32).astype(BF16)
    lo = (np.asarray(a) - hi.astype(np.float64)).astype(np.float32).astype(BF16)
    return jnp.asarray(hi), jnp.asarray(lo)


def split(x):
    hi = x.astype(BF16)
    return hi, (x - hi.astype(F32)).astype(BF16)


def dot(a, b):
    return jnp.dot(a, b, preferred_element_type=F32)


def dot3(a, b):
    return dot(a[0], b[0]) + (dot(a[0], b[1]) + dot(a[1], b[0]))


def phase_tables(member, theta_count, phase_ref):
    rows, lons = phase_ref.shape[2], phase_ref.shape[3]
    quarter = lons // 4
    row = lax.broadcasted_iota(jnp.int32, (rows, 2 * quarter), 0)
    lon = lax.broadcasted_iota(jnp.int32, (rows, 2 * quarter), 1)
    theta = math.pi * ((row + member * rows).astype(F32) + 0.5) / theta_count
    phi = 2.0 * math.pi * lon.astype(F32) / lons
    x_arg = REACH * (jnp.sin(theta) * jnp.cos(phi))
    cos_x, sin_x = jnp.cos(x_arg), jnp.sin(x_arg)
    z_arg = REACH * jnp.cos(theta[:, :quarter])
    cz, sz = jnp.cos(z_arg), jnp.sin(z_arg)
    c0, c1 = cos_x[:, :quarter], cos_x[:, quarter:]
    s0, s1 = sin_x[:, :quarter], sin_x[:, quarter:]
    x_parts = ((c0, s0), (c1, s1), (c0, -s0), (c1, -s1))
    for q in range(4):
        ca, sa = x_parts[q]
        cb, sb = x_parts[(q + 3) % 4]
        cc, ss, sc, cs = ca * cb, sa * sb, sa * cb, ca * sb
        lanes = pl.ds(q * quarter, quarter)
        for octant in range(8):
            sgx = 1 - 2 * (octant % 2)
            sgy = 1 - 2 * (octant // 2 % 2)
            sgz = 1 - 2 * (octant // 4)
            re = cc - ss if sgx * sgy > 0 else cc + ss
            im = (sc if sgx > 0 else -sc) + (cs if sgy > 0 else -cs)
            szz = sz if sgz > 0 else -sz
            phase_ref[octant, 0, :, lanes] = re * cz - im * szz
            phase_ref[octant, 1, :, lanes] = re * szz + im * cz


def own_kernel(
    theta_count, width, table, patterns, operators, out, edge_ops, phase,
    mine, held, sems, mine_sem,
):
    clusters, _, rows, _ = out.shape
    terms = table.shape[1]
    inner = clusters - 2 * width

    def slot(c):
        return jnp.where(c < width, c, c - inner) * terms

    def fetch_edge(c, p):
        e = slot(c) + p
        return pltpu.make_async_copy(
            operators.at[table[clusters + c, p]], edge_ops.at[e], sems.at[c * terms + p]
        )

    def fetch_inner(c, p):
        return pltpu.make_async_copy(
            operators.at[table[clusters + c, p]], held.at[(c - width) * terms + p],
            sems.at[c * terms + p],
        )

    whole = pltpu.make_async_copy(patterns, mine, mine_sem)
    whole.start()

    def edge_cluster(n):
        return jnp.where(n < width, n, n + inner)

    @pl.loop(0, inner * terms)
    def _(e):
        fetch_inner(width + e // terms, e % terms).start()

    @pl.loop(0, 2 * width * terms)
    def _(e):
        fetch_edge(edge_cluster(e // terms), e % terms).start()

    phase_tables(lax.axis_index("member"), theta_count, phase)
    base = lax.axis_index("group") * clusters
    whole.wait()

    def translate(c, ops, first):
        for r in range(rows // 8):
            band = pl.ds(r * 8, 8)
            re, im = 0.0, 0.0
            for p in range(terms):
                q = table[c, p] - base
                keep = jnp.where((q >= 0) & (q < clusters), 1.0, 0.0).astype(F32)
                q = jnp.clip(q, 0, clusters - 1)
                ore, oim = ops[first + p, 0, band, :], ops[first + p, 1, band, :]
                pre, pim = mine[q, 0, band, :] * keep, mine[q, 1, band, :] * keep
                re = re + (ore * pre - oim * pim)
                im = im + (ore * pim + oim * pre)
            out[c, 0, band, :] = re
            out[c, 1, band, :] = im

    @pl.loop(width, clusters - width)
    def _(c):
        for p in range(terms):
            fetch_inner(c, p).wait()
        translate(c, held, (c - width) * terms)

    @pl.loop(0, 2 * width)
    def _(n):
        c = edge_cluster(n)
        for p in range(terms):
            fetch_edge(c, p).wait()
        translate(c, edge_ops, n * terms)


def halo_terms(table, own, edge_ops, below, above, total):
    clusters, _, rows, _ = own.shape
    terms = table.shape[1]
    width = below.shape[0]
    base = lax.axis_index("group") * clusters
    total[...] = own[...]

    for n in range(2 * width):
        c = n if n < width else n + clusters - 2 * width
        halo = below if n < width else above
        shift = width - base if n < width else -base - clusters

        @pl.loop(0, terms)
        def _(p):
            q = table[c, p] - base

            @pl.when((q < 0) | (q >= clusters))
            def _():
                e = n * terms + p
                h = jnp.clip(table[c, p] + shift, 0, width - 1)
                for r in range(rows // 8):
                    band = pl.ds(r * 8, 8)
                    ore, oim = edge_ops[e, 0, band, :], edge_ops[e, 1, band, :]
                    pre, pim = halo[h, 0, band, :], halo[h, 1, band, :]
                    total[c, 0, band, :] += ore * pre - oim * pim
                    total[c, 1, band, :] += ore * pim + oim * pre


def shift_and_phi(order, table, total, phase, phi_hi, phi_lo, outs, shifted):
    clusters, _, rows, _ = total.shape
    terms = table.shape[1]
    base = lax.axis_index("group") * clusters
    chip = lax.axis_index("member") // CORES
    parents = 2 * clusters
    octants = parents + (table.shape[0] - parents) // 2
    for s, out in zip(order, outs):
        first = (chip ^ s) * out.shape[0]
        for i in range(out.shape[0]):
            row, column = (first + i) // terms, (first + i) % terms
            q = table[parents + row, column] - base
            o = table[octants + row, column]
            for r in range(rows // 8):
                band = pl.ds(r * 8, 8)
                pre, pim = total[q, 0, band, :], total[q, 1, band, :]
                ere, eim = phase[o, 0, band, :], phase[o, 1, band, :]
                at = i * 2 * rows + r * 8
                shifted[pl.ds(at, 8), :] = pre * ere - pim * eim
                shifted[pl.ds(at + rows, 8), :] = pre * eim + pim * ere
        y = dot3(split(shifted[...]), (phi_hi[...], phi_lo[...]))
        out[...] = y.reshape(out.shape)


def first_kernel(
    order, table, own, edge_ops, below, above, phase, phi_hi, phi_lo, *rest
):
    outs, (total, shifted) = rest[:-2], rest[-2:]
    halo_terms(table, own, edge_ops, below, above, total)
    shift_and_phi(order, table, total, phase, phi_hi, phi_lo, outs, shifted)


def later_kernel(order, table, total, phase, phi_hi, phi_lo, *rest):
    shift_and_phi(order, table, total, phase, phi_hi, phi_lo, rest[:-1], rest[-1])


def theta_kernel(t_hi, t_lo, *rest):
    blocks, (away, keep, lats) = rest[:-3], rest[-3:]
    member = lax.axis_index("member")
    chip, core = member // CORES, member % CORES
    per_chip, _, rows, _ = blocks[0].shape
    for i in range(per_chip):
        for part in range(2):
            for s, block in enumerate(blocks):
                at = pl.multiple_of((chip ^ s) * rows, rows)
                lats[pl.ds(at, rows), :] = block[i, part]
            x = split(lats[...])
            for out, which in ((away, 1 - core), (keep, core)):
                t = core * CORES + which
                out[i, part] = dot3((t_hi[t], t_lo[t]), x)


def sum_kernel(keep, arrived, *outs):
    chip = lax.axis_index("member") // CORES
    rows = outs[0].shape[2]
    for s, out in enumerate(outs):
        band = pl.ds(pl.multiple_of((chip ^ s) * rows, rows), rows)
        out[...] = keep[:, :, band, :] + arrived[:, :, band, :]


def place_kernel(*rest):
    blocks, (out, sems) = rest[:-2], rest[-2:]
    chip = lax.axis_index("member") // CORES
    per_chip = blocks[0].shape[0]
    copies = []
    for s, block in enumerate(blocks):
        first = (chip ^ s) * per_chip
        copy = pltpu.make_async_copy(block, out.at[pl.ds(first, per_chip)], sems.at[s])
        copy.start()
        copies.append(copy)
    for copy in copies:
        copy.wait()


def in_hbm(x):
    return pltpu.with_memory_space_constraint(x, pltpu.HBM)


def shape(*dims):
    return jax.ShapeDtypeStruct(dims, F32)


def params(limit):
    return pltpu.CompilerParams(vmem_limit_bytes=limit * MIB)


def call(*args, **kwargs):
    return pl.pallas_call(*args, **kwargs)


def cost(us):
    return pl.CostEstimate(flops=us * 2_000_000, bytes_accessed=0, transcendentals=0)


def on_device(patterns, operators, partners, operator_index, child_parent, child_octant):
    clusters, _, rows, lons = patterns.shape
    members = lax.axis_size("member")
    groups = lax.axis_size("group")
    theta_count = rows * members
    chips = members // CORES
    children = child_parent.shape[0]
    per_chip = children // chips
    out_rows = NTC // members
    width = clusters // 4
    member = lax.axis_index("member")
    chip, core = member // CORES, member % CORES
    terms = partners.shape[1]
    table = jnp.concatenate(
        [
            partners,
            operator_index,
            child_parent.reshape(-1, terms),
            child_octant.reshape(-1, terms),
        ]
    )

    up = [(i, i + 1) for i in range(groups - 1)]
    down = [(i + 1, i) for i in range(groups - 1)]
    below = lax.ppermute(patterns[clusters - width:], "group", up)
    above = lax.ppermute(patterns[:width], "group", down)

    edge = 2 * width * terms
    total_shape = shape(clusters, 2, rows, lons)
    own, edge_ops, phase = pl.pallas_call(
        functools.partial(own_kernel, theta_count, width),
        out_shape=(
            total_shape, shape(edge, 2, rows, lons), shape(8, 2, rows, lons),
        ),
        in_specs=[SMEM, HBM, HBM],
        out_specs=(VMEM, VMEM, VMEM),
        scratch_shapes=[
            pltpu.VMEM((clusters, 2, rows, lons), F32),
            pltpu.VMEM((clusters * terms - edge, 2, rows, lons), F32),
            pltpu.SemaphoreType.DMA((clusters * terms,)),
            pltpu.SemaphoreType.DMA,
        ],
        compiler_params=params(20),
        cost_estimate=cost(8),
    )(table, in_hbm(patterns), in_hbm(operators))

    phi = split_const(phi_table(lons, NPC).T)
    block = shape(per_chip, 2, rows, NPC)
    shifted = pltpu.VMEM((per_chip * 2 * rows, lons), F32)
    far, near = [chips - 1], [*range(1, chips - 1), 0]
    sent = dict.fromkeys(range(chips))
    *outs, total = call(
        functools.partial(first_kernel, far),
        out_shape=(block,) * len(far) + (total_shape,),
        in_specs=[SMEM] + [VMEM] * 7,
        out_specs=(VMEM,) * (len(far) + 1),
        scratch_shapes=[shifted],
        compiler_params=params(20),
        cost_estimate=cost(2),
    )(table, own, edge_ops, below, above, phase, *phi)
    sent.update(zip(far, outs))
    outs = call(
        functools.partial(later_kernel, near),
        out_shape=(block,) * len(near),
        in_specs=[SMEM] + [VMEM] * 4,
        out_specs=(VMEM,) * len(near),
        scratch_shapes=[shifted],
        compiler_params=params(20),
        cost_estimate=cost(1),
    )(table, total, phase, *phi)
    sent.update(zip(near, outs))

    def between_chips(blocks):
        moved = dict(blocks)
        for s in range(chips - 1, 0, -1):
            pairs = [(i, i ^ (CORES * s)) for i in range(members)]
            moved[s] = lax.ppermute(blocks[s], "member", pairs)
        return [moved[s] for s in range(chips)]

    arrived = between_chips(sent)

    theta = theta_table(theta_count, NTC).reshape(chips, CORES, out_rows, chips, CORES, rows)
    theta = theta.transpose(4, 1, 0, 2, 3, 5).reshape(
        CORES * CORES, chips * out_rows, chips * rows
    )
    swap = [(i, i ^ 1) for i in range(members)]
    if out_rows % 8 == 0:
        half = shape(per_chip, 2, chips * out_rows, NPC)
        away, keep = call(
            theta_kernel,
            out_shape=(half, half),
            in_specs=[VMEM] * (2 + chips),
            out_specs=(VMEM, VMEM),
            scratch_shapes=[pltpu.VMEM((chips * rows, NPC), F32)],
            compiler_params=params(12),
            cost_estimate=cost(1),
        )(*split_const(theta), *arrived)
        swapped = lax.ppermute(away, "member", swap)
        pieces = call(
            sum_kernel,
            out_shape=(shape(per_chip, 2, out_rows, NPC),) * chips,
            in_specs=[VMEM] * 2,
            out_specs=(VMEM,) * chips,
            compiler_params=params(12),
            cost_estimate=cost(1),
        )(keep, swapped)
    else:
        order = chip ^ jnp.arange(chips)
        lats = jnp.take(jnp.stack(arrived), order, axis=0)
        lats = lats.transpose(1, 2, 0, 3, 4).reshape(per_chip, 2, chips * rows, NPC)
        both = jnp.take(
            jnp.asarray(theta, F32).reshape(CORES, CORES, chips * out_rows, chips * rows),
            core, axis=0,
        )
        sums = jnp.einsum(
            "wjt,kptg->wkpjg", both, lats, precision=lax.Precision.HIGHEST
        )
        moved = lax.ppermute(jnp.take(sums, 1 - core, axis=0), "member", swap)
        pieces = jnp.take(sums, core, axis=0) + moved
        pieces = pieces.reshape(per_chip, 2, chips, out_rows, NPC)
        pieces = [jnp.take(pieces, order[s], axis=2) for s in range(chips)]

    final = between_chips(dict(enumerate(pieces)))
    return call(
        place_kernel,
        out_shape=shape(children, 2, out_rows, NPC),
        in_specs=[VMEM] * chips,
        out_specs=HBM,
        scratch_shapes=[pltpu.SemaphoreType.DMA((chips,))],
        compiler_params=params(12),
        cost_estimate=cost(1),
    )(*final)


def solution(mesh):
    return jax.shard_map(
        on_device,
        mesh=mesh,
        in_specs=(
            P("group", None, "member", None),
            P(None, None, "member", None),
            P("group", None),
            P("group", None),
            P("group"),
            P("group"),
        ),
        out_specs=P("group", None, "member", None),
        check_vma=False,
    )
```

```python
import functools
import math

import jax
import jax.numpy as jnp
import numpy as np
from jax import lax
from jax.experimental import pallas as pl
from jax.experimental.pallas import tpu as pltpu
from jax.sharding import PartitionSpec as P


NTC = 128
NPC = 256
CORES = 2
REACH = 6.0
F32 = jnp.float32
BF16 = jnp.bfloat16
MIB = 1 << 20


VMEM = pl.BlockSpec(memory_space=pltpu.VMEM)
SMEM = pl.BlockSpec(memory_space=pltpu.SMEM)
HBM = pl.BlockSpec(memory_space=pltpu.HBM)


def theta_table(fine, coarse):
    t = math.pi * (np.arange(fine) + 0.5) / fine
    j = math.pi * (np.arange(coarse) + 0.5) / coarse
    m = np.arange(coarse)
    w = np.where(m > 0, 2.0, 1.0)
    return (np.cos(np.outer(j, m)) * w) @ np.cos(np.outer(t, m)).T / fine


def phi_table(fine, coarse):
    f = 2.0 * math.pi * np.arange(fine) / fine
    g = 2.0 * math.pi * np.arange(coarse) / coarse
    m = np.arange(coarse // 2 + 1)
    v = np.where((m > 0) & (m < coarse // 2), 2.0, 1.0)
    cos_part = (np.cos(np.outer(g, m)) * v) @ np.cos(np.outer(f, m)).T
    sin_part = (np.sin(np.outer(g, m)) * v) @ np.sin(np.outer(f, m)).T
    return (cos_part + sin_part) / fine


def split_const(a):
    hi = np.asarray(a, np.float32).astype(BF16)
    lo = (np.asarray(a) - hi.astype(np.float64)).astype(np.float32).astype(BF16)
    return jnp.asarray(hi), jnp.asarray(lo)


def split(x):
    hi = x.astype(BF16)
    return hi, (x - hi.astype(F32)).astype(BF16)


def dot(a, b):
    return jnp.dot(a, b, preferred_element_type=F32)


def dot3(a, b):
    return dot(a[0], b[0]) + (dot(a[0], b[1]) + dot(a[1], b[0]))


def phase_tables(member, theta_count, phase_ref):
    rows, lons = phase_ref.shape[2], phase_ref.shape[3]
    quarter = lons // 4
    row = lax.broadcasted_iota(jnp.int32, (rows, 2 * quarter), 0)
    lon = lax.broadcasted_iota(jnp.int32, (rows, 2 * quarter), 1)
    theta = math.pi * ((row + member * rows).astype(F32) + 0.5) / theta_count
    phi = 2.0 * math.pi * lon.astype(F32) / lons
    x_arg = REACH * (jnp.sin(theta) * jnp.cos(phi))
    cos_x, sin_x = jnp.cos(x_arg), jnp.sin(x_arg)
    z_arg = REACH * jnp.cos(theta[:, :quarter])
    cz, sz = jnp.cos(z_arg), jnp.sin(z_arg)
    c0, c1 = cos_x[:, :quarter], cos_x[:, quarter:]
    s0, s1 = sin_x[:, :quarter], sin_x[:, quarter:]
    x_parts = ((c0, s0), (c1, s1), (c0, -s0), (c1, -s1))
    for q in range(4):
        ca, sa = x_parts[q]
        cb, sb = x_parts[(q + 3) % 4]
        cc, ss, sc, cs = ca * cb, sa * sb, sa * cb, ca * sb
        lanes = pl.ds(q * quarter, quarter)
        for octant in range(8):
            sgx = 1 - 2 * (octant % 2)
            sgy = 1 - 2 * (octant // 2 % 2)
            sgz = 1 - 2 * (octant // 4)
            re = cc - ss if sgx * sgy > 0 else cc + ss
            im = (sc if sgx > 0 else -sc) + (cs if sgy > 0 else -cs)
            szz = sz if sgz > 0 else -sz
            phase_ref[octant, 0, :, lanes] = re * cz - im * szz
            phase_ref[octant, 1, :, lanes] = re * szz + im * cz


def own_kernel(
    theta_count, width, partners_hbm, op_index_hbm, patterns, operators, out, edge_ops, phase,
    mine, held, partners, op_index, sems, more_sems,
):
    clusters, terms = partners.shape
    rows = out.shape[2]
    tables = [
        pltpu.make_async_copy(op_index_hbm, op_index, more_sems.at[0]),
        pltpu.make_async_copy(partners_hbm, partners, more_sems.at[1]),
        pltpu.make_async_copy(patterns, mine, more_sems.at[2]),
    ]
    for copy in tables:
        copy.start()
    phase_tables(lax.axis_index("member"), theta_count, phase)
    tables[0].wait()
    inner = clusters - 2 * width

    def slot(c):
        return jnp.where(c < width, c, c - inner) * terms

    def fetch_edge(c, p):
        e = slot(c) + p
        return pltpu.make_async_copy(
            operators.at[op_index[c, p]], edge_ops.at[e], sems.at[c * terms + p]
        )

    def fetch_inner(c, p):
        return pltpu.make_async_copy(
            operators.at[op_index[c, p]], held.at[(c - width) * terms + p],
            sems.at[c * terms + p],
        )

    def edge_cluster(n):
        return jnp.where(n < width, n, n + inner)

    @pl.loop(width, clusters - width)
    def _(c):
        for p in range(terms):
            fetch_inner(c, p).start()

    @pl.loop(0, 2 * width)
    def _(n):
        for p in range(terms):
            fetch_edge(edge_cluster(n), p).start()

    base = lax.axis_index("group") * clusters
    tables[1].wait()
    tables[2].wait()

    def translate(c, ops, first):
        for r in range(rows // 8):
            band = pl.ds(r * 8, 8)
            re, im = 0.0, 0.0
            for p in range(terms):
                q = partners[c, p] - base
                keep = jnp.where((q >= 0) & (q < clusters), 1.0, 0.0).astype(F32)
                q = jnp.clip(q, 0, clusters - 1)
                ore, oim = ops[first + p, 0, band, :], ops[first + p, 1, band, :]
                pre, pim = mine[q, 0, band, :] * keep, mine[q, 1, band, :] * keep
                re = re + (ore * pre - oim * pim)
                im = im + (ore * pim + oim * pre)
            out[c, 0, band, :] = re
            out[c, 1, band, :] = im

    @pl.loop(width, clusters - width)
    def _(c):
        for p in range(terms):
            fetch_inner(c, p).wait()
        translate(c, held, (c - width) * terms)

    @pl.loop(0, 2 * width)
    def _(n):
        c = edge_cluster(n)
        for p in range(terms):
            fetch_edge(c, p).wait()
        translate(c, edge_ops, n * terms)


def halo_terms(partners, own, edge_ops, below, above, total):
    clusters, _, rows, _ = own.shape
    terms = partners.shape[1]
    width = below.shape[0]
    base = lax.axis_index("group") * clusters
    total[...] = own[...]

    for n in range(2 * width):
        c = n if n < width else n + clusters - 2 * width
        halo = below if n < width else above
        shift = width - base if n < width else -base - clusters

        @pl.loop(0, terms)
        def _(p):
            q = partners[c, p] - base

            @pl.when((q < 0) | (q >= clusters))
            def _():
                e = n * terms + p
                h = jnp.clip(partners[c, p] + shift, 0, width - 1)
                for r in range(rows // 8):
                    band = pl.ds(r * 8, 8)
                    ore, oim = edge_ops[e, 0, band, :], edge_ops[e, 1, band, :]
                    pre, pim = halo[h, 0, band, :], halo[h, 1, band, :]
                    total[c, 0, band, :] += ore * pre - oim * pim
                    total[c, 1, band, :] += ore * pim + oim * pre


def shift_and_phi(
    order, child_parent, child_octant, total, phase, phi_hi, phi_lo, outs, shifted
):
    clusters, _, rows, _ = total.shape
    base = lax.axis_index("group") * clusters
    chip = lax.axis_index("member") // CORES
    for s, out in zip(order, outs):
        first = (chip ^ s) * out.shape[0]
        for i in range(out.shape[0]):
            q = child_parent[first + i] - base
            o = child_octant[first + i]
            for r in range(rows // 8):
                band = pl.ds(r * 8, 8)
                pre, pim = total[q, 0, band, :], total[q, 1, band, :]
                ere, eim = phase[o, 0, band, :], phase[o, 1, band, :]
                at = i * 2 * rows + r * 8
                shifted[pl.ds(at, 8), :] = pre * ere - pim * eim
                shifted[pl.ds(at + rows, 8), :] = pre * eim + pim * ere
        y = dot3(split(shifted[...]), (phi_hi[...], phi_lo[...]))
        out[...] = y.reshape(out.shape)


def first_kernel(
    order, partners, child_parent, child_octant, own, edge_ops, below, above, phase, phi_hi,
    phi_lo, *rest
):
    outs, (total, shifted) = rest[:-2], rest[-2:]
    halo_terms(partners, own, edge_ops, below, above, total)
    shift_and_phi(
        order, child_parent, child_octant, total, phase, phi_hi, phi_lo, outs, shifted
    )


def later_kernel(order, child_parent, child_octant, total, phase, phi_hi, phi_lo, *rest):
    shift_and_phi(
        order, child_parent, child_octant, total, phase, phi_hi, phi_lo, rest[:-1], rest[-1]
    )


def theta_kernel(away, t_hi, t_lo, *rest):
    blocks, (out, lats) = rest[:-2], rest[-2:]
    member = lax.axis_index("member")
    chip, core = member // CORES, member % CORES
    t = core * CORES + (1 - core if away else core)
    per_chip, _, rows, _ = blocks[0].shape
    for i in range(per_chip):
        for part in range(2):
            for s, block in enumerate(blocks):
                at = pl.multiple_of((chip ^ s) * rows, rows)
                lats[pl.ds(at, rows), :] = block[i, part]
            out[i, part] = dot3((t_hi[t], t_lo[t]), split(lats[...]))


def sum_kernel(keep, arrived, *outs):
    chip = lax.axis_index("member") // CORES
    rows = outs[0].shape[2]
    for s, out in enumerate(outs):
        band = pl.ds(pl.multiple_of((chip ^ s) * rows, rows), rows)
        out[...] = keep[:, :, band, :] + arrived[:, :, band, :]


def place_kernel(*rest):
    blocks, (out, sems) = rest[:-2], rest[-2:]
    chip = lax.axis_index("member") // CORES
    per_chip = blocks[0].shape[0]
    copies = []
    for s, block in enumerate(blocks):
        first = (chip ^ s) * per_chip
        copy = pltpu.make_async_copy(block, out.at[pl.ds(first, per_chip)], sems.at[s])
        copy.start()
        copies.append(copy)
    for copy in copies:
        copy.wait()


def in_hbm(x):
    return pltpu.with_memory_space_constraint(x, pltpu.HBM)


def shape(*dims):
    return jax.ShapeDtypeStruct(dims, F32)


def params(limit):
    return pltpu.CompilerParams(vmem_limit_bytes=limit * MIB)


def call(*args, **kwargs):
    return pl.pallas_call(*args, **kwargs)


def cost(us):
    return pl.CostEstimate(flops=us * 2_000_000, bytes_accessed=0, transcendentals=0)


def on_device(patterns, operators, partners, operator_index, child_parent, child_octant):
    clusters, _, rows, lons = patterns.shape
    members = lax.axis_size("member")
    groups = lax.axis_size("group")
    theta_count = rows * members
    chips = members // CORES
    children = child_parent.shape[0]
    per_chip = children // chips
    out_rows = NTC // members
    width = clusters // 4
    member = lax.axis_index("member")
    chip, core = member // CORES, member % CORES
    terms = partners.shape[1]
    up = [(i, i + 1) for i in range(groups - 1)]
    down = [(i + 1, i) for i in range(groups - 1)]
    below = lax.ppermute(patterns[clusters - width:], "group", up)
    above = lax.ppermute(patterns[:width], "group", down)

    edge = 2 * width * terms
    total_shape = shape(clusters, 2, rows, lons)
    own, edge_ops, phase = pl.pallas_call(
        functools.partial(own_kernel, theta_count, width),
        out_shape=(
            total_shape, shape(edge, 2, rows, lons), shape(8, 2, rows, lons),
        ),
        in_specs=[HBM] * 4,
        out_specs=(VMEM, VMEM, VMEM),
        scratch_shapes=[
            pltpu.VMEM((clusters, 2, rows, lons), F32),
            pltpu.VMEM((clusters * terms - edge, 2, rows, lons), F32),
            pltpu.SMEM((clusters, terms), jnp.int32),
            pltpu.SMEM((clusters, terms), jnp.int32),
            pltpu.SemaphoreType.DMA((clusters * terms,)),
            pltpu.SemaphoreType.DMA((3,)),
        ],
        compiler_params=params(20),
        cost_estimate=cost(8),
    )(in_hbm(partners), in_hbm(operator_index), in_hbm(patterns), in_hbm(operators))

    phi = split_const(phi_table(lons, NPC).T)
    block = shape(per_chip, 2, rows, NPC)
    shifted = pltpu.VMEM((per_chip * 2 * rows, lons), F32)
    far, near = [chips - 1], [*range(1, chips - 1), 0]
    sent = dict.fromkeys(range(chips))
    *outs, total = call(
        functools.partial(first_kernel, far),
        out_shape=(block,) * len(far) + (total_shape,),
        in_specs=[SMEM] * 3 + [VMEM] * 7,
        out_specs=(VMEM,) * (len(far) + 1),
        scratch_shapes=[shifted],
        compiler_params=params(20),
        cost_estimate=cost(2),
    )(
        partners, child_parent, child_octant, own, edge_ops, below, above, phase, *phi
    )
    sent.update(zip(far, outs))
    outs = call(
        functools.partial(later_kernel, near),
        out_shape=(block,) * len(near),
        in_specs=[SMEM] * 2 + [VMEM] * 4,
        out_specs=(VMEM,) * len(near),
        scratch_shapes=[shifted],
        compiler_params=params(20),
        cost_estimate=cost(1),
    )(child_parent, child_octant, total, phase, *phi)
    sent.update(zip(near, outs))

    def between_chips(blocks):
        moved = dict(blocks)
        for s in range(chips - 1, 0, -1):
            pairs = [(i, i ^ (CORES * s)) for i in range(members)]
            moved[s] = lax.ppermute(blocks[s], "member", pairs)
        return [moved[s] for s in range(chips)]

    arrived = between_chips(sent)

    theta = theta_table(theta_count, NTC).reshape(chips, CORES, out_rows, chips, CORES, rows)
    theta = theta.transpose(4, 1, 0, 2, 3, 5).reshape(
        CORES * CORES, chips * out_rows, chips * rows
    )
    swap = [(i, i ^ 1) for i in range(members)]
    if out_rows % 8 == 0:
        half = shape(per_chip, 2, chips * out_rows, NPC)
        away, keep = (
            call(
                functools.partial(theta_kernel, name == "away"),
                out_shape=half,
                in_specs=[VMEM] * (2 + chips),
                out_specs=VMEM,
                scratch_shapes=[pltpu.VMEM((chips * rows, NPC), F32)],
                compiler_params=params(12),
                cost_estimate=cost(1),
            )(*split_const(theta), *arrived)
            for name in ("away", "keep")
        )
        swapped = lax.ppermute(away, "member", swap)
        pieces = call(
            sum_kernel,
            out_shape=(shape(per_chip, 2, out_rows, NPC),) * chips,
            in_specs=[VMEM] * 2,
            out_specs=(VMEM,) * chips,
            compiler_params=params(12),
            cost_estimate=cost(1),
        )(keep, swapped)
    else:
        order = chip ^ jnp.arange(chips)
        lats = jnp.take(jnp.stack(arrived), order, axis=0)
        lats = lats.transpose(1, 2, 0, 3, 4).reshape(per_chip, 2, chips * rows, NPC)
        both = jnp.take(
            jnp.asarray(theta, F32).reshape(CORES, CORES, chips * out_rows, chips * rows),
            core, axis=0,
        )
        sums = jnp.einsum(
            "wjt,kptg->wkpjg", both, lats, precision=lax.Precision.HIGHEST
        )
        moved = lax.ppermute(jnp.take(sums, 1 - core, axis=0), "member", swap)
        pieces = jnp.take(sums, core, axis=0) + moved
        pieces = pieces.reshape(per_chip, 2, chips, out_rows, NPC)
        pieces = [jnp.take(pieces, order[s], axis=2) for s in range(chips)]

    final = between_chips(dict(enumerate(pieces)))
    return call(
        place_kernel,
        out_shape=shape(children, 2, out_rows, NPC),
        in_specs=[VMEM] * chips,
        out_specs=HBM,
        scratch_shapes=[pltpu.SemaphoreType.DMA((chips,))],
        compiler_params=params(12),
        cost_estimate=cost(1),
    )(*final)


def solution(mesh):
    return jax.shard_map(
        on_device,
        mesh=mesh,
        in_specs=(
            P("group", None, "member", None),
            P(None, None, "member", None),
            P("group", None),
            P("group", None),
            P("group"),
            P("group"),
        ),
        out_specs=P("group", None, "member", None),
        check_vma=False,
    )
```

```python
import functools
import math

import jax
import jax.numpy as jnp
import numpy as np
from jax import lax
from jax.experimental import pallas as pl
from jax.experimental.pallas import tpu as pltpu
from jax.sharding import PartitionSpec as P


NTC = 128
NPC = 256
CORES = 2
REACH = 6.0
F32 = jnp.float32
BF16 = jnp.bfloat16
MIB = 1 << 20


VMEM = pl.BlockSpec(memory_space=pltpu.VMEM)
SMEM = pl.BlockSpec(memory_space=pltpu.SMEM)
HBM = pl.BlockSpec(memory_space=pltpu.HBM)


def theta_table(fine, coarse):
    t = math.pi * (np.arange(fine) + 0.5) / fine
    j = math.pi * (np.arange(coarse) + 0.5) / coarse
    m = np.arange(coarse)
    w = np.where(m > 0, 2.0, 1.0)
    return (np.cos(np.outer(j, m)) * w) @ np.cos(np.outer(t, m)).T / fine


def phi_table(fine, coarse):
    f = 2.0 * math.pi * np.arange(fine) / fine
    g = 2.0 * math.pi * np.arange(coarse) / coarse
    m = np.arange(coarse // 2 + 1)
    v = np.where((m > 0) & (m < coarse // 2), 2.0, 1.0)
    cos_part = (np.cos(np.outer(g, m)) * v) @ np.cos(np.outer(f, m)).T
    sin_part = (np.sin(np.outer(g, m)) * v) @ np.sin(np.outer(f, m)).T
    return (cos_part + sin_part) / fine


def split_const(a):
    hi = np.asarray(a, np.float32).astype(BF16)
    lo = (np.asarray(a) - hi.astype(np.float64)).astype(np.float32).astype(BF16)
    return jnp.asarray(hi), jnp.asarray(lo)


def split(x):
    hi = x.astype(BF16)
    return hi, (x - hi.astype(F32)).astype(BF16)


def dot(a, b):
    return jnp.dot(a, b, preferred_element_type=F32)


def dot3(a, b):
    return dot(a[0], b[0]) + (dot(a[0], b[1]) + dot(a[1], b[0]))


def phase_tables(member, theta_count, phase_ref):
    rows, lons = phase_ref.shape[2], phase_ref.shape[3]
    quarter = lons // 4
    row = lax.broadcasted_iota(jnp.int32, (rows, 2 * quarter), 0)
    lon = lax.broadcasted_iota(jnp.int32, (rows, 2 * quarter), 1)
    theta = math.pi * ((row + member * rows).astype(F32) + 0.5) / theta_count
    phi = 2.0 * math.pi * lon.astype(F32) / lons
    x_arg = REACH * (jnp.sin(theta) * jnp.cos(phi))
    cos_x, sin_x = jnp.cos(x_arg), jnp.sin(x_arg)
    z_arg = REACH * jnp.cos(theta[:, :quarter])
    cz, sz = jnp.cos(z_arg), jnp.sin(z_arg)
    c0, c1 = cos_x[:, :quarter], cos_x[:, quarter:]
    s0, s1 = sin_x[:, :quarter], sin_x[:, quarter:]
    x_parts = ((c0, s0), (c1, s1), (c0, -s0), (c1, -s1))
    for q in range(4):
        ca, sa = x_parts[q]
        cb, sb = x_parts[(q + 3) % 4]
        cc, ss, sc, cs = ca * cb, sa * sb, sa * cb, ca * sb
        lanes = pl.ds(q * quarter, quarter)
        for octant in range(8):
            sgx = 1 - 2 * (octant % 2)
            sgy = 1 - 2 * (octant // 2 % 2)
            sgz = 1 - 2 * (octant // 4)
            re = cc - ss if sgx * sgy > 0 else cc + ss
            im = (sc if sgx > 0 else -sc) + (cs if sgy > 0 else -cs)
            szz = sz if sgz > 0 else -sz
            phase_ref[octant, 0, :, lanes] = re * cz - im * szz
            phase_ref[octant, 1, :, lanes] = re * szz + im * cz


def copy_all(pairs, sems):
    copies = [
        pltpu.make_async_copy(source, target, sems.at[n])
        for n, (source, target) in enumerate(pairs)
    ]
    for copy in copies:
        copy.start()
    return copies


def ends_kernel(patterns, partners, op_index, operators, low, high, partners_out, op_out, sems):
    width = low.shape[0]
    last = patterns.shape[0] - width
    pairs = [
        (patterns.at[pl.ds(0, width)], low),
        (patterns.at[pl.ds(last, width)], high),
        (partners, partners_out),
        (op_index, op_out),
    ]
    for copy in copy_all(pairs, sems):
        copy.wait()


def own_kernel(
    theta_count, partners_in, op_in, patterns, operators, out, phase, partners, op_index, sems
):
    clusters, terms = partners.shape
    rows = out.shape[2]
    copies = copy_all([(partners_in, partners), (op_in, op_index)], sems)
    phase_tables(lax.axis_index("member"), theta_count, phase)
    base = lax.axis_index("group") * clusters
    for copy in copies:
        copy.wait()

    @pl.loop(0, clusters)
    def _(c):
        for r in range(rows // 8):
            band = pl.ds(r * 8, 8)
            re, im = 0.0, 0.0
            for p in range(terms):
                q = partners[c, p] - base
                keep = jnp.where((q >= 0) & (q < clusters), 1.0, 0.0).astype(F32)
                q = jnp.clip(q, 0, clusters - 1)
                e = op_index[c, p]
                ore, oim = operators[e, 0, band, :], operators[e, 1, band, :]
                pre, pim = patterns[q, 0, band, :] * keep, patterns[q, 1, band, :] * keep
                re = re + (ore * pre - oim * pim)
                im = im + (ore * pim + oim * pre)
            out[c, 0, band, :] = re
            out[c, 1, band, :] = im


def halo_terms(partners, op_index, own, operators, below, above, total):
    clusters, _, rows, _ = own.shape
    terms = partners.shape[1]
    width = below.shape[0]
    base = lax.axis_index("group") * clusters
    total[...] = own[...]

    for n in range(2 * width):
        c = n if n < width else n + clusters - 2 * width
        halo = below if n < width else above
        shift = width - base if n < width else -base - clusters

        @pl.loop(0, terms)
        def _(p):
            q = partners[c, p] - base

            @pl.when((q < 0) | (q >= clusters))
            def _():
                e = op_index[c, p]
                h = jnp.clip(partners[c, p] + shift, 0, width - 1)
                for r in range(rows // 8):
                    band = pl.ds(r * 8, 8)
                    ore, oim = operators[e, 0, band, :], operators[e, 1, band, :]
                    pre, pim = halo[h, 0, band, :], halo[h, 1, band, :]
                    total[c, 0, band, :] += ore * pre - oim * pim
                    total[c, 1, band, :] += ore * pim + oim * pre


def shift_and_phi(
    order, child_parent, child_octant, total, phase, phi_hi, phi_lo, outs, shifted
):
    clusters, _, rows, _ = total.shape
    base = lax.axis_index("group") * clusters
    chip = lax.axis_index("member") // CORES
    for s, out in zip(order, outs):
        first = (chip ^ s) * out.shape[0]
        for i in range(out.shape[0]):
            q = child_parent[first + i] - base
            o = child_octant[first + i]
            for r in range(rows // 8):
                band = pl.ds(r * 8, 8)
                pre, pim = total[q, 0, band, :], total[q, 1, band, :]
                ere, eim = phase[o, 0, band, :], phase[o, 1, band, :]
                at = i * 2 * rows + r * 8
                shifted[pl.ds(at, 8), :] = pre * ere - pim * eim
                shifted[pl.ds(at + rows, 8), :] = pre * eim + pim * ere
        y = dot3(split(shifted[...]), (phi_hi[...], phi_lo[...]))
        out[...] = y.reshape(out.shape)


def first_kernel(
    order, partners, op_index, child_parent, child_octant, own, operators, below, above, phase,
    phi_hi, phi_lo, *rest
):
    outs, (total, shifted) = rest[:-2], rest[-2:]
    halo_terms(partners, op_index, own, operators, below, above, total)
    shift_and_phi(
        order, child_parent, child_octant, total, phase, phi_hi, phi_lo, outs, shifted
    )


def later_kernel(order, child_parent, child_octant, total, phase, phi_hi, phi_lo, *rest):
    shift_and_phi(
        order, child_parent, child_octant, total, phase, phi_hi, phi_lo, rest[:-1], rest[-1]
    )


def theta_kernel(away, t_hi, t_lo, *rest):
    blocks, (out, lats) = rest[:-2], rest[-2:]
    member = lax.axis_index("member")
    chip, core = member // CORES, member % CORES
    t = core * CORES + (1 - core if away else core)
    per_chip, _, rows, _ = blocks[0].shape
    for i in range(per_chip):
        for part in range(2):
            for s, block in enumerate(blocks):
                at = pl.multiple_of((chip ^ s) * rows, rows)
                lats[pl.ds(at, rows), :] = block[i, part]
            out[i, part] = dot3((t_hi[t], t_lo[t]), split(lats[...]))


def sum_kernel(keep, arrived, *outs):
    chip = lax.axis_index("member") // CORES
    rows = outs[0].shape[2]
    for s, out in enumerate(outs):
        band = pl.ds(pl.multiple_of((chip ^ s) * rows, rows), rows)
        out[...] = keep[:, :, band, :] + arrived[:, :, band, :]


def place_kernel(*rest):
    blocks, (out, sems) = rest[:-2], rest[-2:]
    chip = lax.axis_index("member") // CORES
    per_chip = blocks[0].shape[0]
    copies = []
    for s, block in enumerate(blocks):
        first = (chip ^ s) * per_chip
        copy = pltpu.make_async_copy(block, out.at[pl.ds(first, per_chip)], sems.at[s])
        copy.start()
        copies.append(copy)
    for copy in copies:
        copy.wait()


def in_hbm(x):
    return pltpu.with_memory_space_constraint(x, pltpu.HBM)


def shape(*dims):
    return jax.ShapeDtypeStruct(dims, F32)


def params(limit):
    return pltpu.CompilerParams(vmem_limit_bytes=limit * MIB)


def call(*args, **kwargs):
    return pl.pallas_call(*args, **kwargs)


def cost(us):
    return pl.CostEstimate(flops=us * 2_000_000, bytes_accessed=us * 3_000_000, transcendentals=0)


def on_device(patterns, operators, partners, operator_index, child_parent, child_octant):
    clusters, _, rows, lons = patterns.shape
    members = lax.axis_size("member")
    groups = lax.axis_size("group")
    theta_count = rows * members
    chips = members // CORES
    children = child_parent.shape[0]
    per_chip = children // chips
    out_rows = NTC // members
    width = clusters // 4
    member = lax.axis_index("member")
    chip, core = member // CORES, member % CORES
    up = [(i, i + 1) for i in range(groups - 1)]
    down = [(i + 1, i) for i in range(groups - 1)]
    end = shape(width, 2, rows, lons)
    index = jax.ShapeDtypeStruct(partners.shape, jnp.int32)
    low, high, partners, operator_index = pl.pallas_call(
        ends_kernel,
        out_shape=(end, end, index, index),
        in_specs=[HBM] * 4,
        out_specs=(VMEM,) * 4,
        scratch_shapes=[pltpu.SemaphoreType.DMA((4,))],
        compiler_params=params(4),
    )(*map(in_hbm, (patterns, partners, operator_index, operators)))
    below = lax.ppermute(high, "group", up)
    above = lax.ppermute(low, "group", down)

    total_shape = shape(clusters, 2, rows, lons)
    own, phase = pl.pallas_call(
        functools.partial(own_kernel, theta_count),
        out_shape=(total_shape, shape(8, 2, rows, lons)),
        in_specs=[VMEM] * 4,
        out_specs=(VMEM, VMEM),
        scratch_shapes=[
            pltpu.SMEM(partners.shape, jnp.int32),
            pltpu.SMEM(partners.shape, jnp.int32),
            pltpu.SemaphoreType.DMA((2,)),
        ],
        compiler_params=params(20),
        cost_estimate=cost(8),
    )(partners, operator_index, patterns, operators)

    phi = split_const(phi_table(lons, NPC).T)
    block = shape(per_chip, 2, rows, NPC)
    shifted = pltpu.VMEM((per_chip * 2 * rows, lons), F32)
    far, near = [chips - 1], [*range(1, chips - 1), 0]
    sent = dict.fromkeys(range(chips))
    *outs, total = call(
        functools.partial(first_kernel, far),
        out_shape=(block,) * len(far) + (total_shape,),
        in_specs=[SMEM] * 4 + [VMEM] * 7,
        out_specs=(VMEM,) * (len(far) + 1),
        scratch_shapes=[shifted],
        compiler_params=params(20),
        cost_estimate=cost(2),
    )(
        partners, operator_index, child_parent, child_octant, own, operators, below, above,
        phase, *phi,
    )
    sent.update(zip(far, outs))
    outs = call(
        functools.partial(later_kernel, near),
        out_shape=(block,) * len(near),
        in_specs=[SMEM] * 2 + [VMEM] * 4,
        out_specs=(VMEM,) * len(near),
        scratch_shapes=[shifted],
        compiler_params=params(20),
        cost_estimate=cost(1),
    )(child_parent, child_octant, total, phase, *phi)
    sent.update(zip(near, outs))

    def between_chips(blocks):
        moved = dict(blocks)
        for s in range(chips - 1, 0, -1):
            pairs = [(i, i ^ (CORES * s)) for i in range(members)]
            moved[s] = lax.ppermute(blocks[s], "member", pairs)
        return [moved[s] for s in range(chips)]

    arrived = between_chips(sent)

    theta = theta_table(theta_count, NTC).reshape(chips, CORES, out_rows, chips, CORES, rows)
    theta = theta.transpose(4, 1, 0, 2, 3, 5).reshape(
        CORES * CORES, chips * out_rows, chips * rows
    )
    swap = [(i, i ^ 1) for i in range(members)]
    if out_rows % 8 == 0:
        half = shape(per_chip, 2, chips * out_rows, NPC)
        away, keep = (
            call(
                functools.partial(theta_kernel, name == "away"),
                out_shape=half,
                in_specs=[VMEM] * (2 + chips),
                out_specs=VMEM,
                scratch_shapes=[pltpu.VMEM((chips * rows, NPC), F32)],
                compiler_params=params(12),
                cost_estimate=cost(1),
            )(*split_const(theta), *arrived)
            for name in ("away", "keep")
        )
        swapped = lax.ppermute(away, "member", swap)
        pieces = call(
            sum_kernel,
            out_shape=(shape(per_chip, 2, out_rows, NPC),) * chips,
            in_specs=[VMEM] * 2,
            out_specs=(VMEM,) * chips,
            compiler_params=params(12),
            cost_estimate=cost(1),
        )(keep, swapped)
    else:
        order = chip ^ jnp.arange(chips)
        lats = jnp.take(jnp.stack(arrived), order, axis=0)
        lats = lats.transpose(1, 2, 0, 3, 4).reshape(per_chip, 2, chips * rows, NPC)
        both = jnp.take(
            jnp.asarray(theta, F32).reshape(CORES, CORES, chips * out_rows, chips * rows),
            core, axis=0,
        )
        sums = jnp.einsum(
            "wjt,kptg->wkpjg", both, lats, precision=lax.Precision.HIGHEST
        )
        moved = lax.ppermute(jnp.take(sums, 1 - core, axis=0), "member", swap)
        pieces = jnp.take(sums, core, axis=0) + moved
        pieces = pieces.reshape(per_chip, 2, chips, out_rows, NPC)
        pieces = [jnp.take(pieces, order[s], axis=2) for s in range(chips)]

    final = between_chips(dict(enumerate(pieces)))
    return call(
        place_kernel,
        out_shape=shape(children, 2, out_rows, NPC),
        in_specs=[VMEM] * chips,
        out_specs=HBM,
        scratch_shapes=[pltpu.SemaphoreType.DMA((chips,))],
        compiler_params=params(12),
        cost_estimate=cost(1),
    )(*final)


def solution(mesh):
    return jax.shard_map(
        on_device,
        mesh=mesh,
        in_specs=(
            P("group", None, "member", None),
            P(None, None, "member", None),
            P("group", None),
            P("group", None),
            P("group"),
            P("group"),
        ),
        out_specs=P("group", None, "member", None),
        check_vma=False,
    )
```

```python
import functools
import math

import jax
import jax.numpy as jnp
import numpy as np
from jax import lax
from jax.experimental import pallas as pl
from jax.experimental.pallas import tpu as pltpu
from jax.sharding import PartitionSpec as P


NTC = 128
NPC = 256
CORES = 2
REACH = 6.0
F32 = jnp.float32
BF16 = jnp.bfloat16
MIB = 1 << 20


VMEM = pl.BlockSpec(memory_space=pltpu.VMEM)
SMEM = pl.BlockSpec(memory_space=pltpu.SMEM)
HBM = pl.BlockSpec(memory_space=pltpu.HBM)


def theta_table(fine, coarse):
    t = math.pi * (np.arange(fine) + 0.5) / fine
    j = math.pi * (np.arange(coarse) + 0.5) / coarse
    m = np.arange(coarse)
    w = np.where(m > 0, 2.0, 1.0)
    return (np.cos(np.outer(j, m)) * w) @ np.cos(np.outer(t, m)).T / fine


def phi_table(fine, coarse):
    f = 2.0 * math.pi * np.arange(fine) / fine
    g = 2.0 * math.pi * np.arange(coarse) / coarse
    m = np.arange(coarse // 2 + 1)
    v = np.where((m > 0) & (m < coarse // 2), 2.0, 1.0)
    cos_part = (np.cos(np.outer(g, m)) * v) @ np.cos(np.outer(f, m)).T
    sin_part = (np.sin(np.outer(g, m)) * v) @ np.sin(np.outer(f, m)).T
    return (cos_part + sin_part) / fine


def split_const(a):
    hi = np.asarray(a, np.float32).astype(BF16)
    lo = (np.asarray(a) - hi.astype(np.float64)).astype(np.float32).astype(BF16)
    return jnp.asarray(hi), jnp.asarray(lo)


def split(x):
    hi = x.astype(BF16)
    return hi, (x - hi.astype(F32)).astype(BF16)


def dot(a, b):
    return jnp.dot(a, b, preferred_element_type=F32)


def dot3(a, b):
    return dot(a[0], b[0]) + (dot(a[0], b[1]) + dot(a[1], b[0]))


def phase_tables(member, theta_count, phase_ref):
    rows, lons = phase_ref.shape[2], phase_ref.shape[3]
    quarter = lons // 4
    row = lax.broadcasted_iota(jnp.int32, (rows, 2 * quarter), 0)
    lon = lax.broadcasted_iota(jnp.int32, (rows, 2 * quarter), 1)
    theta = math.pi * ((row + member * rows).astype(F32) + 0.5) / theta_count
    phi = 2.0 * math.pi * lon.astype(F32) / lons
    x_arg = REACH * (jnp.sin(theta) * jnp.cos(phi))
    cos_x, sin_x = jnp.cos(x_arg), jnp.sin(x_arg)
    z_arg = REACH * jnp.cos(theta[:, :quarter])
    cz, sz = jnp.cos(z_arg), jnp.sin(z_arg)
    c0, c1 = cos_x[:, :quarter], cos_x[:, quarter:]
    s0, s1 = sin_x[:, :quarter], sin_x[:, quarter:]
    x_parts = ((c0, s0), (c1, s1), (c0, -s0), (c1, -s1))
    for q in range(4):
        ca, sa = x_parts[q]
        cb, sb = x_parts[(q + 3) % 4]
        cc, ss, sc, cs = ca * cb, sa * sb, sa * cb, ca * sb
        lanes = pl.ds(q * quarter, quarter)
        for octant in range(8):
            sgx = 1 - 2 * (octant % 2)
            sgy = 1 - 2 * (octant // 2 % 2)
            sgz = 1 - 2 * (octant // 4)
            re = cc - ss if sgx * sgy > 0 else cc + ss
            im = (sc if sgx > 0 else -sc) + (cs if sgy > 0 else -cs)
            szz = sz if sgz > 0 else -sz
            phase_ref[octant, 0, :, lanes] = re * cz - im * szz
            phase_ref[octant, 1, :, lanes] = re * szz + im * cz


def copy_all(pairs, sems):
    copies = [
        pltpu.make_async_copy(source, target, sems.at[n])
        for n, (source, target) in enumerate(pairs)
    ]
    for copy in copies:
        copy.start()
    return copies


def ends_kernel(
    patterns, partners, op_index, operators, first, second, partners_out, op_out, sems
):
    width = first.shape[0]
    last = patterns.shape[0] - width
    odd = lax.axis_index("group") % 2
    pairs = [
        (patterns.at[pl.ds((1 - odd) * last, width)], first),
        (patterns.at[pl.ds(odd * last, width)], second),
        (partners, partners_out),
        (op_index, op_out),
    ]
    for copy in copy_all(pairs, sems):
        copy.wait()


def own_kernel(
    theta_count, partners_in, op_in, patterns, operators, out, phase, partners, op_index, sems
):
    clusters, terms = partners.shape
    rows = out.shape[2]
    copies = copy_all([(partners_in, partners), (op_in, op_index)], sems)
    phase_tables(lax.axis_index("member"), theta_count, phase)
    base = lax.axis_index("group") * clusters
    for copy in copies:
        copy.wait()

    @pl.loop(0, clusters)
    def _(c):
        for r in range(rows // 8):
            band = pl.ds(r * 8, 8)
            re, im = 0.0, 0.0
            for p in range(terms):
                q = partners[c, p] - base
                keep = jnp.where((q >= 0) & (q < clusters), 1.0, 0.0).astype(F32)
                q = jnp.clip(q, 0, clusters - 1)
                e = op_index[c, p]
                ore, oim = operators[e, 0, band, :], operators[e, 1, band, :]
                pre, pim = patterns[q, 0, band, :] * keep, patterns[q, 1, band, :] * keep
                re = re + (ore * pre - oim * pim)
                im = im + (ore * pim + oim * pre)
            out[c, 0, band, :] = re
            out[c, 1, band, :] = im


def halo_terms(partners, op_index, own, operators, first, second, total):
    clusters, _, rows, _ = own.shape
    terms = partners.shape[1]
    width = first.shape[0]
    group = lax.axis_index("group")
    base = group * clusters
    total[...] = own[...]

    def add(n, halo, shift):
        c = n if n < width else n + clusters - 2 * width

        @pl.loop(0, terms)
        def _(p):
            q = partners[c, p] - base

            @pl.when((q < 0) | (q >= clusters))
            def _():
                e = op_index[c, p]
                h = jnp.clip(q + shift, 0, width - 1)
                for r in range(rows // 8):
                    band = pl.ds(r * 8, 8)
                    ore, oim = operators[e, 0, band, :], operators[e, 1, band, :]
                    pre, pim = halo[h, 0, band, :], halo[h, 1, band, :]
                    total[c, 0, band, :] += ore * pre - oim * pim
                    total[c, 1, band, :] += ore * pim + oim * pre

    for odd, below, above in ((0, second, first), (1, first, second)):

        @pl.when(group % 2 == odd)
        def _():
            for n in range(2 * width):
                if n < width:
                    add(n, below, width)
                else:
                    add(n, above, -clusters)


def shift_and_phi(
    order, child_parent, child_octant, total, phase, phi_hi, phi_lo, outs, shifted
):
    clusters, _, rows, _ = total.shape
    base = lax.axis_index("group") * clusters
    chip = lax.axis_index("member") // CORES
    for s, out in zip(order, outs):
        first = (chip ^ s) * out.shape[0]
        for i in range(out.shape[0]):
            q = child_parent[first + i] - base
            o = child_octant[first + i]
            for r in range(rows // 8):
                band = pl.ds(r * 8, 8)
                pre, pim = total[q, 0, band, :], total[q, 1, band, :]
                ere, eim = phase[o, 0, band, :], phase[o, 1, band, :]
                at = i * 2 * rows + r * 8
                shifted[pl.ds(at, 8), :] = pre * ere - pim * eim
                shifted[pl.ds(at + rows, 8), :] = pre * eim + pim * ere
        y = dot3(split(shifted[...]), (phi_hi[...], phi_lo[...]))
        out[...] = y.reshape(out.shape)


def first_kernel(
    order, partners, op_index, child_parent, child_octant, own, operators, first, second, phase,
    phi_hi, phi_lo, *rest
):
    outs, (total, shifted) = rest[:-2], rest[-2:]
    halo_terms(partners, op_index, own, operators, first, second, total)
    shift_and_phi(
        order, child_parent, child_octant, total, phase, phi_hi, phi_lo, outs, shifted
    )


def later_kernel(order, child_parent, child_octant, total, phase, phi_hi, phi_lo, *rest):
    shift_and_phi(
        order, child_parent, child_octant, total, phase, phi_hi, phi_lo, rest[:-1], rest[-1]
    )


def theta_kernel(away, t_hi, t_lo, *rest):
    blocks, (out, lats) = rest[:-2], rest[-2:]
    member = lax.axis_index("member")
    chip, core = member // CORES, member % CORES
    t = core * CORES + (1 - core if away else core)
    per_chip, _, rows, _ = blocks[0].shape
    for i in range(per_chip):
        for part in range(2):
            for s, block in enumerate(blocks):
                at = pl.multiple_of((chip ^ s) * rows, rows)
                lats[pl.ds(at, rows), :] = block[i, part]
            out[i, part] = dot3((t_hi[t], t_lo[t]), split(lats[...]))


def sum_kernel(keep, arrived, *outs):
    chip = lax.axis_index("member") // CORES
    rows = outs[0].shape[2]
    for s, out in enumerate(outs):
        band = pl.ds(pl.multiple_of((chip ^ s) * rows, rows), rows)
        out[...] = keep[:, :, band, :] + arrived[:, :, band, :]


def place_kernel(*rest):
    blocks, (out, sems) = rest[:-2], rest[-2:]
    chip = lax.axis_index("member") // CORES
    per_chip = blocks[0].shape[0]
    copies = []
    for s, block in enumerate(blocks):
        first = (chip ^ s) * per_chip
        copy = pltpu.make_async_copy(block, out.at[pl.ds(first, per_chip)], sems.at[s])
        copy.start()
        copies.append(copy)
    for copy in copies:
        copy.wait()


def in_hbm(x):
    return pltpu.with_memory_space_constraint(x, pltpu.HBM)


def shape(*dims):
    return jax.ShapeDtypeStruct(dims, F32)


def params(limit):
    return pltpu.CompilerParams(vmem_limit_bytes=limit * MIB)


def call(*args, **kwargs):
    return pl.pallas_call(*args, **kwargs)


def cost(us):
    return pl.CostEstimate(flops=us * 2_000_000, bytes_accessed=us * 3_000_000, transcendentals=0)


def on_device(patterns, operators, partners, operator_index, child_parent, child_octant):
    clusters, _, rows, lons = patterns.shape
    members = lax.axis_size("member")
    groups = lax.axis_size("group")
    theta_count = rows * members
    chips = members // CORES
    children = child_parent.shape[0]
    per_chip = children // chips
    out_rows = NTC // members
    width = clusters // 4
    member = lax.axis_index("member")
    chip, core = member // CORES, member % CORES
    end = shape(width, 2, rows, lons)
    index = jax.ShapeDtypeStruct(partners.shape, jnp.int32)
    first, second, partners, operator_index = pl.pallas_call(
        ends_kernel,
        out_shape=(end, end, index, index),
        in_specs=[HBM] * 4,
        out_specs=(VMEM,) * 4,
        scratch_shapes=[pltpu.SemaphoreType.DMA((4,))],
        compiler_params=params(4),
    )(*map(in_hbm, (patterns, partners, operator_index, operators)))
    pairs = [[(i, i + 1) for i in range(start, groups - 1, 2)] for start in range(2)]
    pairs = [both + [(j, i) for i, j in both] for both in pairs]
    first = lax.ppermute(first, "group", pairs[0])
    second = lax.ppermute(second, "group", pairs[1])

    total_shape = shape(clusters, 2, rows, lons)
    own, phase = pl.pallas_call(
        functools.partial(own_kernel, theta_count),
        out_shape=(total_shape, shape(8, 2, rows, lons)),
        in_specs=[VMEM] * 4,
        out_specs=(VMEM, VMEM),
        scratch_shapes=[
            pltpu.SMEM(partners.shape, jnp.int32),
            pltpu.SMEM(partners.shape, jnp.int32),
            pltpu.SemaphoreType.DMA((2,)),
        ],
        compiler_params=params(20),
        cost_estimate=cost(8),
    )(partners, operator_index, patterns, operators)

    phi = split_const(phi_table(lons, NPC).T)
    block = shape(per_chip, 2, rows, NPC)
    shifted = pltpu.VMEM((per_chip * 2 * rows, lons), F32)
    far, near = [chips - 1], [*range(1, chips - 1), 0]
    sent = dict.fromkeys(range(chips))
    *outs, total = call(
        functools.partial(first_kernel, far),
        out_shape=(block,) * len(far) + (total_shape,),
        in_specs=[SMEM] * 4 + [VMEM] * 7,
        out_specs=(VMEM,) * (len(far) + 1),
        scratch_shapes=[shifted],
        compiler_params=params(20),
        cost_estimate=cost(2),
    )(
        partners, operator_index, child_parent, child_octant, own, operators, first, second,
        phase, *phi,
    )
    sent.update(zip(far, outs))
    outs = call(
        functools.partial(later_kernel, near),
        out_shape=(block,) * len(near),
        in_specs=[SMEM] * 2 + [VMEM] * 4,
        out_specs=(VMEM,) * len(near),
        scratch_shapes=[shifted],
        compiler_params=params(20),
        cost_estimate=cost(1),
    )(child_parent, child_octant, total, phase, *phi)
    sent.update(zip(near, outs))

    def between_chips(blocks):
        moved = dict(blocks)
        for s in range(chips - 1, 0, -1):
            pairs = [(i, i ^ (CORES * s)) for i in range(members)]
            moved[s] = lax.ppermute(blocks[s], "member", pairs)
        return [moved[s] for s in range(chips)]

    arrived = between_chips(sent)

    theta = theta_table(theta_count, NTC).reshape(chips, CORES, out_rows, chips, CORES, rows)
    theta = theta.transpose(4, 1, 0, 2, 3, 5).reshape(
        CORES * CORES, chips * out_rows, chips * rows
    )
    swap = [(i, i ^ 1) for i in range(members)]
    if out_rows % 8 == 0:
        half = shape(per_chip, 2, chips * out_rows, NPC)
        away, keep = (
            call(
                functools.partial(theta_kernel, name == "away"),
                out_shape=half,
                in_specs=[VMEM] * (2 + chips),
                out_specs=VMEM,
                scratch_shapes=[pltpu.VMEM((chips * rows, NPC), F32)],
                compiler_params=params(12),
                cost_estimate=cost(1),
            )(*split_const(theta), *arrived)
            for name in ("away", "keep")
        )
        swapped = lax.ppermute(away, "member", swap)
        pieces = call(
            sum_kernel,
            out_shape=(shape(per_chip, 2, out_rows, NPC),) * chips,
            in_specs=[VMEM] * 2,
            out_specs=(VMEM,) * chips,
            compiler_params=params(12),
            cost_estimate=cost(1),
        )(keep, swapped)
    else:
        order = chip ^ jnp.arange(chips)
        lats = jnp.take(jnp.stack(arrived), order, axis=0)
        lats = lats.transpose(1, 2, 0, 3, 4).reshape(per_chip, 2, chips * rows, NPC)
        both = jnp.take(
            jnp.asarray(theta, F32).reshape(CORES, CORES, chips * out_rows, chips * rows),
            core, axis=0,
        )
        sums = jnp.einsum(
            "wjt,kptg->wkpjg", both, lats, precision=lax.Precision.HIGHEST
        )
        moved = lax.ppermute(jnp.take(sums, 1 - core, axis=0), "member", swap)
        pieces = jnp.take(sums, core, axis=0) + moved
        pieces = pieces.reshape(per_chip, 2, chips, out_rows, NPC)
        pieces = [jnp.take(pieces, order[s], axis=2) for s in range(chips)]

    final = between_chips(dict(enumerate(pieces)))
    return call(
        place_kernel,
        out_shape=shape(children, 2, out_rows, NPC),
        in_specs=[VMEM] * chips,
        out_specs=HBM,
        scratch_shapes=[pltpu.SemaphoreType.DMA((chips,))],
        compiler_params=params(12),
        cost_estimate=cost(1),
    )(*final)


def solution(mesh):
    return jax.shard_map(
        on_device,
        mesh=mesh,
        in_specs=(
            P("group", None, "member", None),
            P(None, None, "member", None),
            P("group", None),
            P("group", None),
            P("group"),
            P("group"),
        ),
        out_specs=P("group", None, "member", None),
        check_vma=False,
    )
```

```python
import functools
import math

import jax
import jax.numpy as jnp
import numpy as np
from jax import lax
from jax.experimental import pallas as pl
from jax.experimental.pallas import tpu as pltpu
from jax.sharding import PartitionSpec as P


NTC = 128
NPC = 256
CORES = 2
ROUNDS = 3
REACH = 6.0
F32 = jnp.float32
BF16 = jnp.bfloat16
MIB = 1 << 20


VMEM = pl.BlockSpec(memory_space=pltpu.VMEM)
SMEM = pl.BlockSpec(memory_space=pltpu.SMEM)
HBM = pl.BlockSpec(memory_space=pltpu.HBM)


def theta_table(fine, coarse):
    t = math.pi * (np.arange(fine) + 0.5) / fine
    j = math.pi * (np.arange(coarse) + 0.5) / coarse
    m = np.arange(coarse)
    w = np.where(m > 0, 2.0, 1.0)
    return (np.cos(np.outer(j, m)) * w) @ np.cos(np.outer(t, m)).T / fine


def phi_table(fine, coarse):
    f = 2.0 * math.pi * np.arange(fine) / fine
    g = 2.0 * math.pi * np.arange(coarse) / coarse
    m = np.arange(coarse // 2 + 1)
    v = np.where((m > 0) & (m < coarse // 2), 2.0, 1.0)
    cos_part = (np.cos(np.outer(g, m)) * v) @ np.cos(np.outer(f, m)).T
    sin_part = (np.sin(np.outer(g, m)) * v) @ np.sin(np.outer(f, m)).T
    return (cos_part + sin_part) / fine


def split_const(a):
    hi = np.asarray(a, np.float32).astype(BF16)
    lo = (np.asarray(a) - hi.astype(np.float64)).astype(np.float32).astype(BF16)
    return jnp.asarray(hi), jnp.asarray(lo)


def split(x):
    hi = x.astype(BF16)
    return hi, (x - hi.astype(F32)).astype(BF16)


def dot(a, b):
    return jnp.dot(a, b, preferred_element_type=F32)


def dot3(a, b):
    return dot(a[0], b[0]) + (dot(a[0], b[1]) + dot(a[1], b[0]))


def phase_tables(member, theta_count, phase_ref):
    rows, lons = phase_ref.shape[2], phase_ref.shape[3]
    quarter = lons // 4
    row = lax.broadcasted_iota(jnp.int32, (rows, 2 * quarter), 0)
    lon = lax.broadcasted_iota(jnp.int32, (rows, 2 * quarter), 1)
    theta = math.pi * ((row + member * rows).astype(F32) + 0.5) / theta_count
    phi = 2.0 * math.pi * lon.astype(F32) / lons
    x_arg = REACH * (jnp.sin(theta) * jnp.cos(phi))
    cos_x, sin_x = jnp.cos(x_arg), jnp.sin(x_arg)
    z_arg = REACH * jnp.cos(theta[:, :quarter])
    cz, sz = jnp.cos(z_arg), jnp.sin(z_arg)
    c0, c1 = cos_x[:, :quarter], cos_x[:, quarter:]
    s0, s1 = sin_x[:, :quarter], sin_x[:, quarter:]
    x_parts = ((c0, s0), (c1, s1), (c0, -s0), (c1, -s1))
    for q in range(4):
        ca, sa = x_parts[q]
        cb, sb = x_parts[(q + 3) % 4]
        cc, ss, sc, cs = ca * cb, sa * sb, sa * cb, ca * sb
        lanes = pl.ds(q * quarter, quarter)
        for octant in range(8):
            sgx = 1 - 2 * (octant % 2)
            sgy = 1 - 2 * (octant // 2 % 2)
            sgz = 1 - 2 * (octant // 4)
            re = cc - ss if sgx * sgy > 0 else cc + ss
            im = (sc if sgx > 0 else -sc) + (cs if sgy > 0 else -cs)
            szz = sz if sgz > 0 else -sz
            phase_ref[octant, 0, :, lanes] = re * cz - im * szz
            phase_ref[octant, 1, :, lanes] = re * szz + im * cz


def copy_all(pairs, sems):
    copies = [
        pltpu.make_async_copy(source, target, sems.at[n])
        for n, (source, target) in enumerate(pairs)
    ]
    for copy in copies:
        copy.start()
    return copies


def ends_kernel(patterns, partners, op_index, operators, *rest):
    *ends, partners_out, op_out, sems = rest
    width = ends[0].shape[0]
    last = patterns.shape[0] - width
    upper = lax.axis_index("group") % ROUNDS
    pairs = [(partners, partners_out), (op_index, op_out)]
    for n, end in enumerate(ends):
        pairs.append((patterns.at[pl.ds(jnp.where(upper == n, last, 0), width)], end))
    for copy in copy_all(pairs, sems):
        copy.wait()


def own_kernel(
    theta_count, partners_in, op_in, patterns, operators, out, phase, partners, op_index, sems
):
    clusters, terms = partners.shape
    rows = out.shape[2]
    copies = copy_all([(partners_in, partners), (op_in, op_index)], sems)
    phase_tables(lax.axis_index("member"), theta_count, phase)
    base = lax.axis_index("group") * clusters
    for copy in copies:
        copy.wait()

    @pl.loop(0, clusters)
    def _(c):
        for r in range(rows // 8):
            band = pl.ds(r * 8, 8)
            re, im = 0.0, 0.0
            for p in range(terms):
                q = partners[c, p] - base
                keep = jnp.where((q >= 0) & (q < clusters), 1.0, 0.0).astype(F32)
                q = jnp.clip(q, 0, clusters - 1)
                e = op_index[c, p]
                ore, oim = operators[e, 0, band, :], operators[e, 1, band, :]
                pre, pim = patterns[q, 0, band, :] * keep, patterns[q, 1, band, :] * keep
                re = re + (ore * pre - oim * pim)
                im = im + (ore * pim + oim * pre)
            out[c, 0, band, :] = re
            out[c, 1, band, :] = im


def halo_terms(partners, op_index, own, operators, halos, total):
    clusters, _, rows, _ = own.shape
    terms = partners.shape[1]
    width = halos[0].shape[0]
    group = lax.axis_index("group")
    base = group * clusters
    total[...] = own[...]

    def add(n, halo, shift):
        c = n if n < width else n + clusters - 2 * width

        @pl.loop(0, terms)
        def _(p):
            q = partners[c, p] - base

            @pl.when((q < 0) | (q >= clusters))
            def _():
                e = op_index[c, p]
                h = jnp.clip(q + shift, 0, width - 1)
                for r in range(rows // 8):
                    band = pl.ds(r * 8, 8)
                    ore, oim = operators[e, 0, band, :], operators[e, 1, band, :]
                    pre, pim = halo[h, 0, band, :], halo[h, 1, band, :]
                    total[c, 0, band, :] += ore * pre - oim * pim
                    total[c, 1, band, :] += ore * pim + oim * pre

    for turn in range(ROUNDS):
        below, above = halos[turn - 1], halos[turn]

        @pl.when(group % ROUNDS == turn)
        def _():
            for n in range(2 * width):
                if n < width:
                    add(n, below, width)
                else:
                    add(n, above, -clusters)


def shift_and_phi(
    order, child_parent, child_octant, total, phase, phi_hi, phi_lo, outs, shifted
):
    clusters, _, rows, _ = total.shape
    base = lax.axis_index("group") * clusters
    chip = lax.axis_index("member") // CORES
    for s, out in zip(order, outs):
        first = (chip ^ s) * out.shape[0]
        for i in range(out.shape[0]):
            q = child_parent[first + i] - base
            o = child_octant[first + i]
            for r in range(rows // 8):
                band = pl.ds(r * 8, 8)
                pre, pim = total[q, 0, band, :], total[q, 1, band, :]
                ere, eim = phase[o, 0, band, :], phase[o, 1, band, :]
                at = i * 2 * rows + r * 8
                shifted[pl.ds(at, 8), :] = pre * ere - pim * eim
                shifted[pl.ds(at + rows, 8), :] = pre * eim + pim * ere
        y = dot3(split(shifted[...]), (phi_hi[...], phi_lo[...]))
        out[...] = y.reshape(out.shape)


def first_kernel(
    order, partners, op_index, child_parent, child_octant, own, operators, phase, phi_hi, phi_lo, *rest
):
    halos, outs, (total, shifted) = rest[:ROUNDS], rest[ROUNDS:-2], rest[-2:]
    halo_terms(partners, op_index, own, operators, halos, total)
    shift_and_phi(
        order, child_parent, child_octant, total, phase, phi_hi, phi_lo, outs, shifted
    )


def later_kernel(order, child_parent, child_octant, total, phase, phi_hi, phi_lo, *rest):
    shift_and_phi(
        order, child_parent, child_octant, total, phase, phi_hi, phi_lo, rest[:-1], rest[-1]
    )


def theta_kernel(away, t_hi, t_lo, *rest):
    blocks, (out, lats) = rest[:-2], rest[-2:]
    member = lax.axis_index("member")
    chip, core = member // CORES, member % CORES
    t = core * CORES + (1 - core if away else core)
    per_chip, _, rows, _ = blocks[0].shape
    for i in range(per_chip):
        for part in range(2):
            for s, block in enumerate(blocks):
                at = pl.multiple_of((chip ^ s) * rows, rows)
                lats[pl.ds(at, rows), :] = block[i, part]
            out[i, part] = dot3((t_hi[t], t_lo[t]), split(lats[...]))


def sum_kernel(keep, arrived, *outs):
    chip = lax.axis_index("member") // CORES
    rows = outs[0].shape[2]
    for s, out in enumerate(outs):
        band = pl.ds(pl.multiple_of((chip ^ s) * rows, rows), rows)
        out[...] = keep[:, :, band, :] + arrived[:, :, band, :]


def place_kernel(*rest):
    blocks, (out, sems) = rest[:-2], rest[-2:]
    chip = lax.axis_index("member") // CORES
    per_chip = blocks[0].shape[0]
    copies = []
    for s, block in enumerate(blocks):
        first = (chip ^ s) * per_chip
        copy = pltpu.make_async_copy(block, out.at[pl.ds(first, per_chip)], sems.at[s])
        copy.start()
        copies.append(copy)
    for copy in copies:
        copy.wait()


def in_hbm(x):
    return pltpu.with_memory_space_constraint(x, pltpu.HBM)


def shape(*dims):
    return jax.ShapeDtypeStruct(dims, F32)


def params(limit):
    return pltpu.CompilerParams(vmem_limit_bytes=limit * MIB)


def call(*args, **kwargs):
    return pl.pallas_call(*args, **kwargs)


def cost(us):
    return pl.CostEstimate(flops=us * 2_000_000, bytes_accessed=us * 3_000_000, transcendentals=0)


def on_device(patterns, operators, partners, operator_index, child_parent, child_octant):
    clusters, _, rows, lons = patterns.shape
    members = lax.axis_size("member")
    groups = lax.axis_size("group")
    theta_count = rows * members
    chips = members // CORES
    children = child_parent.shape[0]
    per_chip = children // chips
    out_rows = NTC // members
    width = clusters // 4
    member = lax.axis_index("member")
    chip, core = member // CORES, member % CORES
    end = shape(width, 2, rows, lons)
    index = jax.ShapeDtypeStruct(partners.shape, jnp.int32)
    *halos, partners, operator_index = pl.pallas_call(
        ends_kernel,
        out_shape=(end,) * ROUNDS + (index, index),
        in_specs=[HBM] * 4,
        out_specs=(VMEM,) * (ROUNDS + 2),
        scratch_shapes=[pltpu.SemaphoreType.DMA((ROUNDS + 2,))],
        compiler_params=params(4),
    )(*map(in_hbm, (patterns, partners, operator_index, operators)))
    for n in range(ROUNDS):
        both = [(i, i + 1) for i in range(n, groups - 1, ROUNDS)]
        halos[n] = lax.ppermute(halos[n], "group", both + [(j, i) for i, j in both])

    total_shape = shape(clusters, 2, rows, lons)
    own, phase = pl.pallas_call(
        functools.partial(own_kernel, theta_count),
        out_shape=(total_shape, shape(8, 2, rows, lons)),
        in_specs=[VMEM] * 4,
        out_specs=(VMEM, VMEM),
        scratch_shapes=[
            pltpu.SMEM(partners.shape, jnp.int32),
            pltpu.SMEM(partners.shape, jnp.int32),
            pltpu.SemaphoreType.DMA((2,)),
        ],
        compiler_params=params(20),
        cost_estimate=cost(8),
    )(partners, operator_index, patterns, operators)

    phi = split_const(phi_table(lons, NPC).T)
    block = shape(per_chip, 2, rows, NPC)
    shifted = pltpu.VMEM((per_chip * 2 * rows, lons), F32)
    far, near = [chips - 1], [*range(1, chips - 1), 0]
    sent = dict.fromkeys(range(chips))
    *outs, total = call(
        functools.partial(first_kernel, far),
        out_shape=(block,) * len(far) + (total_shape,),
        in_specs=[SMEM] * 4 + [VMEM] * (5 + ROUNDS),
        out_specs=(VMEM,) * (len(far) + 1),
        scratch_shapes=[shifted],
        compiler_params=params(20),
        cost_estimate=cost(2),
    )(
        partners, operator_index, child_parent, child_octant, own, operators,
        phase, *phi, *halos,
    )
    sent.update(zip(far, outs))
    outs = call(
        functools.partial(later_kernel, near),
        out_shape=(block,) * len(near),
        in_specs=[SMEM] * 2 + [VMEM] * 4,
        out_specs=(VMEM,) * len(near),
        scratch_shapes=[shifted],
        compiler_params=params(20),
        cost_estimate=cost(1),
    )(child_parent, child_octant, total, phase, *phi)
    sent.update(zip(near, outs))

    def between_chips(blocks):
        moved = dict(blocks)
        for s in range(chips - 1, 0, -1):
            pairs = [(i, i ^ (CORES * s)) for i in range(members)]
            moved[s] = lax.ppermute(blocks[s], "member", pairs)
        return [moved[s] for s in range(chips)]

    arrived = between_chips(sent)

    theta = theta_table(theta_count, NTC).reshape(chips, CORES, out_rows, chips, CORES, rows)
    theta = theta.transpose(4, 1, 0, 2, 3, 5).reshape(
        CORES * CORES, chips * out_rows, chips * rows
    )
    swap = [(i, i ^ 1) for i in range(members)]
    if out_rows % 8 == 0:
        half = shape(per_chip, 2, chips * out_rows, NPC)
        away, keep = (
            call(
                functools.partial(theta_kernel, name == "away"),
                out_shape=half,
                in_specs=[VMEM] * (2 + chips),
                out_specs=VMEM,
                scratch_shapes=[pltpu.VMEM((chips * rows, NPC), F32)],
                compiler_params=params(12),
                cost_estimate=cost(1),
            )(*split_const(theta), *arrived)
            for name in ("away", "keep")
        )
        swapped = lax.ppermute(away, "member", swap)
        pieces = call(
            sum_kernel,
            out_shape=(shape(per_chip, 2, out_rows, NPC),) * chips,
            in_specs=[VMEM] * 2,
            out_specs=(VMEM,) * chips,
            compiler_params=params(12),
            cost_estimate=cost(1),
        )(keep, swapped)
    else:
        order = chip ^ jnp.arange(chips)
        lats = jnp.take(jnp.stack(arrived), order, axis=0)
        lats = lats.transpose(1, 2, 0, 3, 4).reshape(per_chip, 2, chips * rows, NPC)
        both = jnp.take(
            jnp.asarray(theta, F32).reshape(CORES, CORES, chips * out_rows, chips * rows),
            core, axis=0,
        )
        sums = jnp.einsum(
            "wjt,kptg->wkpjg", both, lats, precision=lax.Precision.HIGHEST
        )
        moved = lax.ppermute(jnp.take(sums, 1 - core, axis=0), "member", swap)
        pieces = jnp.take(sums, core, axis=0) + moved
        pieces = pieces.reshape(per_chip, 2, chips, out_rows, NPC)
        pieces = [jnp.take(pieces, order[s], axis=2) for s in range(chips)]

    final = between_chips(dict(enumerate(pieces)))
    return call(
        place_kernel,
        out_shape=shape(children, 2, out_rows, NPC),
        in_specs=[VMEM] * chips,
        out_specs=HBM,
        scratch_shapes=[pltpu.SemaphoreType.DMA((chips,))],
        compiler_params=params(12),
        cost_estimate=cost(1),
    )(*final)


def solution(mesh):
    return jax.shard_map(
        on_device,
        mesh=mesh,
        in_specs=(
            P("group", None, "member", None),
            P(None, None, "member", None),
            P("group", None),
            P("group", None),
            P("group"),
            P("group"),
        ),
        out_specs=P("group", None, "member", None),
        check_vma=False,
    )
```

```python
import functools
import math

import jax
import jax.numpy as jnp
import numpy as np
from jax import lax
from jax.experimental import pallas as pl
from jax.experimental.pallas import tpu as pltpu
from jax.sharding import PartitionSpec as P


NTC = 128
NPC = 256
CORES = 2
REACH = 6.0
F32 = jnp.float32
BF16 = jnp.bfloat16
MIB = 1 << 20


VMEM = pl.BlockSpec(memory_space=pltpu.VMEM)
SMEM = pl.BlockSpec(memory_space=pltpu.SMEM)
HBM = pl.BlockSpec(memory_space=pltpu.HBM)


def theta_table(fine, coarse):
    t = math.pi * (np.arange(fine) + 0.5) / fine
    j = math.pi * (np.arange(coarse) + 0.5) / coarse
    m = np.arange(coarse)
    w = np.where(m > 0, 2.0, 1.0)
    return (np.cos(np.outer(j, m)) * w) @ np.cos(np.outer(t, m)).T / fine


def phi_table(fine, coarse):
    f = 2.0 * math.pi * np.arange(fine) / fine
    g = 2.0 * math.pi * np.arange(coarse) / coarse
    m = np.arange(coarse // 2 + 1)
    v = np.where((m > 0) & (m < coarse // 2), 2.0, 1.0)
    cos_part = (np.cos(np.outer(g, m)) * v) @ np.cos(np.outer(f, m)).T
    sin_part = (np.sin(np.outer(g, m)) * v) @ np.sin(np.outer(f, m)).T
    return (cos_part + sin_part) / fine


def split_const(a):
    hi = np.asarray(a, np.float32).astype(BF16)
    lo = (np.asarray(a) - hi.astype(np.float64)).astype(np.float32).astype(BF16)
    return jnp.asarray(hi), jnp.asarray(lo)


def split(x):
    hi = x.astype(BF16)
    return hi, (x - hi.astype(F32)).astype(BF16)


def dot(a, b):
    return jnp.dot(a, b, preferred_element_type=F32)


def dot3(a, b):
    return dot(a[0], b[0]) + (dot(a[0], b[1]) + dot(a[1], b[0]))


def phase_tables(member, theta_count, phase_ref):
    rows, lons = phase_ref.shape[2], phase_ref.shape[3]
    quarter = lons // 4
    row = lax.broadcasted_iota(jnp.int32, (rows, 2 * quarter), 0)
    lon = lax.broadcasted_iota(jnp.int32, (rows, 2 * quarter), 1)
    theta = math.pi * ((row + member * rows).astype(F32) + 0.5) / theta_count
    phi = 2.0 * math.pi * lon.astype(F32) / lons
    x_arg = REACH * (jnp.sin(theta) * jnp.cos(phi))
    cos_x, sin_x = jnp.cos(x_arg), jnp.sin(x_arg)
    z_arg = REACH * jnp.cos(theta[:, :quarter])
    cz, sz = jnp.cos(z_arg), jnp.sin(z_arg)
    c0, c1 = cos_x[:, :quarter], cos_x[:, quarter:]
    s0, s1 = sin_x[:, :quarter], sin_x[:, quarter:]
    x_parts = ((c0, s0), (c1, s1), (c0, -s0), (c1, -s1))
    for q in range(4):
        ca, sa = x_parts[q]
        cb, sb = x_parts[(q + 3) % 4]
        cc, ss, sc, cs = ca * cb, sa * sb, sa * cb, ca * sb
        lanes = pl.ds(q * quarter, quarter)
        for octant in range(8):
            sgx = 1 - 2 * (octant % 2)
            sgy = 1 - 2 * (octant // 2 % 2)
            sgz = 1 - 2 * (octant // 4)
            re = cc - ss if sgx * sgy > 0 else cc + ss
            im = (sc if sgx > 0 else -sc) + (cs if sgy > 0 else -cs)
            szz = sz if sgz > 0 else -sz
            phase_ref[octant, 0, :, lanes] = re * cz - im * szz
            phase_ref[octant, 1, :, lanes] = re * szz + im * cz


def copy_all(pairs, sems):
    copies = [
        pltpu.make_async_copy(source, target, sems.at[n])
        for n, (source, target) in enumerate(pairs)
    ]
    for copy in copies:
        copy.start()
    return copies


def ends_kernel(
    patterns, partners, op_index, operators, first, second, partners_out, op_out, sems
):
    width = first.shape[0]
    last = patterns.shape[0] - width
    odd = lax.axis_index("group") % 2
    pairs = [
        (patterns.at[pl.ds((1 - odd) * last, width)], first),
        (patterns.at[pl.ds(odd * last, width)], second),
        (partners, partners_out),
        (op_index, op_out),
    ]
    for copy in copy_all(pairs, sems):
        copy.wait()


def own_kernel(
    theta_count, partners_in, op_in, patterns, operators, out, phase, partners, op_index, sems
):
    clusters, terms = partners.shape
    rows = out.shape[2]
    copies = copy_all([(partners_in, partners), (op_in, op_index)], sems)
    phase_tables(lax.axis_index("member"), theta_count, phase)
    base = lax.axis_index("group") * clusters
    for copy in copies:
        copy.wait()

    @pl.loop(0, clusters)
    def _(c):
        for r in range(rows // 8):
            band = pl.ds(r * 8, 8)
            re, im = 0.0, 0.0
            for p in range(terms):
                q = partners[c, p] - base
                keep = jnp.where((q >= 0) & (q < clusters), 1.0, 0.0).astype(F32)
                q = jnp.clip(q, 0, clusters - 1)
                e = op_index[c, p]
                ore, oim = operators[e, 0, band, :], operators[e, 1, band, :]
                pre, pim = patterns[q, 0, band, :] * keep, patterns[q, 1, band, :] * keep
                re = re + (ore * pre - oim * pim)
                im = im + (ore * pim + oim * pre)
            out[c, 0, band, :] = re
            out[c, 1, band, :] = im


def halo_terms(partners, op_index, own, operators, first, second, total):
    clusters, _, rows, _ = own.shape
    terms = partners.shape[1]
    width = first.shape[0]
    group = lax.axis_index("group")
    base = group * clusters
    total[...] = own[...]

    def add(n, halo, shift):
        c = n if n < width else n + clusters - 2 * width

        @pl.loop(0, terms)
        def _(p):
            q = partners[c, p] - base

            @pl.when((q < 0) | (q >= clusters))
            def _():
                e = op_index[c, p]
                h = jnp.clip(q + shift, 0, width - 1)
                for r in range(rows // 8):
                    band = pl.ds(r * 8, 8)
                    ore, oim = operators[e, 0, band, :], operators[e, 1, band, :]
                    pre, pim = halo[h, 0, band, :], halo[h, 1, band, :]
                    total[c, 0, band, :] += ore * pre - oim * pim
                    total[c, 1, band, :] += ore * pim + oim * pre

    for odd, below, above in ((0, second, first), (1, first, second)):

        @pl.when(group % 2 == odd)
        def _():
            for n in range(2 * width):
                if n < width:
                    add(n, below, width)
                else:
                    add(n, above, -clusters)


def fill_slots(child_parent, slots, clusters, width, chips):
    base = lax.axis_index("group") * clusters

    def place_child(k, counts):
        early, late = counts
        q = child_parent[k] - base
        inner = (q >= width) & (q < clusters - width) & (early < chips)
        slots[jnp.where(inner, early, late)] = k
        step = jnp.where(inner, 1, 0)
        return early + step, late + 1 - step

    lax.fori_loop(0, slots.shape[0], place_child, (jnp.int32(0), jnp.int32(chips)))


def slot_of(chip, i, chips, per_chip):
    return jnp.where(i == 0, chip, chips + chip * (per_chip - 1) + i - 1)


def shift_and_phi(
    order, first, slots, child_parent, child_octant, total, phase, phi_hi, phi_lo, outs, shifted
):
    clusters, _, rows, _ = total.shape
    chips = lax.axis_size("member") // CORES
    per_chip = slots.shape[0] // chips
    base = lax.axis_index("group") * clusters
    chip = lax.axis_index("member") // CORES
    count = outs[0].shape[0]
    size = count * 2 * rows
    group = shifted.shape[0] // size
    for start in range(0, len(order), group):
        part = list(zip(order, outs))[start:start + group]
        for m, (s, _) in enumerate(part):
            for i in range(count):
                k = slots[slot_of(chip ^ s, first + i, chips, per_chip)]
                q = child_parent[k] - base
                o = child_octant[k]
                for r in range(rows // 8):
                    band = pl.ds(r * 8, 8)
                    pre, pim = total[q, 0, band, :], total[q, 1, band, :]
                    ere, eim = phase[o, 0, band, :], phase[o, 1, band, :]
                    at = m * size + i * 2 * rows + r * 8
                    shifted[pl.ds(at, 8), :] = pre * ere - pim * eim
                    shifted[pl.ds(at + rows, 8), :] = pre * eim + pim * ere
        y = dot3(split(shifted[...]), (phi_hi[...], phi_lo[...]))
        for m, (_, out) in enumerate(part):
            out[...] = y[m * size:(m + 1) * size].reshape(out.shape)


def early_kernel(width, child_parent, child_octant, own, phase, phi_hi, phi_lo, *rest):
    *outs, slots, shifted = rest
    fill_slots(child_parent, slots, own.shape[0], width, len(outs))
    shift_and_phi(
        range(len(outs)), 0, slots, child_parent, child_octant, own, phase, phi_hi, phi_lo,
        outs, shifted,
    )


def first_kernel(
    order, partners, op_index, child_parent, child_octant, own, operators, first, second, phase,
    phi_hi, phi_lo, *rest
):
    *outs, total, slots, shifted = rest
    chips = lax.axis_size("member") // CORES
    fill_slots(child_parent, slots, own.shape[0], first.shape[0], chips)
    halo_terms(partners, op_index, own, operators, first, second, total)
    shift_and_phi(
        order, 1, slots, child_parent, child_octant, total, phase, phi_hi, phi_lo, outs, shifted
    )


def later_kernel(
    order, width, child_parent, child_octant, total, phase, phi_hi, phi_lo, *rest
):
    *outs, slots, shifted = rest
    fill_slots(child_parent, slots, total.shape[0], width, len(outs) + 1)
    shift_and_phi(
        order, 1, slots, child_parent, child_octant, total, phase, phi_hi, phi_lo, outs, shifted
    )


def theta_kernel(away, t_hi, t_lo, *rest):
    *blocks, out, lats = rest
    chips = len(blocks) // 2
    early, late = blocks[:chips], blocks[chips:]
    member = lax.axis_index("member")
    chip, core = member // CORES, member % CORES
    t = core * CORES + (1 - core if away else core)
    rows = early[0].shape[2]
    for i in range(out.shape[0]):
        for part in range(2):
            for s in range(chips):
                at = pl.multiple_of((chip ^ s) * rows, rows)
                block = early[s][0, part] if i == 0 else late[s][i - 1, part]
                lats[pl.ds(at, rows), :] = block
            out[i, part] = dot3((t_hi[t], t_lo[t]), split(lats[...]))


def sum_kernel(keep, arrived, *outs):
    chip = lax.axis_index("member") // CORES
    rows = outs[0].shape[2]
    for s, out in enumerate(outs):
        band = pl.ds(pl.multiple_of((chip ^ s) * rows, rows), rows)
        out[...] = keep[:, :, band, :] + arrived[:, :, band, :]


def place_kernel(clusters, width, child_parent, *rest):
    *blocks, out, slots, sems = rest
    chips, per_chip = len(blocks), blocks[0].shape[0]
    chip = lax.axis_index("member") // CORES
    fill_slots(child_parent, slots, clusters, width, chips)
    pairs = [
        (block.at[i], out.at[slots[slot_of(chip ^ s, i, chips, per_chip)]])
        for s, block in enumerate(blocks)
        for i in range(per_chip)
    ]
    for copy in copy_all(pairs, sems):
        copy.wait()


def in_hbm(x):
    return pltpu.with_memory_space_constraint(x, pltpu.HBM)


def shape(*dims):
    return jax.ShapeDtypeStruct(dims, F32)


def params(limit):
    return pltpu.CompilerParams(vmem_limit_bytes=limit * MIB)


def call(*args, **kwargs):
    return pl.pallas_call(*args, **kwargs)


def cost(us):
    return pl.CostEstimate(flops=us * 2_000_000, bytes_accessed=us * 3_000_000, transcendentals=0)


def on_device(patterns, operators, partners, operator_index, child_parent, child_octant):
    clusters, _, rows, lons = patterns.shape
    members = lax.axis_size("member")
    groups = lax.axis_size("group")
    theta_count = rows * members
    chips = members // CORES
    children = child_parent.shape[0]
    per_chip = children // chips
    out_rows = NTC // members
    width = clusters // 4
    member = lax.axis_index("member")
    chip, core = member // CORES, member % CORES
    end = shape(width, 2, rows, lons)
    index = jax.ShapeDtypeStruct(partners.shape, jnp.int32)
    first, second, partners, operator_index = pl.pallas_call(
        ends_kernel,
        out_shape=(end, end, index, index),
        in_specs=[HBM] * 4,
        out_specs=(VMEM,) * 4,
        scratch_shapes=[pltpu.SemaphoreType.DMA((4,))],
        compiler_params=params(4),
    )(*map(in_hbm, (patterns, partners, operator_index, operators)))
    pairs = [[(i, i + 1) for i in range(start, groups - 1, 2)] for start in range(2)]
    pairs = [both + [(j, i) for i, j in both] for both in pairs]
    first = lax.ppermute(first, "group", pairs[0])
    second = lax.ppermute(second, "group", pairs[1])

    total_shape = shape(clusters, 2, rows, lons)
    own, phase = pl.pallas_call(
        functools.partial(own_kernel, theta_count),
        out_shape=(total_shape, shape(8, 2, rows, lons)),
        in_specs=[VMEM] * 4,
        out_specs=(VMEM, VMEM),
        scratch_shapes=[
            pltpu.SMEM(partners.shape, jnp.int32),
            pltpu.SMEM(partners.shape, jnp.int32),
            pltpu.SemaphoreType.DMA((2,)),
        ],
        compiler_params=params(20),
        cost_estimate=cost(8),
    )(partners, operator_index, patterns, operators)

    phi = split_const(phi_table(lons, NPC).T)
    assert per_chip > 1 and clusters - 2 * width >= chips
    slots = pltpu.SMEM((children,), jnp.int32)

    def blocks_of(count, number):
        return (shape(count, 2, rows, NPC),) * number

    def rows_of(count):
        return pltpu.VMEM((count * 2 * rows, lons), F32)

    def between_chips(blocks):
        moved = dict(blocks)
        for s in range(chips - 1, 0, -1):
            pairs = [(i, i ^ (CORES * s)) for i in range(members)]
            moved[s] = lax.ppermute(blocks[s], "member", pairs)
        return [moved[s] for s in range(chips)]

    early = call(
        functools.partial(early_kernel, width),
        out_shape=blocks_of(1, chips),
        in_specs=[SMEM] * 2 + [VMEM] * 4,
        out_specs=(VMEM,) * chips,
        scratch_shapes=[slots, rows_of(chips)],
        compiler_params=params(20),
        cost_estimate=cost(1),
    )(child_parent, child_octant, own, phase, *phi)
    early = between_chips(dict(enumerate(early)))

    count = per_chip - 1
    far, near = [chips - 1], [*range(1, chips - 1), 0]
    late = {}
    *outs, total = call(
        functools.partial(first_kernel, far),
        out_shape=blocks_of(count, len(far)) + (total_shape,),
        in_specs=[SMEM] * 4 + [VMEM] * 7,
        out_specs=(VMEM,) * (len(far) + 1),
        scratch_shapes=[slots, rows_of(count)],
        compiler_params=params(20),
        cost_estimate=cost(2),
    )(
        partners, operator_index, child_parent, child_octant, own, operators, first, second,
        phase, *phi,
    )
    late.update(zip(far, outs))
    outs = call(
        functools.partial(later_kernel, near, width),
        out_shape=blocks_of(count, len(near)),
        in_specs=[SMEM] * 2 + [VMEM] * 4,
        out_specs=(VMEM,) * len(near),
        scratch_shapes=[slots, rows_of(count)],
        compiler_params=params(20),
        cost_estimate=cost(1),
    )(child_parent, child_octant, total, phase, *phi)
    late.update(zip(near, outs))
    late = between_chips(late)

    theta = theta_table(theta_count, NTC).reshape(chips, CORES, out_rows, chips, CORES, rows)
    theta = theta.transpose(4, 1, 0, 2, 3, 5).reshape(
        CORES * CORES, chips * out_rows, chips * rows
    )
    swap = [(i, i ^ 1) for i in range(members)]
    if out_rows % 8 == 0:
        half = shape(per_chip, 2, chips * out_rows, NPC)
        away, keep = (
            call(
                functools.partial(theta_kernel, name == "away"),
                out_shape=half,
                in_specs=[VMEM] * (2 + 2 * chips),
                out_specs=VMEM,
                scratch_shapes=[pltpu.VMEM((chips * rows, NPC), F32)],
                compiler_params=params(12),
                cost_estimate=cost(1),
            )(*split_const(theta), *early, *late)
            for name in ("away", "keep")
        )
        swapped = lax.ppermute(away, "member", swap)
        pieces = call(
            sum_kernel,
            out_shape=(shape(per_chip, 2, out_rows, NPC),) * chips,
            in_specs=[VMEM] * 2,
            out_specs=(VMEM,) * chips,
            compiler_params=params(12),
            cost_estimate=cost(1),
        )(keep, swapped)
    else:
        order = chip ^ jnp.arange(chips)
        lats = jnp.stack([jnp.concatenate(pair) for pair in zip(early, late)])
        lats = jnp.take(lats, order, axis=0)
        lats = lats.transpose(1, 2, 0, 3, 4).reshape(per_chip, 2, chips * rows, NPC)
        both = jnp.take(
            jnp.asarray(theta, F32).reshape(CORES, CORES, chips * out_rows, chips * rows),
            core, axis=0,
        )
        sums = jnp.einsum(
            "wjt,kptg->wkpjg", both, lats, precision=lax.Precision.HIGHEST
        )
        moved = lax.ppermute(jnp.take(sums, 1 - core, axis=0), "member", swap)
        pieces = jnp.take(sums, core, axis=0) + moved
        pieces = pieces.reshape(per_chip, 2, chips, out_rows, NPC)
        pieces = [jnp.take(pieces, order[s], axis=2) for s in range(chips)]

    final = between_chips(dict(enumerate(pieces)))
    return call(
        functools.partial(place_kernel, clusters, width),
        out_shape=shape(children, 2, out_rows, NPC),
        in_specs=[SMEM] + [VMEM] * chips,
        out_specs=HBM,
        scratch_shapes=[slots, pltpu.SemaphoreType.DMA((children,))],
        compiler_params=params(12),
        cost_estimate=cost(1),
    )(child_parent, *final)


def solution(mesh):
    return jax.shard_map(
        on_device,
        mesh=mesh,
        in_specs=(
            P("group", None, "member", None),
            P(None, None, "member", None),
            P("group", None),
            P("group", None),
            P("group"),
            P("group"),
        ),
        out_specs=P("group", None, "member", None),
        check_vma=False,
    )
```

```python
import functools
import math

import jax
import jax.numpy as jnp
import numpy as np
from jax import lax
from jax.experimental import pallas as pl
from jax.experimental.pallas import tpu as pltpu
from jax.sharding import PartitionSpec as P


NTC = 128
NPC = 256
CORES = 2
REACH = 6.0
F32 = jnp.float32
BF16 = jnp.bfloat16
MIB = 1 << 20


VMEM = pl.BlockSpec(memory_space=pltpu.VMEM)
SMEM = pl.BlockSpec(memory_space=pltpu.SMEM)
HBM = pl.BlockSpec(memory_space=pltpu.HBM)


def theta_table(fine, coarse):
    t = math.pi * (np.arange(fine) + 0.5) / fine
    j = math.pi * (np.arange(coarse) + 0.5) / coarse
    m = np.arange(coarse)
    w = np.where(m > 0, 2.0, 1.0)
    return (np.cos(np.outer(j, m)) * w) @ np.cos(np.outer(t, m)).T / fine


def phi_table(fine, coarse):
    f = 2.0 * math.pi * np.arange(fine) / fine
    g = 2.0 * math.pi * np.arange(coarse) / coarse
    m = np.arange(coarse // 2 + 1)
    v = np.where((m > 0) & (m < coarse // 2), 2.0, 1.0)
    cos_part = (np.cos(np.outer(g, m)) * v) @ np.cos(np.outer(f, m)).T
    sin_part = (np.sin(np.outer(g, m)) * v) @ np.sin(np.outer(f, m)).T
    return (cos_part + sin_part) / fine


def split_const(a):
    hi = np.asarray(a, np.float32).astype(BF16)
    lo = (np.asarray(a) - hi.astype(np.float64)).astype(np.float32).astype(BF16)
    return jnp.asarray(hi), jnp.asarray(lo)


def split(x):
    hi = x.astype(BF16)
    return hi, (x - hi.astype(F32)).astype(BF16)


def dot(a, b):
    return jnp.dot(a, b, preferred_element_type=F32)


def dot3(a, b):
    return dot(a[0], b[0]) + (dot(a[0], b[1]) + dot(a[1], b[0]))


def phase_tables(member, theta_count, phase_ref):
    rows, lons = phase_ref.shape[2], phase_ref.shape[3]
    quarter = lons // 4
    row = lax.broadcasted_iota(jnp.int32, (rows, 2 * quarter), 0)
    lon = lax.broadcasted_iota(jnp.int32, (rows, 2 * quarter), 1)
    theta = math.pi * ((row + member * rows).astype(F32) + 0.5) / theta_count
    phi = 2.0 * math.pi * lon.astype(F32) / lons
    x_arg = REACH * (jnp.sin(theta) * jnp.cos(phi))
    cos_x, sin_x = jnp.cos(x_arg), jnp.sin(x_arg)
    z_arg = REACH * jnp.cos(theta[:, :quarter])
    cz, sz = jnp.cos(z_arg), jnp.sin(z_arg)
    c0, c1 = cos_x[:, :quarter], cos_x[:, quarter:]
    s0, s1 = sin_x[:, :quarter], sin_x[:, quarter:]
    x_parts = ((c0, s0), (c1, s1), (c0, -s0), (c1, -s1))
    for q in range(4):
        ca, sa = x_parts[q]
        cb, sb = x_parts[(q + 3) % 4]
        cc, ss, sc, cs = ca * cb, sa * sb, sa * cb, ca * sb
        lanes = pl.ds(q * quarter, quarter)
        for octant in range(8):
            sgx = 1 - 2 * (octant % 2)
            sgy = 1 - 2 * (octant // 2 % 2)
            sgz = 1 - 2 * (octant // 4)
            re = cc - ss if sgx * sgy > 0 else cc + ss
            im = (sc if sgx > 0 else -sc) + (cs if sgy > 0 else -cs)
            szz = sz if sgz > 0 else -sz
            phase_ref[octant, 0, :, lanes] = re * cz - im * szz
            phase_ref[octant, 1, :, lanes] = re * szz + im * cz


def copy_all(pairs, sems):
    copies = [
        pltpu.make_async_copy(source, target, sems.at[n])
        for n, (source, target) in enumerate(pairs)
    ]
    for copy in copies:
        copy.start()
    return copies


def ends_kernel(
    patterns, partners, op_index, operators, first, second, partners_out, op_out, sems
):
    width = first.shape[0]
    last = patterns.shape[0] - width
    odd = lax.axis_index("group") % 2
    pairs = [
        (patterns.at[pl.ds((1 - odd) * last, width)], first),
        (patterns.at[pl.ds(odd * last, width)], second),
        (partners, partners_out),
        (op_index, op_out),
    ]
    for copy in copy_all(pairs, sems):
        copy.wait()


def halo_terms(partners, op_index, own, operators, first, second, total):
    clusters, _, rows, _ = own.shape
    terms = partners.shape[1]
    width = first.shape[0]
    group = lax.axis_index("group")
    base = group * clusters
    total[...] = own[...]

    def add(n, halo, shift):
        c = n if n < width else n + clusters - 2 * width

        @pl.loop(0, terms)
        def _(p):
            q = partners[c, p] - base

            @pl.when((q < 0) | (q >= clusters))
            def _():
                e = op_index[c, p]
                h = jnp.clip(q + shift, 0, width - 1)
                for r in range(rows // 8):
                    band = pl.ds(r * 8, 8)
                    ore, oim = operators[e, 0, band, :], operators[e, 1, band, :]
                    pre, pim = halo[h, 0, band, :], halo[h, 1, band, :]
                    total[c, 0, band, :] += ore * pre - oim * pim
                    total[c, 1, band, :] += ore * pim + oim * pre

    for odd, below, above in ((0, second, first), (1, first, second)):

        @pl.when(group % 2 == odd)
        def _():
            for n in range(2 * width):
                if n < width:
                    add(n, below, width)
                else:
                    add(n, above, -clusters)


def fill_slots(child_parent, slots, clusters, width, chips):
    base = lax.axis_index("group") * clusters

    early, late = jnp.int32(0), jnp.int32(chips)
    for k in range(slots.shape[0]):
        q = child_parent[k] - base
        inner = (q >= width) & (q < clusters - width) & (early < chips)
        slots[jnp.where(inner, early, late)] = k
        step = jnp.where(inner, 1, 0)
        early, late = early + step, late + 1 - step


def slot_of(chip, i, chips, per_chip):
    return chip if i == 0 else chips + chip * (per_chip - 1) + i - 1


def shift_and_phi(
    order, first, slots, child_parent, child_octant, total, phase, phi_hi, phi_lo, outs, shifted
):
    clusters, _, rows, _ = total.shape
    chips = lax.axis_size("member") // CORES
    per_chip = slots.shape[0] // chips
    base = lax.axis_index("group") * clusters
    chip = lax.axis_index("member") // CORES
    count = outs[0].shape[0]
    size = count * 2 * rows
    group = shifted.shape[0] // size
    for start in range(0, len(order), group):
        part = list(zip(order, outs))[start:start + group]
        for m, (s, _) in enumerate(part):
            for i in range(count):
                k = slots[slot_of(chip ^ s, first + i, chips, per_chip)]
                q = child_parent[k] - base
                o = child_octant[k]
                for r in range(rows // 8):
                    band = pl.ds(r * 8, 8)
                    pre, pim = total[q, 0, band, :], total[q, 1, band, :]
                    ere, eim = phase[o, 0, band, :], phase[o, 1, band, :]
                    at = m * size + i * 2 * rows + r * 8
                    shifted[pl.ds(at, 8), :] = pre * ere - pim * eim
                    shifted[pl.ds(at + rows, 8), :] = pre * eim + pim * ere
        used = pl.ds(0, len(part) * size)
        y = dot3(split(shifted[used, :]), (phi_hi[...], phi_lo[...]))
        for m, (_, out) in enumerate(part):
            out[...] = y[m * size:(m + 1) * size].reshape(out.shape)


def first_kernel(
    order, partners, op_index, child_parent, child_octant, own, operators, first, second, phase,
    phi_hi, phi_lo, *rest
):
    *outs, total, slots, shifted = rest
    chips = lax.axis_size("member") // CORES
    fill_slots(child_parent, slots, own.shape[0], first.shape[0], chips)
    halo_terms(partners, op_index, own, operators, first, second, total)
    shift_and_phi(
        order, 1, slots, child_parent, child_octant, total, phase, phi_hi, phi_lo, outs, shifted
    )


def later_kernel(
    order, first, width, child_parent, child_octant, total, phase, phi_hi, phi_lo, *rest
):
    *outs, slots, shifted = rest
    chips = lax.axis_size("member") // CORES
    fill_slots(child_parent, slots, total.shape[0], width, chips)
    shift_and_phi(
        order, first, slots, child_parent, child_octant, total, phase, phi_hi, phi_lo, outs,
        shifted,
    )


def own_kernel(
    theta_count, width, partners_in, op_in, parent_in, octant_in, patterns, operators, phi_hi,
    phi_lo, out, phase, *rest
):
    *early, partners, op_index, child_parent, child_octant, slots, shifted, sems = rest
    clusters, terms = partners.shape
    rows = out.shape[2]
    copies = copy_all(
        [
            (partners_in, partners),
            (op_in, op_index),
            (parent_in, child_parent),
            (octant_in, child_octant),
        ],
        sems,
    )
    phase_tables(lax.axis_index("member"), theta_count, phase)
    base = lax.axis_index("group") * clusters
    for copy in copies:
        copy.wait()

    @pl.loop(0, clusters)
    def _(c):
        for r in range(rows // 8):
            band = pl.ds(r * 8, 8)
            re, im = 0.0, 0.0
            for p in range(terms):
                q = partners[c, p] - base
                keep = jnp.where((q >= 0) & (q < clusters), 1.0, 0.0).astype(F32)
                q = jnp.clip(q, 0, clusters - 1)
                e = op_index[c, p]
                ore, oim = operators[e, 0, band, :], operators[e, 1, band, :]
                pre, pim = patterns[q, 0, band, :] * keep, patterns[q, 1, band, :] * keep
                re = re + (ore * pre - oim * pim)
                im = im + (ore * pim + oim * pre)
            out[c, 0, band, :] = re
            out[c, 1, band, :] = im

    chips = len(early) + 1
    fill_slots(child_parent, slots, clusters, width, chips)
    shift_and_phi(
        range(1, chips), 0, slots, child_parent, child_octant, out, phase, phi_hi, phi_lo,
        early, shifted,
    )


def theta_kernel(away, t_hi, t_lo, *rest):
    mine, *blocks, out, lats = rest
    chips = len(blocks) // 2 + 1
    early, late = blocks[:chips - 1], blocks[chips - 1:]
    member = lax.axis_index("member")
    chip, core = member // CORES, member % CORES
    t = core * CORES + (1 - core if away else core)
    rows = mine.shape[2]
    for i in range(out.shape[0]):
        for part in range(2):
            for s in range(chips):
                at = pl.multiple_of((chip ^ s) * rows, rows)
                if s == 0:
                    block = mine[i, part]
                else:
                    block = early[s - 1][0, part] if i == 0 else late[s - 1][i - 1, part]
                lats[pl.ds(at, rows), :] = block
            out[i, part] = dot3((t_hi[t], t_lo[t]), split(lats[...]))


def sum_kernel(keep, arrived, *outs):
    chip = lax.axis_index("member") // CORES
    rows = outs[0].shape[2]
    for s, out in enumerate(outs):
        band = pl.ds(pl.multiple_of((chip ^ s) * rows, rows), rows)
        out[...] = keep[:, :, band, :] + arrived[:, :, band, :]


def place_kernel(clusters, width, child_parent, *rest):
    *blocks, out, slots, sems = rest
    chips, per_chip = len(blocks), blocks[0].shape[0]
    chip = lax.axis_index("member") // CORES
    fill_slots(child_parent, slots, clusters, width, chips)
    pairs = [
        (block.at[i], out.at[slots[slot_of(chip ^ s, i, chips, per_chip)]])
        for s, block in enumerate(blocks)
        for i in range(per_chip)
    ]
    for copy in copy_all(pairs, sems):
        copy.wait()


def in_hbm(x):
    return pltpu.with_memory_space_constraint(x, pltpu.HBM)


def shape(*dims):
    return jax.ShapeDtypeStruct(dims, F32)


def params(limit):
    return pltpu.CompilerParams(vmem_limit_bytes=limit * MIB)


def call(*args, **kwargs):
    return pl.pallas_call(*args, **kwargs)


def cost(us):
    return pl.CostEstimate(flops=us * 2_000_000, bytes_accessed=us * 3_000_000, transcendentals=0)


def on_device(patterns, operators, partners, operator_index, child_parent, child_octant):
    clusters, _, rows, lons = patterns.shape
    members = lax.axis_size("member")
    groups = lax.axis_size("group")
    theta_count = rows * members
    chips = members // CORES
    children = child_parent.shape[0]
    per_chip = children // chips
    out_rows = NTC // members
    width = clusters // 4
    member = lax.axis_index("member")
    chip, core = member // CORES, member % CORES
    end = shape(width, 2, rows, lons)
    index = jax.ShapeDtypeStruct(partners.shape, jnp.int32)
    first, second, partners, operator_index = pl.pallas_call(
        ends_kernel,
        out_shape=(end, end, index, index),
        in_specs=[HBM] * 4,
        out_specs=(VMEM,) * 4,
        scratch_shapes=[pltpu.SemaphoreType.DMA((4,))],
        compiler_params=params(4),
    )(*map(in_hbm, (patterns, partners, operator_index, operators)))
    pairs = [[(i, i + 1) for i in range(start, groups - 1, 2)] for start in range(2)]
    pairs = [both + [(j, i) for i, j in both] for both in pairs]
    first = lax.ppermute(first, "group", pairs[0])
    second = lax.ppermute(second, "group", pairs[1])

    phi = split_const(phi_table(lons, NPC).T)
    assert per_chip > 1 and clusters - 2 * width >= chips
    slots = pltpu.SMEM((children,), jnp.int32)
    total_shape = shape(clusters, 2, rows, lons)

    def blocks_of(count, number):
        return (shape(count, 2, rows, NPC),) * number

    def rows_of(count):
        return pltpu.VMEM((count * 2 * rows, lons), F32)

    def between_chips(blocks):
        moved = []
        for s in range(chips - 1, 0, -1):
            pairs = [(i, i ^ (CORES * s)) for i in range(members)]
            moved.append(lax.ppermute(blocks[s], "member", pairs))
        return moved[::-1]

    own, phase, *early = call(
        functools.partial(own_kernel, theta_count, width),
        out_shape=(total_shape, shape(8, 2, rows, lons)) + blocks_of(1, chips - 1),
        in_specs=[VMEM] * 8,
        out_specs=(VMEM,) * (chips + 1),
        scratch_shapes=[
            pltpu.SMEM(partners.shape, jnp.int32),
            pltpu.SMEM(partners.shape, jnp.int32),
            slots,
            slots,
            slots,
            rows_of(chips - 1),
            pltpu.SemaphoreType.DMA((4,)),
        ],
        compiler_params=params(20),
        cost_estimate=cost(8),
    )(partners, operator_index, child_parent, child_octant, patterns, operators, *phi)
    early = between_chips(dict(enumerate(early, 1)))

    count = per_chip - 1
    far, near = [chips - 1], list(range(1, chips - 1))
    late = {}
    *outs, total = call(
        functools.partial(first_kernel, far),
        out_shape=blocks_of(count, len(far)) + (total_shape,),
        in_specs=[SMEM] * 4 + [VMEM] * 7,
        out_specs=(VMEM,) * (len(far) + 1),
        scratch_shapes=[slots, rows_of(count)],
        compiler_params=params(20),
        cost_estimate=cost(2),
    )(
        partners, operator_index, child_parent, child_octant, own, operators, first, second,
        phase, *phi,
    )
    late.update(zip(far, outs))

    def later(order, first_child, number):
        return call(
            functools.partial(later_kernel, order, first_child, width),
            out_shape=blocks_of(number, len(order)),
            in_specs=[SMEM] * 2 + [VMEM] * 4,
            out_specs=(VMEM,) * len(order),
            scratch_shapes=[slots, rows_of(number * len(order))],
            compiler_params=params(20),
            cost_estimate=cost(1),
        )(child_parent, child_octant, total, phase, *phi)

    late.update(zip(near, later(near, 1, count)))
    late = between_chips(late)
    (mine,) = later([0], 0, per_chip)

    theta = theta_table(theta_count, NTC).reshape(chips, CORES, out_rows, chips, CORES, rows)
    theta = theta.transpose(4, 1, 0, 2, 3, 5).reshape(
        CORES * CORES, chips * out_rows, chips * rows
    )
    swap = [(i, i ^ 1) for i in range(members)]
    if out_rows % 8 == 0:
        half = shape(per_chip, 2, chips * out_rows, NPC)
        away, keep = (
            call(
                functools.partial(theta_kernel, name == "away"),
                out_shape=half,
                in_specs=[VMEM] * (1 + 2 * chips),
                out_specs=VMEM,
                scratch_shapes=[pltpu.VMEM((chips * rows, NPC), F32)],
                compiler_params=params(12),
                cost_estimate=cost(1),
            )(*split_const(theta), mine, *early, *late)
            for name in ("away", "keep")
        )
        swapped = lax.ppermute(away, "member", swap)
        pieces = call(
            sum_kernel,
            out_shape=(shape(per_chip, 2, out_rows, NPC),) * chips,
            in_specs=[VMEM] * 2,
            out_specs=(VMEM,) * chips,
            compiler_params=params(12),
            cost_estimate=cost(1),
        )(keep, swapped)
    else:
        order = chip ^ jnp.arange(chips)
        lats = jnp.stack([mine] + [jnp.concatenate(pair) for pair in zip(early, late)])
        lats = jnp.take(lats, order, axis=0)
        lats = lats.transpose(1, 2, 0, 3, 4).reshape(per_chip, 2, chips * rows, NPC)
        both = jnp.take(
            jnp.asarray(theta, F32).reshape(CORES, CORES, chips * out_rows, chips * rows),
            core, axis=0,
        )
        sums = jnp.einsum(
            "wjt,kptg->wkpjg", both, lats, precision=lax.Precision.HIGHEST
        )
        moved = lax.ppermute(jnp.take(sums, 1 - core, axis=0), "member", swap)
        pieces = jnp.take(sums, core, axis=0) + moved
        pieces = pieces.reshape(per_chip, 2, chips, out_rows, NPC)
        pieces = [jnp.take(pieces, order[s], axis=2) for s in range(chips)]

    final = [pieces[0], *between_chips(dict(enumerate(pieces)))]
    return call(
        functools.partial(place_kernel, clusters, width),
        out_shape=shape(children, 2, out_rows, NPC),
        in_specs=[SMEM] + [VMEM] * chips,
        out_specs=HBM,
        scratch_shapes=[slots, pltpu.SemaphoreType.DMA((children,))],
        compiler_params=params(12),
        cost_estimate=cost(1),
    )(child_parent, *final)


def solution(mesh):
    return jax.shard_map(
        on_device,
        mesh=mesh,
        in_specs=(
            P("group", None, "member", None),
            P(None, None, "member", None),
            P("group", None),
            P("group", None),
            P("group"),
            P("group"),
        ),
        out_specs=P("group", None, "member", None),
        check_vma=False,
    )
```

```python
import functools
import math

import jax
import jax.numpy as jnp
import numpy as np
from jax import lax
from jax.experimental import pallas as pl
from jax.experimental.pallas import tpu as pltpu
from jax.sharding import PartitionSpec as P


NTC = 128
NPC = 256
CORES = 2
REACH = 6.0
F32 = jnp.float32
BF16 = jnp.bfloat16
MIB = 1 << 20


VMEM = pl.BlockSpec(memory_space=pltpu.VMEM)
SMEM = pl.BlockSpec(memory_space=pltpu.SMEM)
HBM = pl.BlockSpec(memory_space=pltpu.HBM)


def theta_table(fine, coarse):
    t = math.pi * (np.arange(fine) + 0.5) / fine
    j = math.pi * (np.arange(coarse) + 0.5) / coarse
    m = np.arange(coarse)
    w = np.where(m > 0, 2.0, 1.0)
    return (np.cos(np.outer(j, m)) * w) @ np.cos(np.outer(t, m)).T / fine


def phi_table(fine, coarse):
    f = 2.0 * math.pi * np.arange(fine) / fine
    g = 2.0 * math.pi * np.arange(coarse) / coarse
    m = np.arange(coarse // 2 + 1)
    v = np.where((m > 0) & (m < coarse // 2), 2.0, 1.0)
    cos_part = (np.cos(np.outer(g, m)) * v) @ np.cos(np.outer(f, m)).T
    sin_part = (np.sin(np.outer(g, m)) * v) @ np.sin(np.outer(f, m)).T
    return (cos_part + sin_part) / fine


def split_const(a):
    hi = np.asarray(a, np.float32).astype(BF16)
    lo = (np.asarray(a) - hi.astype(np.float64)).astype(np.float32).astype(BF16)
    return jnp.asarray(hi), jnp.asarray(lo)


def split(x):
    hi = x.astype(BF16)
    return hi, (x - hi.astype(F32)).astype(BF16)


def dot(a, b):
    return jnp.dot(a, b, preferred_element_type=F32)


def dot3(a, b):
    return dot(a[0], b[0]) + (dot(a[0], b[1]) + dot(a[1], b[0]))


def phase_tables(member, theta_count, phase_ref):
    rows, lons = phase_ref.shape[2], phase_ref.shape[3]
    quarter = lons // 4
    row = lax.broadcasted_iota(jnp.int32, (rows, 2 * quarter), 0)
    lon = lax.broadcasted_iota(jnp.int32, (rows, 2 * quarter), 1)
    theta = math.pi * ((row + member * rows).astype(F32) + 0.5) / theta_count
    phi = 2.0 * math.pi * lon.astype(F32) / lons
    x_arg = REACH * (jnp.sin(theta) * jnp.cos(phi))
    cos_x, sin_x = jnp.cos(x_arg), jnp.sin(x_arg)
    z_arg = REACH * jnp.cos(theta[:, :quarter])
    cz, sz = jnp.cos(z_arg), jnp.sin(z_arg)
    c0, c1 = cos_x[:, :quarter], cos_x[:, quarter:]
    s0, s1 = sin_x[:, :quarter], sin_x[:, quarter:]
    x_parts = ((c0, s0), (c1, s1), (c0, -s0), (c1, -s1))
    for q in range(4):
        ca, sa = x_parts[q]
        cb, sb = x_parts[(q + 3) % 4]
        cc, ss, sc, cs = ca * cb, sa * sb, sa * cb, ca * sb
        lanes = pl.ds(q * quarter, quarter)
        for octant in range(8):
            sgx = 1 - 2 * (octant % 2)
            sgy = 1 - 2 * (octant // 2 % 2)
            sgz = 1 - 2 * (octant // 4)
            re = cc - ss if sgx * sgy > 0 else cc + ss
            im = (sc if sgx > 0 else -sc) + (cs if sgy > 0 else -cs)
            szz = sz if sgz > 0 else -sz
            phase_ref[octant, 0, :, lanes] = re * cz - im * szz
            phase_ref[octant, 1, :, lanes] = re * szz + im * cz


def copy_all(pairs, sems):
    copies = [
        pltpu.make_async_copy(source, target, sems.at[n])
        for n, (source, target) in enumerate(pairs)
    ]
    for copy in copies:
        copy.start()
    return copies


def ends_kernel(patterns, operators, *rest):
    *rest, first, second, sems = rest
    tables = len(rest) // 2
    width = first.shape[0]
    last = patterns.shape[0] - width
    odd = lax.axis_index("group") % 2
    pairs = [
        (patterns.at[pl.ds((1 - odd) * last, width)], first),
        (patterns.at[pl.ds(odd * last, width)], second),
        *zip(rest[:tables], rest[tables:]),
    ]
    for copy in copy_all(pairs, sems):
        copy.wait()


def halo_terms(partners, op_index, own, operators, first, second, total):
    clusters, _, rows, _ = own.shape
    terms = partners.shape[1]
    width = first.shape[0]
    group = lax.axis_index("group")
    base = group * clusters
    total[...] = own[...]

    def add(n, halo, shift):
        c = n if n < width else n + clusters - 2 * width

        @pl.loop(0, terms)
        def _(p):
            q = partners[c, p] - base

            @pl.when((q < 0) | (q >= clusters))
            def _():
                e = op_index[c, p]
                h = jnp.clip(q + shift, 0, width - 1)
                for r in range(rows // 8):
                    band = pl.ds(r * 8, 8)
                    ore, oim = operators[e, 0, band, :], operators[e, 1, band, :]
                    pre, pim = halo[h, 0, band, :], halo[h, 1, band, :]
                    total[c, 0, band, :] += ore * pre - oim * pim
                    total[c, 1, band, :] += ore * pim + oim * pre

    for odd, below, above in ((0, second, first), (1, first, second)):

        @pl.when(group % 2 == odd)
        def _():
            for n in range(2 * width):
                if n < width:
                    add(n, below, width)
                else:
                    add(n, above, -clusters)


def fill_slots(child_parent, slots, clusters, width, chips):
    base = lax.axis_index("group") * clusters

    early, late = jnp.int32(0), jnp.int32(chips)
    for k in range(slots.shape[0]):
        q = child_parent[k] - base
        inner = (q >= width) & (q < clusters - width) & (early < chips)
        slots[jnp.where(inner, early, late)] = k
        step = jnp.where(inner, 1, 0)
        early, late = early + step, late + 1 - step


def slot_of(chip, i, chips, per_chip):
    return chip if i == 0 else chips + chip * (per_chip - 1) + i - 1


def shift_and_phi(
    order, first, slots, child_parent, child_octant, total, phase, phi_hi, phi_lo, outs, shifted
):
    clusters, _, rows, _ = total.shape
    chips = lax.axis_size("member") // CORES
    per_chip = slots.shape[0] // chips
    base = lax.axis_index("group") * clusters
    chip = lax.axis_index("member") // CORES
    count = outs[0].shape[0]
    size = count * 2 * rows
    group = shifted.shape[0] // size
    for start in range(0, len(order), group):
        part = list(zip(order, outs))[start:start + group]
        for m, (s, _) in enumerate(part):
            for i in range(count):
                k = slots[slot_of(chip ^ s, first + i, chips, per_chip)]
                q = child_parent[k] - base
                o = child_octant[k]
                for r in range(rows // 8):
                    band = pl.ds(r * 8, 8)
                    pre, pim = total[q, 0, band, :], total[q, 1, band, :]
                    ere, eim = phase[o, 0, band, :], phase[o, 1, band, :]
                    at = m * size + i * 2 * rows + r * 8
                    shifted[pl.ds(at, 8), :] = pre * ere - pim * eim
                    shifted[pl.ds(at + rows, 8), :] = pre * eim + pim * ere
        used = pl.ds(0, len(part) * size)
        y = dot3(split(shifted[used, :]), (phi_hi[...], phi_lo[...]))
        for m, (_, out) in enumerate(part):
            out[...] = y[m * size:(m + 1) * size].reshape(out.shape)


def first_kernel(
    order, partners, op_index, child_parent, child_octant, own, operators, first, second, phase,
    phi_hi, phi_lo, *rest
):
    *outs, total, slots, shifted = rest
    chips = lax.axis_size("member") // CORES
    fill_slots(child_parent, slots, own.shape[0], first.shape[0], chips)
    halo_terms(partners, op_index, own, operators, first, second, total)
    shift_and_phi(
        order, 1, slots, child_parent, child_octant, total, phase, phi_hi, phi_lo, outs, shifted
    )


def later_kernel(
    order, first, width, child_parent, child_octant, total, phase, phi_hi, phi_lo, *rest
):
    *outs, slots, shifted = rest
    chips = lax.axis_size("member") // CORES
    fill_slots(child_parent, slots, total.shape[0], width, chips)
    shift_and_phi(
        order, first, slots, child_parent, child_octant, total, phase, phi_hi, phi_lo, outs,
        shifted,
    )


def own_kernel(
    theta_count, width, partners_in, op_in, parent_in, octant_in, patterns, operators, hi_in,
    lo_in, out, phase, *rest
):
    *early, partners, op_index, child_parent, child_octant, slots, shifted, phi_hi, phi_lo, sems = (
        rest
    )
    clusters, terms = partners.shape
    rows = out.shape[2]
    copies = copy_all(
        [
            (partners_in, partners),
            (op_in, op_index),
            (parent_in, child_parent),
            (octant_in, child_octant),
            (hi_in, phi_hi),
            (lo_in, phi_lo),
        ],
        sems,
    )
    phase_tables(lax.axis_index("member"), theta_count, phase)
    base = lax.axis_index("group") * clusters
    for copy in copies[:4]:
        copy.wait()

    def translate(c, edge):
        for r in range(rows // 8):
            band = pl.ds(r * 8, 8)
            re, im = 0.0, 0.0
            for p in range(terms):
                q, e = partners[c, p] - base, op_index[c, p]
                ore, oim = operators[e, 0, band, :], operators[e, 1, band, :]
                if edge:
                    keep = jnp.where((q >= 0) & (q < clusters), 1.0, 0.0).astype(F32)
                    q = jnp.clip(q, 0, clusters - 1)
                    ore, oim = ore * keep, oim * keep
                pre, pim = patterns[q, 0, band, :], patterns[q, 1, band, :]
                re = re + (ore * pre - oim * pim)
                im = im + (ore * pim + oim * pre)
            out[c, 0, band, :] = re
            out[c, 1, band, :] = im

    @pl.loop(width, clusters - width)
    def _(c):
        translate(c, False)

    @pl.loop(0, 2 * width)
    def _(n):
        translate(jnp.where(n < width, n, n + clusters - 2 * width), True)

    for copy in copies[4:]:
        copy.wait()

    chips = len(early) + 1
    fill_slots(child_parent, slots, clusters, width, chips)
    shift_and_phi(
        range(1, chips), 0, slots, child_parent, child_octant, out, phase, phi_hi, phi_lo,
        early, shifted,
    )


def theta_kernel(away, t_hi, t_lo, *rest):
    mine, *blocks, out, lats = rest
    chips = len(blocks) // 2 + 1
    early, late = blocks[:chips - 1], blocks[chips - 1:]
    member = lax.axis_index("member")
    chip, core = member // CORES, member % CORES
    t = core * CORES + (1 - core if away else core)
    rows = mine.shape[2]
    for i in range(out.shape[0]):
        for part in range(2):
            for s in range(chips):
                at = pl.multiple_of((chip ^ s) * rows, rows)
                if s == 0:
                    block = mine[i, part]
                else:
                    block = early[s - 1][0, part] if i == 0 else late[s - 1][i - 1, part]
                lats[pl.ds(at, rows), :] = block
            out[i, part] = dot3((t_hi[t], t_lo[t]), split(lats[...]))


def sum_kernel(keep, arrived, *outs):
    chip = lax.axis_index("member") // CORES
    rows = outs[0].shape[2]
    for s, out in enumerate(outs):
        band = pl.ds(pl.multiple_of((chip ^ s) * rows, rows), rows)
        out[...] = keep[:, :, band, :] + arrived[:, :, band, :]


def place_kernel(clusters, width, child_parent, *rest):
    *blocks, out, slots, sems = rest
    chips, per_chip = len(blocks), blocks[0].shape[0]
    chip = lax.axis_index("member") // CORES
    fill_slots(child_parent, slots, clusters, width, chips)
    pairs = [
        (block.at[i], out.at[slots[slot_of(chip ^ s, i, chips, per_chip)]])
        for s, block in enumerate(blocks)
        for i in range(per_chip)
    ]
    for copy in copy_all(pairs, sems):
        copy.wait()


def in_hbm(x):
    return pltpu.with_memory_space_constraint(x, pltpu.HBM)


def shape(*dims):
    return jax.ShapeDtypeStruct(dims, F32)


def params(limit):
    return pltpu.CompilerParams(vmem_limit_bytes=limit * MIB)


def call(*args, **kwargs):
    return pl.pallas_call(*args, **kwargs)


def cost(us):
    return pl.CostEstimate(flops=us * 2_000_000, bytes_accessed=us * 3_000_000, transcendentals=0)


def on_device(patterns, operators, partners, operator_index, child_parent, child_octant):
    clusters, _, rows, lons = patterns.shape
    members = lax.axis_size("member")
    groups = lax.axis_size("group")
    theta_count = rows * members
    chips = members // CORES
    children = child_parent.shape[0]
    per_chip = children // chips
    out_rows = NTC // members
    width = clusters // 4
    member = lax.axis_index("member")
    chip, core = member // CORES, member % CORES
    end = shape(width, 2, rows, lons)
    tables = (partners, operator_index, child_parent, child_octant)
    *tables, first, second = pl.pallas_call(
        ends_kernel,
        out_shape=tuple(jax.ShapeDtypeStruct(x.shape, x.dtype) for x in tables) + (end, end),
        in_specs=[HBM] * (2 + len(tables)),
        out_specs=(VMEM,) * (2 + len(tables)),
        scratch_shapes=[pltpu.SemaphoreType.DMA((2 + len(tables),))],
        compiler_params=params(4),
    )(*map(in_hbm, (patterns, operators, *tables)))
    partners, operator_index, child_parent, child_octant = tables
    pairs = [[(i, i + 1) for i in range(start, groups - 1, 2)] for start in range(2)]
    pairs = [both + [(j, i) for i, j in both] for both in pairs]
    first = lax.ppermute(first, "group", pairs[0])
    second = lax.ppermute(second, "group", pairs[1])

    phi = split_const(phi_table(lons, NPC).T)
    assert per_chip > 1 and clusters - 2 * width >= chips
    slots = pltpu.SMEM((children,), jnp.int32)
    total_shape = shape(clusters, 2, rows, lons)

    def blocks_of(count, number):
        return (shape(count, 2, rows, NPC),) * number

    def rows_of(count):
        return pltpu.VMEM((count * 2 * rows, lons), F32)

    def between_chips(blocks):
        moved = []
        for s in range(chips - 1, 0, -1):
            pairs = [(i, i ^ (CORES * s)) for i in range(members)]
            moved.append(lax.ppermute(blocks[s], "member", pairs))
        return moved[::-1]

    own, phase, *early = call(
        functools.partial(own_kernel, theta_count, width),
        out_shape=(total_shape, shape(8, 2, rows, lons)) + blocks_of(1, chips - 1),
        in_specs=[VMEM] * 6 + [HBM] * 2,
        out_specs=(VMEM,) * (chips + 1),
        scratch_shapes=[
            pltpu.SMEM(partners.shape, jnp.int32),
            pltpu.SMEM(partners.shape, jnp.int32),
            slots,
            slots,
            slots,
            rows_of(chips - 1),
            pltpu.VMEM(phi[0].shape, BF16),
            pltpu.VMEM(phi[1].shape, BF16),
            pltpu.SemaphoreType.DMA((6,)),
        ],
        compiler_params=params(20),
        cost_estimate=cost(8),
    )(
        partners, operator_index, child_parent, child_octant, patterns, operators,
        *map(in_hbm, phi),
    )
    early = between_chips(dict(enumerate(early, 1)))

    count = per_chip - 1
    far, near = [chips - 1], list(range(1, chips - 1))
    late = {}
    *outs, total = call(
        functools.partial(first_kernel, far),
        out_shape=blocks_of(count, len(far)) + (total_shape,),
        in_specs=[SMEM] * 4 + [VMEM] * 7,
        out_specs=(VMEM,) * (len(far) + 1),
        scratch_shapes=[slots, rows_of(count)],
        compiler_params=params(20),
        cost_estimate=cost(2),
    )(
        partners, operator_index, child_parent, child_octant, own, operators, first, second,
        phase, *phi,
    )
    late.update(zip(far, outs))

    def later(order, first_child, number):
        return call(
            functools.partial(later_kernel, order, first_child, width),
            out_shape=blocks_of(number, len(order)),
            in_specs=[SMEM] * 2 + [VMEM] * 4,
            out_specs=(VMEM,) * len(order),
            scratch_shapes=[slots, rows_of(number * len(order))],
            compiler_params=params(20),
            cost_estimate=cost(1),
        )(child_parent, child_octant, total, phase, *phi)

    late.update(zip(near, later(near, 1, count)))
    late = between_chips(late)
    (mine,) = later([0], 0, per_chip)

    theta = theta_table(theta_count, NTC).reshape(chips, CORES, out_rows, chips, CORES, rows)
    theta = theta.transpose(4, 1, 0, 2, 3, 5).reshape(
        CORES * CORES, chips * out_rows, chips * rows
    )
    swap = [(i, i ^ 1) for i in range(members)]
    if out_rows % 8 == 0:
        half = shape(per_chip, 2, chips * out_rows, NPC)
        away, keep = (
            call(
                functools.partial(theta_kernel, name == "away"),
                out_shape=half,
                in_specs=[VMEM] * (1 + 2 * chips),
                out_specs=VMEM,
                scratch_shapes=[pltpu.VMEM((chips * rows, NPC), F32)],
                compiler_params=params(12),
                cost_estimate=cost(1),
            )(*split_const(theta), mine, *early, *late)
            for name in ("away", "keep")
        )
        swapped = lax.ppermute(away, "member", swap)
        pieces = call(
            sum_kernel,
            out_shape=(shape(per_chip, 2, out_rows, NPC),) * chips,
            in_specs=[VMEM] * 2,
            out_specs=(VMEM,) * chips,
            compiler_params=params(12),
            cost_estimate=cost(1),
        )(keep, swapped)
    else:
        order = chip ^ jnp.arange(chips)
        lats = jnp.stack([mine] + [jnp.concatenate(pair) for pair in zip(early, late)])
        lats = jnp.take(lats, order, axis=0)
        lats = lats.transpose(1, 2, 0, 3, 4).reshape(per_chip, 2, chips * rows, NPC)
        both = jnp.take(
            jnp.asarray(theta, F32).reshape(CORES, CORES, chips * out_rows, chips * rows),
            core, axis=0,
        )
        sums = jnp.einsum(
            "wjt,kptg->wkpjg", both, lats, precision=lax.Precision.HIGHEST
        )
        moved = lax.ppermute(jnp.take(sums, 1 - core, axis=0), "member", swap)
        pieces = jnp.take(sums, core, axis=0) + moved
        pieces = pieces.reshape(per_chip, 2, chips, out_rows, NPC)
        pieces = [jnp.take(pieces, order[s], axis=2) for s in range(chips)]

    final = [pieces[0], *between_chips(dict(enumerate(pieces)))]
    return call(
        functools.partial(place_kernel, clusters, width),
        out_shape=shape(children, 2, out_rows, NPC),
        in_specs=[SMEM] + [VMEM] * chips,
        out_specs=HBM,
        scratch_shapes=[slots, pltpu.SemaphoreType.DMA((children,))],
        compiler_params=params(12),
        cost_estimate=cost(1),
    )(child_parent, *final)


def solution(mesh):
    return jax.shard_map(
        on_device,
        mesh=mesh,
        in_specs=(
            P("group", None, "member", None),
            P(None, None, "member", None),
            P("group", None),
            P("group", None),
            P("group"),
            P("group"),
        ),
        out_specs=P("group", None, "member", None),
        check_vma=False,
    )
```

```python
import functools
import math

import jax
import jax.numpy as jnp
import numpy as np
from jax import lax
from jax.experimental import pallas as pl
from jax.experimental.pallas import tpu as pltpu
from jax.sharding import PartitionSpec as P


NTC = 128
NPC = 256
CORES = 2
REACH = 6.0
F32 = jnp.float32
BF16 = jnp.bfloat16
MIB = 1 << 20


VMEM = pl.BlockSpec(memory_space=pltpu.VMEM)
SMEM = pl.BlockSpec(memory_space=pltpu.SMEM)
HBM = pl.BlockSpec(memory_space=pltpu.HBM)


def theta_table(fine, coarse):
    t = math.pi * (np.arange(fine) + 0.5) / fine
    j = math.pi * (np.arange(coarse) + 0.5) / coarse
    m = np.arange(coarse)
    w = np.where(m > 0, 2.0, 1.0)
    return (np.cos(np.outer(j, m)) * w) @ np.cos(np.outer(t, m)).T / fine


def phi_table(fine, coarse):
    f = 2.0 * math.pi * np.arange(fine) / fine
    g = 2.0 * math.pi * np.arange(coarse) / coarse
    m = np.arange(coarse // 2 + 1)
    v = np.where((m > 0) & (m < coarse // 2), 2.0, 1.0)
    cos_part = (np.cos(np.outer(g, m)) * v) @ np.cos(np.outer(f, m)).T
    sin_part = (np.sin(np.outer(g, m)) * v) @ np.sin(np.outer(f, m)).T
    return (cos_part + sin_part) / fine


def split_const(a):
    hi = np.asarray(a, np.float32).astype(BF16)
    lo = (np.asarray(a) - hi.astype(np.float64)).astype(np.float32).astype(BF16)
    return jnp.asarray(hi), jnp.asarray(lo)


def split(x):
    hi = x.astype(BF16)
    return hi, (x - hi.astype(F32)).astype(BF16)


def dot(a, b):
    return jnp.dot(a, b, preferred_element_type=F32)


def dot3(a, b):
    return dot(a[0], b[0]) + (dot(a[0], b[1]) + dot(a[1], b[0]))


def phase_tables(member, theta_count, phase_ref):
    rows, lons = phase_ref.shape[2], phase_ref.shape[3]
    quarter = lons // 4
    row = lax.broadcasted_iota(jnp.int32, (rows, 2 * quarter), 0)
    lon = lax.broadcasted_iota(jnp.int32, (rows, 2 * quarter), 1)
    theta = math.pi * ((row + member * rows).astype(F32) + 0.5) / theta_count
    phi = 2.0 * math.pi * lon.astype(F32) / lons
    x_arg = REACH * (jnp.sin(theta) * jnp.cos(phi))
    cos_x, sin_x = jnp.cos(x_arg), jnp.sin(x_arg)
    z_arg = REACH * jnp.cos(theta[:, :quarter])
    cz, sz = jnp.cos(z_arg), jnp.sin(z_arg)
    c0, c1 = cos_x[:, :quarter], cos_x[:, quarter:]
    s0, s1 = sin_x[:, :quarter], sin_x[:, quarter:]
    x_parts = ((c0, s0), (c1, s1), (c0, -s0), (c1, -s1))
    for q in range(4):
        ca, sa = x_parts[q]
        cb, sb = x_parts[(q + 3) % 4]
        cc, ss, sc, cs = ca * cb, sa * sb, sa * cb, ca * sb
        lanes = pl.ds(q * quarter, quarter)
        for octant in range(8):
            sgx = 1 - 2 * (octant % 2)
            sgy = 1 - 2 * (octant // 2 % 2)
            sgz = 1 - 2 * (octant // 4)
            re = cc - ss if sgx * sgy > 0 else cc + ss
            im = (sc if sgx > 0 else -sc) + (cs if sgy > 0 else -cs)
            szz = sz if sgz > 0 else -sz
            phase_ref[octant, 0, :, lanes] = re * cz - im * szz
            phase_ref[octant, 1, :, lanes] = re * szz + im * cz


def copy_all(pairs, sems):
    copies = [
        pltpu.make_async_copy(source, target, sems.at[n])
        for n, (source, target) in enumerate(pairs)
    ]
    for copy in copies:
        copy.start()
    return copies


def ends_kernel(patterns, operators, *rest):
    *rest, first, second, sems = rest
    tables = len(rest) // 2
    width = first.shape[0]
    last = patterns.shape[0] - width
    odd = lax.axis_index("group") % 2
    pairs = [
        (patterns.at[pl.ds((1 - odd) * last, width)], first),
        (patterns.at[pl.ds(odd * last, width)], second),
        *zip(rest[:tables], rest[tables:]),
    ]
    for copy in copy_all(pairs, sems):
        copy.wait()


def halo_terms(partners, op_index, own, operators, first, second, total):
    clusters, _, rows, _ = own.shape
    terms = partners.shape[1]
    width = first.shape[0]
    group = lax.axis_index("group")
    base = group * clusters
    total[...] = own[...]

    def add(n, halo, shift):
        c = n if n < width else n + clusters - 2 * width

        @pl.loop(0, terms)
        def _(p):
            q = partners[c, p] - base

            @pl.when((q < 0) | (q >= clusters))
            def _():
                e = op_index[c, p]
                h = jnp.clip(q + shift, 0, width - 1)
                for r in range(rows // 8):
                    band = pl.ds(r * 8, 8)
                    ore, oim = operators[e, 0, band, :], operators[e, 1, band, :]
                    pre, pim = halo[h, 0, band, :], halo[h, 1, band, :]
                    total[c, 0, band, :] += ore * pre - oim * pim
                    total[c, 1, band, :] += ore * pim + oim * pre

    for odd, below, above in ((0, second, first), (1, first, second)):

        @pl.when(group % 2 == odd)
        def _():
            for n in range(2 * width):
                if n < width:
                    add(n, below, width)
                else:
                    add(n, above, -clusters)


def fill_slots(child_parent, slots, clusters, width, chips):
    base = lax.axis_index("group") * clusters

    early, late = jnp.int32(0), jnp.int32(chips)
    for k in range(slots.shape[0]):
        q = child_parent[k] - base
        inner = (q >= width) & (q < clusters - width) & (early < chips)
        slots[jnp.where(inner, early, late)] = k
        step = jnp.where(inner, 1, 0)
        early, late = early + step, late + 1 - step


def slot_of(chip, i, chips, per_chip):
    return chip if i == 0 else chips + chip * (per_chip - 1) + i - 1


def shift_and_phi(
    order, first, slots, child_parent, child_octant, total, phase, phi_hi, phi_lo, outs, shifted
):
    clusters, _, rows, _ = total.shape
    chips = lax.axis_size("member") // CORES
    per_chip = slots.shape[0] // chips
    base = lax.axis_index("group") * clusters
    chip = lax.axis_index("member") // CORES
    count = outs[0].shape[0]
    size = count * 2 * rows
    group = shifted.shape[0] // size
    for start in range(0, len(order), group):
        part = list(zip(order, outs))[start:start + group]
        for m, (s, _) in enumerate(part):
            for i in range(count):
                k = slots[slot_of(chip ^ s, first + i, chips, per_chip)]
                q = child_parent[k] - base
                o = child_octant[k]
                for r in range(rows // 8):
                    band = pl.ds(r * 8, 8)
                    pre, pim = total[q, 0, band, :], total[q, 1, band, :]
                    ere, eim = phase[o, 0, band, :], phase[o, 1, band, :]
                    at = m * size + i * 2 * rows + r * 8
                    shifted[pl.ds(at, 8), :] = pre * ere - pim * eim
                    shifted[pl.ds(at + rows, 8), :] = pre * eim + pim * ere
        used = pl.ds(0, len(part) * size)
        y = dot3(split(shifted[used, :]), (phi_hi[...], phi_lo[...]))
        for m, (_, out) in enumerate(part):
            out[...] = y[m * size:(m + 1) * size].reshape(out.shape)


def first_kernel(
    order, partners, op_index, child_parent, child_octant, own, operators, first, second, phase,
    phi_hi, phi_lo, *rest
):
    *outs, total, slots, shifted = rest
    chips = lax.axis_size("member") // CORES
    fill_slots(child_parent, slots, own.shape[0], first.shape[0], chips)
    halo_terms(partners, op_index, own, operators, first, second, total)
    shift_and_phi(
        order, 1, slots, child_parent, child_octant, total, phase, phi_hi, phi_lo, outs, shifted
    )


def later_kernel(
    order, first, width, child_parent, child_octant, total, phase, phi_hi, phi_lo, *rest
):
    *outs, slots, shifted = rest
    chips = lax.axis_size("member") // CORES
    fill_slots(child_parent, slots, total.shape[0], width, chips)
    shift_and_phi(
        order, first, slots, child_parent, child_octant, total, phase, phi_hi, phi_lo, outs,
        shifted,
    )


def own_kernel(
    theta_count, width, partners_in, op_in, parent_in, octant_in, patterns, operators, hi_in,
    lo_in, out, phase, *rest
):
    *early, partners, op_index, child_parent, child_octant, slots, shifted, phi_hi, phi_lo, sems = (
        rest
    )
    clusters, terms = partners.shape
    rows = out.shape[2]
    copies = copy_all(
        [
            (partners_in, partners),
            (op_in, op_index),
            (parent_in, child_parent),
            (octant_in, child_octant),
            (hi_in, phi_hi),
            (lo_in, phi_lo),
        ],
        sems,
    )
    phase_tables(lax.axis_index("member"), theta_count, phase)
    base = lax.axis_index("group") * clusters
    for copy in copies[:4]:
        copy.wait()

    def translate(c, edge):
        for r in range(rows // 8):
            band = pl.ds(r * 8, 8)
            re, im = 0.0, 0.0
            for p in range(terms):
                q, e = partners[c, p] - base, op_index[c, p]
                ore, oim = operators[e, 0, band, :], operators[e, 1, band, :]
                if edge:
                    keep = jnp.where((q >= 0) & (q < clusters), 1.0, 0.0).astype(F32)
                    q = jnp.clip(q, 0, clusters - 1)
                    ore, oim = ore * keep, oim * keep
                pre, pim = patterns[q, 0, band, :], patterns[q, 1, band, :]
                re = re + (ore * pre - oim * pim)
                im = im + (ore * pim + oim * pre)
            out[c, 0, band, :] = re
            out[c, 1, band, :] = im

    @pl.loop(width, clusters - width)
    def _(c):
        translate(c, False)

    @pl.loop(0, 2 * width)
    def _(n):
        translate(jnp.where(n < width, n, n + clusters - 2 * width), True)

    for copy in copies[4:]:
        copy.wait()

    chips = len(early) + 1
    fill_slots(child_parent, slots, clusters, width, chips)
    shift_and_phi(
        range(1, chips), 0, slots, child_parent, child_octant, out, phase, phi_hi, phi_lo,
        early, shifted,
    )


def last_kernel(width, child_parent, child_octant, total, phase, phi_hi, phi_lo, *rest):
    out, child_of, slots, shifted = rest
    chips = lax.axis_size("member") // CORES
    chip = lax.axis_index("member") // CORES
    per_chip = out.shape[0]
    args = (child_parent, child_octant, total, phase, phi_hi, phi_lo, out, slots, shifted)
    later_kernel([0], 0, width, *args)
    for s in range(chips):
        for i in range(per_chip):
            k = slots[slot_of(chip ^ s, i, chips, per_chip)]
            child_of[s * per_chip + i] = jnp.full(child_of.shape[1:], k, jnp.int32)


def theta_kernel(away, t_hi, t_lo, *rest):
    mine, *blocks, out, lats = rest
    chips = len(blocks) // 2 + 1
    early, late = blocks[:chips - 1], blocks[chips - 1:]
    member = lax.axis_index("member")
    chip, core = member // CORES, member % CORES
    t = core * CORES + (1 - core if away else core)
    rows = mine.shape[2]
    for i in range(out.shape[0]):
        for part in range(2):
            for s in range(chips):
                at = pl.multiple_of((chip ^ s) * rows, rows)
                if s == 0:
                    block = mine[i, part]
                else:
                    block = early[s - 1][0, part] if i == 0 else late[s - 1][i - 1, part]
                lats[pl.ds(at, rows), :] = block
            out[i, part] = dot3((t_hi[t], t_lo[t]), split(lats[...]))


def sum_kernel(keep, arrived, *outs):
    chip = lax.axis_index("member") // CORES
    rows = outs[0].shape[2]
    for s, out in enumerate(outs):
        band = pl.ds(pl.multiple_of((chip ^ s) * rows, rows), rows)
        out[...] = keep[:, :, band, :] + arrived[:, :, band, :]


def place_kernel(child_of, *rest):
    *blocks, out, sems = rest
    per_chip = blocks[0].shape[0]
    pairs = [
        (block.at[i], out.at[child_of[s * per_chip + i][0, 0]])
        for s, block in enumerate(blocks)
        for i in range(per_chip)
    ]
    for copy in copy_all(pairs, sems):
        copy.wait()


def in_hbm(x):
    return pltpu.with_memory_space_constraint(x, pltpu.HBM)


def shape(*dims):
    return jax.ShapeDtypeStruct(dims, F32)


def params(limit):
    return pltpu.CompilerParams(vmem_limit_bytes=limit * MIB)


def call(*args, **kwargs):
    return pl.pallas_call(*args, **kwargs)


def cost(us):
    return pl.CostEstimate(flops=us * 2_000_000, bytes_accessed=us * 3_000_000, transcendentals=0)


def on_device(patterns, operators, partners, operator_index, child_parent, child_octant):
    clusters, _, rows, lons = patterns.shape
    members = lax.axis_size("member")
    groups = lax.axis_size("group")
    theta_count = rows * members
    chips = members // CORES
    children = child_parent.shape[0]
    per_chip = children // chips
    out_rows = NTC // members
    width = clusters // 4
    member = lax.axis_index("member")
    chip, core = member // CORES, member % CORES
    end = shape(width, 2, rows, lons)
    tables = (partners, operator_index, child_parent, child_octant)
    *tables, first, second = pl.pallas_call(
        ends_kernel,
        out_shape=tuple(jax.ShapeDtypeStruct(x.shape, x.dtype) for x in tables) + (end, end),
        in_specs=[HBM] * (2 + len(tables)),
        out_specs=(VMEM,) * (2 + len(tables)),
        scratch_shapes=[pltpu.SemaphoreType.DMA((2 + len(tables),))],
        compiler_params=params(4),
    )(*map(in_hbm, (patterns, operators, *tables)))
    partners, operator_index, child_parent, child_octant = tables
    pairs = [[(i, i + 1) for i in range(start, groups - 1, 2)] for start in range(2)]
    pairs = [both + [(j, i) for i, j in both] for both in pairs]
    first = lax.ppermute(first, "group", pairs[0])
    second = lax.ppermute(second, "group", pairs[1])

    phi = split_const(phi_table(lons, NPC).T)
    assert per_chip > 1 and clusters - 2 * width >= chips
    slots = pltpu.SMEM((children,), jnp.int32)
    total_shape = shape(clusters, 2, rows, lons)

    def blocks_of(count, number):
        return (shape(count, 2, rows, NPC),) * number

    def rows_of(count):
        return pltpu.VMEM((count * 2 * rows, lons), F32)

    def between_chips(blocks):
        moved = []
        for s in range(chips - 1, 0, -1):
            pairs = [(i, i ^ (CORES * s)) for i in range(members)]
            moved.append(lax.ppermute(blocks[s], "member", pairs))
        return moved[::-1]

    own, phase, *early = call(
        functools.partial(own_kernel, theta_count, width),
        out_shape=(total_shape, shape(8, 2, rows, lons)) + blocks_of(1, chips - 1),
        in_specs=[VMEM] * 6 + [HBM] * 2,
        out_specs=(VMEM,) * (chips + 1),
        scratch_shapes=[
            pltpu.SMEM(partners.shape, jnp.int32),
            pltpu.SMEM(partners.shape, jnp.int32),
            slots,
            slots,
            slots,
            rows_of(chips - 1),
            pltpu.VMEM(phi[0].shape, BF16),
            pltpu.VMEM(phi[1].shape, BF16),
            pltpu.SemaphoreType.DMA((6,)),
        ],
        compiler_params=params(20),
        cost_estimate=cost(8),
    )(
        partners, operator_index, child_parent, child_octant, patterns, operators,
        *map(in_hbm, phi),
    )
    early = between_chips(dict(enumerate(early, 1)))

    count = per_chip - 1
    far, near = [chips - 1], list(range(1, chips - 1))
    late = {}
    *outs, total = call(
        functools.partial(first_kernel, far),
        out_shape=blocks_of(count, len(far)) + (total_shape,),
        in_specs=[SMEM] * 4 + [VMEM] * 7,
        out_specs=(VMEM,) * (len(far) + 1),
        scratch_shapes=[slots, rows_of(count)],
        compiler_params=params(20),
        cost_estimate=cost(2),
    )(
        partners, operator_index, child_parent, child_octant, own, operators, first, second,
        phase, *phi,
    )
    late.update(zip(far, outs))

    def later(kernel, out_shape, number):
        return call(
            kernel,
            out_shape=out_shape,
            in_specs=[SMEM] * 2 + [VMEM] * 4,
            out_specs=(VMEM,) * len(out_shape),
            scratch_shapes=[slots, rows_of(number)],
            compiler_params=params(20),
            cost_estimate=cost(1),
        )(child_parent, child_octant, total, phase, *phi)

    outs = later(
        functools.partial(later_kernel, near, 1, width),
        blocks_of(count, len(near)), count * len(near),
    )
    late.update(zip(near, outs))
    late = between_chips(late)
    tiles = jax.ShapeDtypeStruct((children, 8, 128), jnp.int32)
    mine, child_of = later(
        functools.partial(last_kernel, width),
        blocks_of(per_chip, 1) + (tiles,), per_chip,
    )

    theta = theta_table(theta_count, NTC).reshape(chips, CORES, out_rows, chips, CORES, rows)
    theta = theta.transpose(4, 1, 0, 2, 3, 5).reshape(
        CORES * CORES, chips * out_rows, chips * rows
    )
    swap = [(i, i ^ 1) for i in range(members)]
    if out_rows % 8 == 0:
        half = shape(per_chip, 2, chips * out_rows, NPC)
        away, keep = (
            call(
                functools.partial(theta_kernel, name == "away"),
                out_shape=half,
                in_specs=[VMEM] * (1 + 2 * chips),
                out_specs=VMEM,
                scratch_shapes=[pltpu.VMEM((chips * rows, NPC), F32)],
                compiler_params=params(12),
                cost_estimate=cost(1),
            )(*split_const(theta), mine, *early, *late)
            for name in ("away", "keep")
        )
        swapped = lax.ppermute(away, "member", swap)
        pieces = call(
            sum_kernel,
            out_shape=(shape(per_chip, 2, out_rows, NPC),) * chips,
            in_specs=[VMEM] * 2,
            out_specs=(VMEM,) * chips,
            compiler_params=params(12),
            cost_estimate=cost(1),
        )(keep, swapped)
    else:
        order = chip ^ jnp.arange(chips)
        lats = jnp.stack([mine] + [jnp.concatenate(pair) for pair in zip(early, late)])
        lats = jnp.take(lats, order, axis=0)
        lats = lats.transpose(1, 2, 0, 3, 4).reshape(per_chip, 2, chips * rows, NPC)
        both = jnp.take(
            jnp.asarray(theta, F32).reshape(CORES, CORES, chips * out_rows, chips * rows),
            core, axis=0,
        )
        sums = jnp.einsum(
            "wjt,kptg->wkpjg", both, lats, precision=lax.Precision.HIGHEST
        )
        moved = lax.ppermute(jnp.take(sums, 1 - core, axis=0), "member", swap)
        pieces = jnp.take(sums, core, axis=0) + moved
        pieces = pieces.reshape(per_chip, 2, chips, out_rows, NPC)
        pieces = [jnp.take(pieces, order[s], axis=2) for s in range(chips)]

    final = [pieces[0], *between_chips(dict(enumerate(pieces)))]
    return call(
        place_kernel,
        out_shape=shape(children, 2, out_rows, NPC),
        in_specs=[VMEM] * (1 + chips),
        out_specs=HBM,
        scratch_shapes=[pltpu.SemaphoreType.DMA((children,))],
        compiler_params=params(12),
        cost_estimate=cost(1),
    )(child_of, *final)


def solution(mesh):
    return jax.shard_map(
        on_device,
        mesh=mesh,
        in_specs=(
            P("group", None, "member", None),
            P(None, None, "member", None),
            P("group", None),
            P("group", None),
            P("group"),
            P("group"),
        ),
        out_specs=P("group", None, "member", None),
        check_vma=False,
    )
```

```python
import functools
import math

import jax
import jax.numpy as jnp
import numpy as np
from jax import lax
from jax.experimental import pallas as pl
from jax.experimental.pallas import tpu as pltpu
from jax.sharding import PartitionSpec as P


NTC = 128
NPC = 256
CORES = 2
REACH = 6.0
F32 = jnp.float32
BF16 = jnp.bfloat16
MIB = 1 << 20


VMEM = pl.BlockSpec(memory_space=pltpu.VMEM)
SMEM = pl.BlockSpec(memory_space=pltpu.SMEM)
HBM = pl.BlockSpec(memory_space=pltpu.HBM)


def theta_table(fine, coarse):
    t = math.pi * (np.arange(fine) + 0.5) / fine
    j = math.pi * (np.arange(coarse) + 0.5) / coarse
    m = np.arange(coarse)
    w = np.where(m > 0, 2.0, 1.0)
    return (np.cos(np.outer(j, m)) * w) @ np.cos(np.outer(t, m)).T / fine


def phi_table(fine, coarse):
    f = 2.0 * math.pi * np.arange(fine) / fine
    g = 2.0 * math.pi * np.arange(coarse) / coarse
    m = np.arange(coarse // 2 + 1)
    v = np.where((m > 0) & (m < coarse // 2), 2.0, 1.0)
    cos_part = (np.cos(np.outer(g, m)) * v) @ np.cos(np.outer(f, m)).T
    sin_part = (np.sin(np.outer(g, m)) * v) @ np.sin(np.outer(f, m)).T
    return (cos_part + sin_part) / fine


def split_const(a):
    hi = np.asarray(a, np.float32).astype(BF16)
    lo = (np.asarray(a) - hi.astype(np.float64)).astype(np.float32).astype(BF16)
    return jnp.asarray(hi), jnp.asarray(lo)


def split(x):
    hi = x.astype(BF16)
    return hi, (x - hi.astype(F32)).astype(BF16)


def dot(a, b):
    return jnp.dot(a, b, preferred_element_type=F32)


def dot3(a, b):
    return dot(a[0], b[0]) + (dot(a[0], b[1]) + dot(a[1], b[0]))


def phase_tables(member, theta_count, phase_ref):
    rows, lons = phase_ref.shape[2], phase_ref.shape[3]
    quarter = lons // 4
    row = lax.broadcasted_iota(jnp.int32, (rows, 2 * quarter), 0)
    lon = lax.broadcasted_iota(jnp.int32, (rows, 2 * quarter), 1)
    theta = math.pi * ((row + member * rows).astype(F32) + 0.5) / theta_count
    phi = 2.0 * math.pi * lon.astype(F32) / lons
    x_arg = REACH * (jnp.sin(theta) * jnp.cos(phi))
    cos_x, sin_x = jnp.cos(x_arg), jnp.sin(x_arg)
    z_arg = REACH * jnp.cos(theta[:, :quarter])
    cz, sz = jnp.cos(z_arg), jnp.sin(z_arg)
    c0, c1 = cos_x[:, :quarter], cos_x[:, quarter:]
    s0, s1 = sin_x[:, :quarter], sin_x[:, quarter:]
    x_parts = ((c0, s0), (c1, s1), (c0, -s0), (c1, -s1))
    for q in range(4):
        ca, sa = x_parts[q]
        cb, sb = x_parts[(q + 3) % 4]
        cc, ss, sc, cs = ca * cb, sa * sb, sa * cb, ca * sb
        lanes = pl.ds(q * quarter, quarter)
        for octant in range(8):
            sgx = 1 - 2 * (octant % 2)
            sgy = 1 - 2 * (octant // 2 % 2)
            sgz = 1 - 2 * (octant // 4)
            re = cc - ss if sgx * sgy > 0 else cc + ss
            im = (sc if sgx > 0 else -sc) + (cs if sgy > 0 else -cs)
            szz = sz if sgz > 0 else -sz
            phase_ref[octant, 0, :, lanes] = re * cz - im * szz
            phase_ref[octant, 1, :, lanes] = re * szz + im * cz


def copy_all(pairs, sems):
    copies = [
        pltpu.make_async_copy(source, target, sems.at[n])
        for n, (source, target) in enumerate(pairs)
    ]
    for copy in copies:
        copy.start()
    return copies


def ends_kernel(patterns, operators, again, *rest):
    *rest, first, second, sems = rest
    tables = len(rest) // 2
    width = first.shape[0]
    last = patterns.shape[0] - width
    odd = lax.axis_index("group") % 2
    pairs = [
        (patterns.at[pl.ds((1 - odd) * last, width)], first),
        (patterns.at[pl.ds(odd * last, width)], second),
        *zip(rest[:tables], rest[tables:]),
    ]
    for copy in copy_all(pairs, sems):
        copy.wait()


def halo_terms(jobs, own, operators, first, second, total):
    clusters, _, rows, _ = own.shape
    width = first.shape[0]
    total[...] = own[...]

    @pl.loop(0, jobs[jobs.shape[0] - 1][0, 0])
    def _(t):
        code = jobs[t][0, 0]
        e, h, n = code >> 16, (code >> 8) & 127, code & 255
        c = jnp.where(n < width, n, n + clusters - 2 * width)
        for source, halo in enumerate((first, second)):

            @pl.when(((code >> 15) & 1) == source)
            def _(halo=halo):
                for r in range(rows // 8):
                    band = pl.ds(r * 8, 8)
                    ore, oim = operators[e, 0, band, :], operators[e, 1, band, :]
                    pre, pim = halo[h, 0, band, :], halo[h, 1, band, :]
                    total[c, 0, band, :] += ore * pre - oim * pim
                    total[c, 1, band, :] += ore * pim + oim * pre


def tile(ref, value):
    return jnp.full(ref.shape[1:], value, jnp.int32)


def list_halo_terms(partners, op_index, width, jobs):
    clusters, terms = partners.shape
    group = lax.axis_index("group")
    count = jnp.int32(0)
    for n in range(2 * width):
        below = n < width
        c = n if below else n + clusters - 2 * width
        source = (1 - group % 2) if below else group % 2
        for p in range(terms):
            q = partners[c, p] - group * clusters
            h = jnp.clip(q + width if below else q - clusters, 0, width - 1)
            code = (op_index[c, p] << 16) + (source << 15) + (h << 8) + n
            jobs[count] = tile(jobs, code)
            count = count + jnp.where((q < 0) | (q >= clusters), 1, 0)
    jobs[jobs.shape[0] - 1] = tile(jobs, count)


def fill_slots(child_parent, slots, clusters, width, chips):
    base = lax.axis_index("group") * clusters

    early, late = jnp.int32(0), jnp.int32(chips)
    for k in range(slots.shape[0]):
        q = child_parent[k] - base
        inner = (q >= width) & (q < clusters - width) & (early < chips)
        slots[jnp.where(inner, early, late)] = k
        step = jnp.where(inner, 1, 0)
        early, late = early + step, late + 1 - step


def slot_of(chip, i, chips, per_chip):
    return chip if i == 0 else chips + chip * (per_chip - 1) + i - 1


def list_slots(child_parent, child_octant, slots, base, kids, child_of):
    chips = lax.axis_size("member") // CORES
    chip = lax.axis_index("member") // CORES
    per_chip = slots.shape[0] // chips
    for s in range(chips):
        for i in range(per_chip):
            k = slots[slot_of(chip ^ s, i, chips, per_chip)]
            at = s * per_chip + i
            kids[at] = tile(kids, ((child_parent[k] - base) << 3) + child_octant[k])
            child_of[at] = tile(child_of, k)


def shift_and_phi(order, first, kids, total, phase, phi_hi, phi_lo, outs, shifted):
    rows = total.shape[2]
    per_chip = kids.shape[0] * CORES // lax.axis_size("member")
    count = outs[0].shape[0]
    size = count * 2 * rows
    for m, s in enumerate(order):
        for i in range(count):
            code = kids[s * per_chip + first + i][0, 0]
            q, o = code >> 3, code & 7
            for r in range(rows // 8):
                band = pl.ds(r * 8, 8)
                pre, pim = total[q, 0, band, :], total[q, 1, band, :]
                ere, eim = phase[o, 0, band, :], phase[o, 1, band, :]
                at = m * size + i * 2 * rows + r * 8
                shifted[pl.ds(at, 8), :] = pre * ere - pim * eim
                shifted[pl.ds(at + rows, 8), :] = pre * eim + pim * ere
    y = dot3(split(shifted[...]), (phi_hi[...], phi_lo[...]))
    for m, out in enumerate(outs):
        out[...] = y[m * size:(m + 1) * size].reshape(out.shape)


def first_kernel(
    order, jobs, kids, own, operators, first, second, phase, phi_hi, phi_lo, *rest
):
    *outs, total, shifted = rest
    halo_terms(jobs, own, operators, first, second, total)
    shift_and_phi(order, 1, kids, total, phase, phi_hi, phi_lo, outs, shifted)


def later_kernel(order, first, kids, total, phase, phi_hi, phi_lo, *rest):
    *outs, shifted = rest
    shift_and_phi(order, first, kids, total, phase, phi_hi, phi_lo, outs, shifted)


def own_kernel(
    theta_count, width, partners_in, op_in, parent_in, octant_in, patterns, operators, hi_in,
    lo_in, out, phase, kids, child_of, jobs, *rest
):
    *early, partners, op_index, child_parent, child_octant, slots, shifted, phi_hi, phi_lo, sems = (
        rest
    )
    clusters, terms = partners.shape
    rows = out.shape[2]
    copies = copy_all(
        [
            (partners_in, partners),
            (op_in, op_index),
            (parent_in, child_parent),
            (octant_in, child_octant),
            (hi_in, phi_hi),
            (lo_in, phi_lo),
        ],
        sems,
    )
    phase_tables(lax.axis_index("member"), theta_count, phase)
    base = lax.axis_index("group") * clusters
    for copy in copies[:4]:
        copy.wait()

    def translate(c, edge):
        for r in range(rows // 8):
            band = pl.ds(r * 8, 8)
            re, im = 0.0, 0.0
            for p in range(terms):
                q, e = partners[c, p] - base, op_index[c, p]
                ore, oim = operators[e, 0, band, :], operators[e, 1, band, :]
                if edge:
                    keep = jnp.where((q >= 0) & (q < clusters), 1.0, 0.0).astype(F32)
                    q = jnp.clip(q, 0, clusters - 1)
                    ore, oim = ore * keep, oim * keep
                pre, pim = patterns[q, 0, band, :], patterns[q, 1, band, :]
                re = re + (ore * pre - oim * pim)
                im = im + (ore * pim + oim * pre)
            out[c, 0, band, :] = re
            out[c, 1, band, :] = im

    @pl.loop(width, clusters - width)
    def _(c):
        translate(c, False)

    @pl.loop(0, 2 * width)
    def _(n):
        translate(jnp.where(n < width, n, n + clusters - 2 * width), True)

    for copy in copies[4:]:
        copy.wait()

    chips = len(early) + 1
    fill_slots(child_parent, slots, clusters, width, chips)
    list_slots(child_parent, child_octant, slots, base, kids, child_of)
    list_halo_terms(partners, op_index, width, jobs)
    shift_and_phi(range(1, chips), 0, kids, out, phase, phi_hi, phi_lo, early, shifted)


def theta_kernel(away, t_hi, t_lo, *rest):
    mine, *blocks, out, lats = rest
    chips = len(blocks) // 2 + 1
    early, late = blocks[:chips - 1], blocks[chips - 1:]
    member = lax.axis_index("member")
    chip, core = member // CORES, member % CORES
    t = core * CORES + (1 - core if away else core)
    rows = mine.shape[2]
    for i in range(out.shape[0]):
        for part in range(2):
            for s in range(chips):
                at = pl.multiple_of((chip ^ s) * rows, rows)
                if s == 0:
                    block = mine[i, part]
                else:
                    block = early[s - 1][0, part] if i == 0 else late[s - 1][i - 1, part]
                lats[pl.ds(at, rows), :] = block
            out[i, part] = dot3((t_hi[t], t_lo[t]), split(lats[...]))


def sum_kernel(keep, arrived, *outs):
    chip = lax.axis_index("member") // CORES
    rows = outs[0].shape[2]
    for s, out in enumerate(outs):
        band = pl.ds(pl.multiple_of((chip ^ s) * rows, rows), rows)
        out[...] = keep[:, :, band, :] + arrived[:, :, band, :]


def place_kernel(child_of, *rest):
    *blocks, out, sems = rest
    per_chip = blocks[0].shape[0]
    pairs = [
        (block.at[i], out.at[child_of[s * per_chip + i][0, 0]])
        for s, block in enumerate(blocks)
        for i in range(per_chip)
    ]
    for copy in copy_all(pairs, sems):
        copy.wait()


def in_hbm(x):
    return pltpu.with_memory_space_constraint(x, pltpu.HBM)


def shape(*dims):
    return jax.ShapeDtypeStruct(dims, F32)


def params(limit):
    return pltpu.CompilerParams(vmem_limit_bytes=limit * MIB)


def call(*args, **kwargs):
    return pl.pallas_call(*args, **kwargs)


def cost(us):
    return pl.CostEstimate(flops=us * 2_000_000, bytes_accessed=us * 3_000_000, transcendentals=0)


def on_device(patterns, operators, partners, operator_index, child_parent, child_octant):
    clusters, _, rows, lons = patterns.shape
    members = lax.axis_size("member")
    groups = lax.axis_size("group")
    theta_count = rows * members
    chips = members // CORES
    children = child_parent.shape[0]
    per_chip = children // chips
    out_rows = NTC // members
    width = clusters // 4
    member = lax.axis_index("member")
    chip, core = member // CORES, member % CORES
    end = shape(width, 2, rows, lons)
    tables = (partners, operator_index, child_parent, child_octant)
    *tables, first, second = pl.pallas_call(
        ends_kernel,
        out_shape=tuple(jax.ShapeDtypeStruct(x.shape, x.dtype) for x in tables) + (end, end),
        in_specs=[HBM] * (3 + len(tables)),
        out_specs=(VMEM,) * (2 + len(tables)),
        scratch_shapes=[pltpu.SemaphoreType.DMA((2 + len(tables),))],
        compiler_params=params(4),
    )(*map(in_hbm, (patterns, operators, operators, *tables)))
    partners, operator_index, child_parent, child_octant = tables
    pairs = [[(i, i + 1) for i in range(start, groups - 1, 2)] for start in range(2)]
    pairs = [both + [(j, i) for i, j in both] for both in pairs]
    first = lax.ppermute(first, "group", pairs[0])
    second = lax.ppermute(second, "group", pairs[1])

    phi = split_const(phi_table(lons, NPC).T)
    assert per_chip > 1 and clusters - 2 * width >= chips
    slots = pltpu.SMEM((children,), jnp.int32)
    total_shape = shape(clusters, 2, rows, lons)

    def blocks_of(count, number):
        return (shape(count, 2, rows, NPC),) * number

    def rows_of(count):
        return pltpu.VMEM((count * 2 * rows, lons), F32)

    def between_chips(blocks):
        moved = []
        for s in range(chips - 1, 0, -1):
            pairs = [(i, i ^ (CORES * s)) for i in range(members)]
            moved.append(lax.ppermute(blocks[s], "member", pairs))
        return moved[::-1]

    def tiles(count):
        return jax.ShapeDtypeStruct((count, 8, 128), jnp.int32)

    own, phase, kids, child_of, jobs, *early = call(
        functools.partial(own_kernel, theta_count, width),
        out_shape=(
            total_shape,
            shape(8, 2, rows, lons),
            tiles(children),
            tiles(children),
            tiles(2 * width * partners.shape[1] + 1),
        )
        + blocks_of(1, chips - 1),
        in_specs=[VMEM] * 6 + [HBM] * 2,
        out_specs=(VMEM,) * (chips + 4),
        scratch_shapes=[
            pltpu.SMEM(partners.shape, jnp.int32),
            pltpu.SMEM(partners.shape, jnp.int32),
            slots,
            slots,
            slots,
            rows_of(chips - 1),
            pltpu.VMEM(phi[0].shape, BF16),
            pltpu.VMEM(phi[1].shape, BF16),
            pltpu.SemaphoreType.DMA((6,)),
        ],
        compiler_params=params(20),
        cost_estimate=cost(8),
    )(
        partners, operator_index, child_parent, child_octant, patterns, operators,
        *map(in_hbm, phi),
    )
    early = between_chips(dict(enumerate(early, 1)))

    count = per_chip - 1
    far, near = [chips - 1], list(range(1, chips - 1))
    late = {}
    *outs, total = call(
        functools.partial(first_kernel, far),
        out_shape=blocks_of(count, len(far)) + (total_shape,),
        in_specs=[VMEM] * 9,
        out_specs=(VMEM,) * (len(far) + 1),
        scratch_shapes=[rows_of(count * len(far))],
        compiler_params=params(20),
        cost_estimate=cost(2),
    )(jobs, kids, own, operators, first, second, phase, *phi)
    late.update(zip(far, outs))

    def later(order, first_child, number):
        return call(
            functools.partial(later_kernel, order, first_child),
            out_shape=blocks_of(number, len(order)),
            in_specs=[VMEM] * 5,
            out_specs=(VMEM,) * len(order),
            scratch_shapes=[rows_of(number * len(order))],
            compiler_params=params(20),
            cost_estimate=cost(1),
        )(kids, total, phase, *phi)

    late.update(zip(near, later(near, 1, count)))
    late = between_chips(late)
    (mine,) = later([0], 0, per_chip)

    theta = theta_table(theta_count, NTC).reshape(chips, CORES, out_rows, chips, CORES, rows)
    theta = theta.transpose(4, 1, 0, 2, 3, 5).reshape(
        CORES * CORES, chips * out_rows, chips * rows
    )
    swap = [(i, i ^ 1) for i in range(members)]
    if out_rows % 8 == 0:
        half = shape(per_chip, 2, chips * out_rows, NPC)
        away, keep = (
            call(
                functools.partial(theta_kernel, name == "away"),
                out_shape=half,
                in_specs=[VMEM] * (1 + 2 * chips),
                out_specs=VMEM,
                scratch_shapes=[pltpu.VMEM((chips * rows, NPC), F32)],
                compiler_params=params(12),
                cost_estimate=cost(1),
            )(*split_const(theta), mine, *early, *late)
            for name in ("away", "keep")
        )
        swapped = lax.ppermute(away, "member", swap)
        pieces = call(
            sum_kernel,
            out_shape=(shape(per_chip, 2, out_rows, NPC),) * chips,
            in_specs=[VMEM] * 2,
            out_specs=(VMEM,) * chips,
            compiler_params=params(12),
            cost_estimate=cost(1),
        )(keep, swapped)
    else:
        order = chip ^ jnp.arange(chips)
        lats = jnp.stack([mine] + [jnp.concatenate(pair) for pair in zip(early, late)])
        lats = jnp.take(lats, order, axis=0)
        lats = lats.transpose(1, 2, 0, 3, 4).reshape(per_chip, 2, chips * rows, NPC)
        both = jnp.take(
            jnp.asarray(theta, F32).reshape(CORES, CORES, chips * out_rows, chips * rows),
            core, axis=0,
        )
        sums = jnp.einsum(
            "wjt,kptg->wkpjg", both, lats, precision=lax.Precision.HIGHEST
        )
        moved = lax.ppermute(jnp.take(sums, 1 - core, axis=0), "member", swap)
        pieces = jnp.take(sums, core, axis=0) + moved
        pieces = pieces.reshape(per_chip, 2, chips, out_rows, NPC)
        pieces = [jnp.take(pieces, order[s], axis=2) for s in range(chips)]

    final = [pieces[0], *between_chips(dict(enumerate(pieces)))]
    return call(
        place_kernel,
        out_shape=shape(children, 2, out_rows, NPC),
        in_specs=[VMEM] * (1 + chips),
        out_specs=HBM,
        scratch_shapes=[pltpu.SemaphoreType.DMA((children,))],
        compiler_params=params(12),
        cost_estimate=cost(1),
    )(child_of, *final)


def solution(mesh):
    return jax.shard_map(
        on_device,
        mesh=mesh,
        in_specs=(
            P("group", None, "member", None),
            P(None, None, "member", None),
            P("group", None),
            P("group", None),
            P("group"),
            P("group"),
        ),
        out_specs=P("group", None, "member", None),
        check_vma=False,
    )
```

```python
import functools
import math

import jax
import jax.numpy as jnp
import numpy as np
from jax import lax
from jax.experimental import pallas as pl
from jax.experimental.pallas import tpu as pltpu
from jax.sharding import PartitionSpec as P


NTC = 128
NPC = 256
CORES = 2
REACH = 6.0
F32 = jnp.float32
BF16 = jnp.bfloat16
MIB = 1 << 20


VMEM = pl.BlockSpec(memory_space=pltpu.VMEM)
SMEM = pl.BlockSpec(memory_space=pltpu.SMEM)
HBM = pl.BlockSpec(memory_space=pltpu.HBM)


def theta_table(fine, coarse):
    t = math.pi * (np.arange(fine) + 0.5) / fine
    j = math.pi * (np.arange(coarse) + 0.5) / coarse
    m = np.arange(coarse)
    w = np.where(m > 0, 2.0, 1.0)
    return (np.cos(np.outer(j, m)) * w) @ np.cos(np.outer(t, m)).T / fine


def phi_table(fine, coarse):
    f = 2.0 * math.pi * np.arange(fine) / fine
    g = 2.0 * math.pi * np.arange(coarse) / coarse
    m = np.arange(coarse // 2 + 1)
    v = np.where((m > 0) & (m < coarse // 2), 2.0, 1.0)
    cos_part = (np.cos(np.outer(g, m)) * v) @ np.cos(np.outer(f, m)).T
    sin_part = (np.sin(np.outer(g, m)) * v) @ np.sin(np.outer(f, m)).T
    return (cos_part + sin_part) / fine


def split_const(a):
    hi = np.asarray(a, np.float32).astype(BF16)
    lo = (np.asarray(a) - hi.astype(np.float64)).astype(np.float32).astype(BF16)
    return jnp.asarray(hi), jnp.asarray(lo)


def split(x):
    hi = x.astype(BF16)
    return hi, (x - hi.astype(F32)).astype(BF16)


def dot(a, b):
    return jnp.dot(a, b, preferred_element_type=F32)


def dot3(a, b):
    return dot(a[0], b[0]) + (dot(a[0], b[1]) + dot(a[1], b[0]))


def phase_tables(member, theta_count, phase_ref, between):
    rows, lons = phase_ref.shape[2], phase_ref.shape[3]
    quarter = lons // 4
    row = lax.broadcasted_iota(jnp.int32, (rows, 2 * quarter), 0)
    lon = lax.broadcasted_iota(jnp.int32, (rows, 2 * quarter), 1)
    theta = math.pi * ((row + member * rows).astype(F32) + 0.5) / theta_count
    phi = 2.0 * math.pi * lon.astype(F32) / lons
    x_arg = REACH * (jnp.sin(theta) * jnp.cos(phi))
    cos_x, sin_x = jnp.cos(x_arg), jnp.sin(x_arg)
    z_arg = REACH * jnp.cos(theta[:, :quarter])
    cz, sz = jnp.cos(z_arg), jnp.sin(z_arg)
    c0, c1 = cos_x[:, :quarter], cos_x[:, quarter:]
    s0, s1 = sin_x[:, :quarter], sin_x[:, quarter:]
    x_parts = ((c0, s0), (c1, s1), (c0, -s0), (c1, -s1))
    between()
    for q in range(4):
        ca, sa = x_parts[q]
        cb, sb = x_parts[(q + 3) % 4]
        cc, ss, sc, cs = ca * cb, sa * sb, sa * cb, ca * sb
        lanes = pl.ds(q * quarter, quarter)
        for octant in range(8):
            sgx = 1 - 2 * (octant % 2)
            sgy = 1 - 2 * (octant // 2 % 2)
            sgz = 1 - 2 * (octant // 4)
            re = cc - ss if sgx * sgy > 0 else cc + ss
            im = (sc if sgx > 0 else -sc) + (cs if sgy > 0 else -cs)
            szz = sz if sgz > 0 else -sz
            phase_ref[octant, 0, :, lanes] = re * cz - im * szz
            phase_ref[octant, 1, :, lanes] = re * szz + im * cz


def copy_all(pairs, sems):
    copies = [
        pltpu.make_async_copy(source, target, sems.at[n])
        for n, (source, target) in enumerate(pairs)
    ]
    for copy in copies:
        copy.start()
    return copies


def ends_kernel(patterns, operators, again, *rest):
    *rest, first, second, sems = rest
    tables = len(rest) // 2
    width = first.shape[0]
    last = patterns.shape[0] - width
    odd = lax.axis_index("group") % 2
    pairs = [
        (patterns.at[pl.ds((1 - odd) * last, width)], first),
        (patterns.at[pl.ds(odd * last, width)], second),
        *zip(rest[:tables], rest[tables:]),
    ]
    for copy in copy_all(pairs, sems):
        copy.wait()


def halo_terms(jobs, own, operators, first, second, total):
    clusters, _, rows, _ = own.shape
    width = first.shape[0]
    total[...] = own[...]

    @pl.loop(0, jobs[jobs.shape[0] - 1][0, 0])
    def _(t):
        code = jobs[t][0, 0]
        e, h, n = code >> 16, (code >> 8) & 127, code & 255
        c = jnp.where(n < width, n, n + clusters - 2 * width)
        for source, halo in enumerate((first, second)):

            @pl.when(((code >> 15) & 1) == source)
            def _(halo=halo):
                for r in range(rows // 8):
                    band = pl.ds(r * 8, 8)
                    ore, oim = operators[e, 0, band, :], operators[e, 1, band, :]
                    pre, pim = halo[h, 0, band, :], halo[h, 1, band, :]
                    total[c, 0, band, :] += ore * pre - oim * pim
                    total[c, 1, band, :] += ore * pim + oim * pre


def tile(ref, value):
    return jnp.full(ref.shape[1:], value, jnp.int32)


def list_halo_terms(partners, op_index, width, jobs):
    clusters, terms = partners.shape
    group = lax.axis_index("group")
    count = jnp.int32(0)
    for n in range(2 * width):
        below = n < width
        c = n if below else n + clusters - 2 * width
        source = (1 - group % 2) if below else group % 2
        for p in range(terms):
            q = partners[c, p] - group * clusters
            h = jnp.clip(q + width if below else q - clusters, 0, width - 1)
            code = (op_index[c, p] << 16) + (source << 15) + (h << 8) + n
            jobs[count] = tile(jobs, code)
            count = count + jnp.where((q < 0) | (q >= clusters), 1, 0)
    jobs[jobs.shape[0] - 1] = tile(jobs, count)


def fill_slots(child_parent, slots, clusters, width, chips):
    base = lax.axis_index("group") * clusters

    early, late = jnp.int32(0), jnp.int32(chips)
    for k in range(slots.shape[0]):
        q = child_parent[k] - base
        inner = (q >= width) & (q < clusters - width) & (early < chips)
        slots[jnp.where(inner, early, late)] = k
        step = jnp.where(inner, 1, 0)
        early, late = early + step, late + 1 - step


def slot_of(chip, i, chips, per_chip):
    return chip if i == 0 else chips + chip * (per_chip - 1) + i - 1


def list_slots(child_parent, child_octant, slots, base, kids, child_of):
    chips = lax.axis_size("member") // CORES
    chip = lax.axis_index("member") // CORES
    per_chip = slots.shape[0] // chips
    for s in range(chips):
        for i in range(per_chip):
            k = slots[slot_of(chip ^ s, i, chips, per_chip)]
            at = s * per_chip + i
            kids[at] = tile(kids, ((child_parent[k] - base) << 3) + child_octant[k])
            child_of[at] = tile(child_of, k)


def shift_and_phi(order, first, kids, total, phase, phi_hi, phi_lo, outs, shifted):
    rows = total.shape[2]
    per_chip = kids.shape[0] * CORES // lax.axis_size("member")
    count = outs[0].shape[0]
    size = count * 2 * rows
    for m, s in enumerate(order):
        for i in range(count):
            code = kids[s * per_chip + first + i][0, 0]
            q, o = code >> 3, code & 7
            for r in range(rows // 8):
                band = pl.ds(r * 8, 8)
                pre, pim = total[q, 0, band, :], total[q, 1, band, :]
                ere, eim = phase[o, 0, band, :], phase[o, 1, band, :]
                at = m * size + i * 2 * rows + r * 8
                shifted[pl.ds(at, 8), :] = pre * ere - pim * eim
                shifted[pl.ds(at + rows, 8), :] = pre * eim + pim * ere
    y = dot3(split(shifted[...]), (phi_hi[...], phi_lo[...]))
    for m, out in enumerate(outs):
        out[...] = y[m * size:(m + 1) * size].reshape(out.shape)


def first_kernel(
    order, jobs, kids, own, operators, first, second, phase, phi_hi, phi_lo, *rest
):
    *outs, total, shifted = rest
    halo_terms(jobs, own, operators, first, second, total)
    shift_and_phi(order, 1, kids, total, phase, phi_hi, phi_lo, outs, shifted)


def later_kernel(order, first, kids, total, phase, phi_hi, phi_lo, *rest):
    *outs, shifted = rest
    shift_and_phi(order, first, kids, total, phase, phi_hi, phi_lo, outs, shifted)


def own_kernel(
    theta_count, width, partners_in, op_in, parent_in, octant_in, patterns, operators, hi_in,
    lo_in, out, phase, kids, child_of, jobs, *rest
):
    *early, partners, op_index, child_parent, child_octant, slots, shifted, phi_hi, phi_lo, sems = (
        rest
    )
    clusters, terms = partners.shape
    rows = out.shape[2]
    copies = copy_all(
        [
            (partners_in, partners),
            (op_in, op_index),
            (parent_in, child_parent),
            (octant_in, child_octant),
            (hi_in, phi_hi),
            (lo_in, phi_lo),
        ],
        sems,
    )
    base = lax.axis_index("group") * clusters
    chips = len(early) + 1

    def lists():
        for copy in copies[:4]:
            copy.wait()
        fill_slots(child_parent, slots, clusters, width, chips)
        list_slots(child_parent, child_octant, slots, base, kids, child_of)
        list_halo_terms(partners, op_index, width, jobs)

    phase_tables(lax.axis_index("member"), theta_count, phase, lists)

    def translate(c, edge):
        for r in range(rows // 8):
            band = pl.ds(r * 8, 8)
            re, im = 0.0, 0.0
            for p in range(terms):
                q, e = partners[c, p] - base, op_index[c, p]
                ore, oim = operators[e, 0, band, :], operators[e, 1, band, :]
                if edge:
                    keep = jnp.where((q >= 0) & (q < clusters), 1.0, 0.0).astype(F32)
                    q = jnp.clip(q, 0, clusters - 1)
                    ore, oim = ore * keep, oim * keep
                pre, pim = patterns[q, 0, band, :], patterns[q, 1, band, :]
                re = re + (ore * pre - oim * pim)
                im = im + (ore * pim + oim * pre)
            out[c, 0, band, :] = re
            out[c, 1, band, :] = im

    @pl.loop(width, clusters - width)
    def _(c):
        translate(c, False)

    @pl.loop(0, 2 * width)
    def _(n):
        translate(jnp.where(n < width, n, n + clusters - 2 * width), True)

    for copy in copies[4:]:
        copy.wait()

    shift_and_phi(range(1, chips), 0, kids, out, phase, phi_hi, phi_lo, early, shifted)


def theta_kernel(away, t_hi, t_lo, *rest):
    mine, *blocks, out, lats = rest
    chips = len(blocks) // 2 + 1
    early, late = blocks[:chips - 1], blocks[chips - 1:]
    member = lax.axis_index("member")
    chip, core = member // CORES, member % CORES
    t = core * CORES + (1 - core if away else core)
    rows = mine.shape[2]
    for i in range(out.shape[0]):
        for part in range(2):
            for s in range(chips):
                at = pl.multiple_of((chip ^ s) * rows, rows)
                if s == 0:
                    block = mine[i, part]
                else:
                    block = early[s - 1][0, part] if i == 0 else late[s - 1][i - 1, part]
                lats[pl.ds(at, rows), :] = block
            out[i, part] = dot3((t_hi[t], t_lo[t]), split(lats[...]))


def sum_kernel(keep, arrived, *outs):
    chip = lax.axis_index("member") // CORES
    rows = outs[0].shape[2]
    for s, out in enumerate(outs):
        band = pl.ds(pl.multiple_of((chip ^ s) * rows, rows), rows)
        out[...] = keep[:, :, band, :] + arrived[:, :, band, :]


def place_kernel(child_of, *rest):
    *blocks, out, sems = rest
    per_chip = blocks[0].shape[0]
    pairs = [
        (block.at[i], out.at[child_of[s * per_chip + i][0, 0]])
        for s, block in enumerate(blocks)
        for i in range(per_chip)
    ]
    for copy in copy_all(pairs, sems):
        copy.wait()


def in_hbm(x):
    return pltpu.with_memory_space_constraint(x, pltpu.HBM)


def shape(*dims):
    return jax.ShapeDtypeStruct(dims, F32)


def params(limit):
    return pltpu.CompilerParams(vmem_limit_bytes=limit * MIB)


def call(*args, **kwargs):
    return pl.pallas_call(*args, **kwargs)


def cost(us):
    return pl.CostEstimate(flops=us * 2_000_000, bytes_accessed=us * 3_000_000, transcendentals=0)


def on_device(patterns, operators, partners, operator_index, child_parent, child_octant):
    clusters, _, rows, lons = patterns.shape
    members = lax.axis_size("member")
    groups = lax.axis_size("group")
    theta_count = rows * members
    chips = members // CORES
    children = child_parent.shape[0]
    per_chip = children // chips
    out_rows = NTC // members
    width = clusters // 4
    member = lax.axis_index("member")
    chip, core = member // CORES, member % CORES
    end = shape(width, 2, rows, lons)
    tables = (partners, operator_index, child_parent, child_octant)
    *tables, first, second = pl.pallas_call(
        ends_kernel,
        out_shape=tuple(jax.ShapeDtypeStruct(x.shape, x.dtype) for x in tables) + (end, end),
        in_specs=[HBM] * (3 + len(tables)),
        out_specs=(VMEM,) * (2 + len(tables)),
        scratch_shapes=[pltpu.SemaphoreType.DMA((2 + len(tables),))],
        compiler_params=params(4),
    )(*map(in_hbm, (patterns, operators, operators, *tables)))
    partners, operator_index, child_parent, child_octant = tables
    pairs = [[(i, i + 1) for i in range(start, groups - 1, 2)] for start in range(2)]
    pairs = [both + [(j, i) for i, j in both] for both in pairs]
    first = lax.ppermute(first, "group", pairs[0])
    second = lax.ppermute(second, "group", pairs[1])

    phi = split_const(phi_table(lons, NPC).T)
    assert per_chip > 1 and clusters - 2 * width >= chips
    slots = pltpu.SMEM((children,), jnp.int32)
    total_shape = shape(clusters, 2, rows, lons)

    def blocks_of(count, number):
        return (shape(count, 2, rows, NPC),) * number

    def rows_of(count):
        return pltpu.VMEM((count * 2 * rows, lons), F32)

    def between_chips(blocks):
        moved = []
        for s in range(chips - 1, 0, -1):
            pairs = [(i, i ^ (CORES * s)) for i in range(members)]
            moved.append(lax.ppermute(blocks[s], "member", pairs))
        return moved[::-1]

    def tiles(count):
        return jax.ShapeDtypeStruct((count, 8, 128), jnp.int32)

    own, phase, kids, child_of, jobs, *early = call(
        functools.partial(own_kernel, theta_count, width),
        out_shape=(
            total_shape,
            shape(8, 2, rows, lons),
            tiles(children),
            tiles(children),
            tiles(2 * width * partners.shape[1] + 1),
        )
        + blocks_of(1, chips - 1),
        in_specs=[VMEM] * 6 + [HBM] * 2,
        out_specs=(VMEM,) * (chips + 4),
        scratch_shapes=[
            pltpu.SMEM(partners.shape, jnp.int32),
            pltpu.SMEM(partners.shape, jnp.int32),
            slots,
            slots,
            slots,
            rows_of(chips - 1),
            pltpu.VMEM(phi[0].shape, BF16),
            pltpu.VMEM(phi[1].shape, BF16),
            pltpu.SemaphoreType.DMA((6,)),
        ],
        compiler_params=params(20),
        cost_estimate=cost(8),
    )(
        partners, operator_index, child_parent, child_octant, patterns, operators,
        *map(in_hbm, phi),
    )
    early = between_chips(dict(enumerate(early, 1)))

    count = per_chip - 1
    far, near = [chips - 1], list(range(1, chips - 1))
    late = {}
    *outs, total = call(
        functools.partial(first_kernel, far),
        out_shape=blocks_of(count, len(far)) + (total_shape,),
        in_specs=[VMEM] * 9,
        out_specs=(VMEM,) * (len(far) + 1),
        scratch_shapes=[rows_of(count * len(far))],
        compiler_params=params(20),
        cost_estimate=cost(2),
    )(jobs, kids, own, operators, first, second, phase, *phi)
    late.update(zip(far, outs))

    def later(order, first_child, number):
        return call(
            functools.partial(later_kernel, order, first_child),
            out_shape=blocks_of(number, len(order)),
            in_specs=[VMEM] * 5,
            out_specs=(VMEM,) * len(order),
            scratch_shapes=[rows_of(number * len(order))],
            compiler_params=params(20),
            cost_estimate=cost(1),
        )(kids, total, phase, *phi)

    late.update(zip(near, later(near, 1, count)))
    late = between_chips(late)
    (mine,) = later([0], 0, per_chip)

    theta = theta_table(theta_count, NTC).reshape(chips, CORES, out_rows, chips, CORES, rows)
    theta = theta.transpose(4, 1, 0, 2, 3, 5).reshape(
        CORES * CORES, chips * out_rows, chips * rows
    )
    swap = [(i, i ^ 1) for i in range(members)]
    if out_rows % 8 == 0:
        half = shape(per_chip, 2, chips * out_rows, NPC)
        away, keep = (
            call(
                functools.partial(theta_kernel, name == "away"),
                out_shape=half,
                in_specs=[VMEM] * (1 + 2 * chips),
                out_specs=VMEM,
                scratch_shapes=[pltpu.VMEM((chips * rows, NPC), F32)],
                compiler_params=params(12),
                cost_estimate=cost(1),
            )(*split_const(theta), mine, *early, *late)
            for name in ("away", "keep")
        )
        swapped = lax.ppermute(away, "member", swap)
        pieces = call(
            sum_kernel,
            out_shape=(shape(per_chip, 2, out_rows, NPC),) * chips,
            in_specs=[VMEM] * 2,
            out_specs=(VMEM,) * chips,
            compiler_params=params(12),
            cost_estimate=cost(1),
        )(keep, swapped)
    else:
        order = chip ^ jnp.arange(chips)
        lats = jnp.stack([mine] + [jnp.concatenate(pair) for pair in zip(early, late)])
        lats = jnp.take(lats, order, axis=0)
        lats = lats.transpose(1, 2, 0, 3, 4).reshape(per_chip, 2, chips * rows, NPC)
        both = jnp.take(
            jnp.asarray(theta, F32).reshape(CORES, CORES, chips * out_rows, chips * rows),
            core, axis=0,
        )
        sums = jnp.einsum(
            "wjt,kptg->wkpjg", both, lats, precision=lax.Precision.HIGHEST
        )
        moved = lax.ppermute(jnp.take(sums, 1 - core, axis=0), "member", swap)
        pieces = jnp.take(sums, core, axis=0) + moved
        pieces = pieces.reshape(per_chip, 2, chips, out_rows, NPC)
        pieces = [jnp.take(pieces, order[s], axis=2) for s in range(chips)]

    final = [pieces[0], *between_chips(dict(enumerate(pieces)))]
    return call(
        place_kernel,
        out_shape=shape(children, 2, out_rows, NPC),
        in_specs=[VMEM] * (1 + chips),
        out_specs=HBM,
        scratch_shapes=[pltpu.SemaphoreType.DMA((children,))],
        compiler_params=params(12),
        cost_estimate=cost(1),
    )(child_of, *final)


def solution(mesh):
    return jax.shard_map(
        on_device,
        mesh=mesh,
        in_specs=(
            P("group", None, "member", None),
            P(None, None, "member", None),
            P("group", None),
            P("group", None),
            P("group"),
            P("group"),
        ),
        out_specs=P("group", None, "member", None),
        check_vma=False,
    )
```
